256 devices in a mesh: loader: 64 (over z, x, core), split: 4 (over y).
Axes of the slice: x: 4, y: 4, z: 8, core: 2. Of those that a mesh axis runs over, the one named last changes fastest.
Arguments:
- embeddings: bfloat16 [131072, 768], P(('loader', 'split')), may hold values from -6 to 6
- cluster_ids: int32 [131072, 1], P(('loader', 'split')), may hold values from 0 to 255; in each aligned block of 512 rows (0 to 511, 512 to 1023, ...) at most 4 rows name the same one
- ranks: int32 [131072], P(('loader', 'split')), may hold values from 0 to 131071, each once
Outputs:
- nearest: float32 [131072], P(('loader', 'split'))
The draws below stay inside these ranges and needn't reach their ends.
Inputs may be any that keep to these rules, and one draw needn't show every extreme that they name: `cluster_ids`: among the 512 rows of one device no cluster appears more than 4 times. All ranks differ.
All inputs are finite; a program needn't handle non-finite values.
Results may differ from the reference program's by a relative error of at most 0.0014.
Values may be sent and summed in bfloat16 or wider, within the bound.
A program may use at most 64 MiB of HBM per device.

```python
import math
import jax
import jax.numpy as jnp
import numpy as np
from jax import lax

D = 768
ROWS_DEV = 512
CLUSTERS = 256
CAP = 4
ROWS = 131072
WINDOW = 1024


def steps_of(stream_key, extent, cuts, least, largest):
    factor_of, own = 1.0, jax.random.fold_in(stream_key, 6)
    for dim, parts in cuts:
        steps = jnp.exp(jax.random.uniform(jax.random.fold_in(own, dim), (parts,), jnp.float32, least / len(cuts), largest / len(cuts)))
        factor_of = factor_of * jnp.repeat(steps, extent[dim] // parts).reshape([-1 if axis == dim else 1 for axis in range(len(extent))])
    return factor_of


def routed_block(stream_key, own, number, rows, count, top, limit, skew):
    order = jax.random.permutation(stream_key, count)
    crowded, common = load_shares(count, rows * top, limit, skew, True), load_shares(count, rows * top, limit, skew, False)
    places = jnp.arange(count)

    def named(lengths, turn):
        used = int((lengths > 0).sum())
        fixed = max(1, used // 4)
        shifted = fixed + (places - fixed + turn * (used - fixed)) % max(1, count - fixed)
        return jnp.zeros((count,), jnp.int32).at[order[jnp.where(places < fixed, places, shifted)]].set(jnp.asarray(lengths, jnp.int32))

    lengths = jnp.where(number % 4 == 0, named(crowded, number // 4), named(common, number - number // 4 - 1))
    mixed = jax.random.permutation(jax.random.fold_in(own, 3), count)
    giver, taker = mixed[0:count // 2 * 2:2], mixed[1:count // 2 * 2:2]
    margin = jnp.minimum(lengths[giver] - 1, limit - lengths[taker]) // 2
    margin = jnp.where((giver == order[0]) | (taker == order[0]) | (lengths[taker] == 0), 0, jnp.maximum(margin, 0))
    shifted = jax.random.randint(jax.random.fold_in(own, 4), (count // 2,), 0, 1 << 20) % (margin + 1)
    lengths = lengths.at[giver].add(-shifted).at[taker].add(shifted)
    items = jnp.searchsorted(jnp.cumsum(lengths), jnp.arange(rows * top), side="right").astype(jnp.int32)
    grid = items.reshape(top, rows).T
    grid = grid[jax.random.permutation(jax.random.fold_in(own, 1), rows)]
    turn = jax.random.randint(jax.random.fold_in(own, 2), (rows, 1), 0, top)
    return jnp.take_along_axis(grid, (jnp.arange(top)[None, :] + turn) % top, axis=1)


def load_shares(amount, total, most, lean, full):
    portions = [(1 << 20) // math.isqrt(standing ** lean) + 1 for standing in range(1, amount + 1)]
    largest = most if full else min(most, max(-(-total // amount), total * portions[0] // sum(portions)))
    least = 1 if total - largest >= amount - 1 else 0
    given, surplus = [largest] + [least] * (amount - 1), total - largest - least * (amount - 1)
    while surplus > 0:
        movable = [i for i in range(1, amount) if given[i] < largest] or [i for i in range(1, amount) if given[i] < most]
        whole, left = sum([portions[i] for i in movable]), surplus
        for i in movable:
            addition = min(most - given[i], max(1, left * portions[i] // whole), surplus)
            given[i] = given[i] + addition
            surplus = surplus - addition
    return np.array(given)


def scatter_about(own_key, dims, scale, limit, cuts=(), kind=jnp.bfloat16):
    entries = jax.random.normal(own_key, dims, jnp.float32) * scale
    if len(cuts) > 0:
        entries = steps_of(own_key, dims, cuts, -0.22, 0.18) * entries
    return jnp.clip(entries, min=-limit, max=limit).astype(kind)


def setup_inputs(seed: int = 0) -> dict:
    keys = jax.random.split(jax.random.key(seed), 4)
    embeddings = scatter_about(keys[0], (ROWS, D), 1.0, 6.0, ((0, 256),))
    cluster_ids_keys = jax.random.split(jax.random.fold_in(keys[1], 1), ROWS // ROWS_DEV)
    cluster_ids_turns = jax.random.permutation(jax.random.fold_in(keys[1], 3), ROWS // ROWS_DEV)
    cluster_ids = jax.vmap(lambda own, number: routed_block(jax.random.fold_in(keys[1], 2), own, number, ROWS_DEV, CLUSTERS, 1, CAP, 2))(cluster_ids_keys, cluster_ids_turns).reshape((ROWS, 1))
    ranks = jax.random.permutation(keys[2], ROWS).astype(jnp.int32)
    return dict(embeddings=embeddings, cluster_ids=cluster_ids, ranks=ranks)


epsilon = 1e-06

def reference(embeddings, cluster_ids, ranks):
    values = embeddings.astype(jnp.float32)
    unit = (values * lax.rsqrt(lax.optimization_barrier(jnp.sum(values * values, axis=1, keepdims=True)) + epsilon)).astype(jnp.bfloat16)
    cluster = cluster_ids[:, 0].astype(jnp.int32)
    row_order = jnp.argsort(cluster, stable=True).astype(jnp.int32)
    sorted_cluster = cluster[row_order]
    sorted_unit = unit[row_order]
    sorted_rank = ranks[row_order]
    offsets = jnp.searchsorted(sorted_cluster, jnp.arange(CLUSTERS, dtype=jnp.int32)).astype(jnp.int32)
    padded_unit = jnp.concatenate([sorted_unit, jnp.zeros((WINDOW, unit.shape[1]), jnp.bfloat16)], axis=0)
    padded_cluster = jnp.concatenate([sorted_cluster, jnp.full((WINDOW,), -1, jnp.int32)], axis=0)
    padded_rank = jnp.concatenate([sorted_rank, jnp.full((WINDOW,), -1, jnp.int32)], axis=0)

    def per_cluster(which):
        offset = offsets[which]
        members = lax.dynamic_slice_in_dim(padded_unit, offset, WINDOW, 0)
        member_cluster = lax.dynamic_slice_in_dim(padded_cluster, offset, WINDOW, 0)
        member_rank = lax.dynamic_slice_in_dim(padded_rank, offset, WINDOW, 0)
        scores = jnp.dot(members, members.T, preferred_element_type=jnp.float32)
        allowed = (member_cluster == which)[None, :] & (member_rank[None, :] < member_rank[:, None])
        return lax.optimization_barrier(jnp.max(jnp.where(allowed, scores, jnp.float32(-1.0)), axis=1))
    results = lax.map(per_cluster, jnp.arange(CLUSTERS, dtype=jnp.int32))
    position = jnp.arange(sorted_cluster.shape[0], dtype=jnp.int32) - offsets[sorted_cluster]
    sorted_result = results[sorted_cluster, position]
    return jnp.zeros((cluster.shape[0],), jnp.float32).at[row_order].set(sorted_result)
```

```python
import functools

import jax
import jax.numpy as jnp
from jax import lax
from jax.experimental import pallas as pl
from jax.experimental.pallas import tpu as pltpu
from jax.sharding import PartitionSpec as P

MESH = pl.DeviceIdType.MESH
CLUSTERS = 256
CAP = 4
WIDTH = 768
ROWS_DEV = 512
PLANES = 8
PEERS = 32
SLOTS = PEERS * CAP
BLOCKS = ROWS_DEV // 128
ROOM = 128
EMPTY = float(1 << 17)
GROUPS = ((0,), (1, 7), (2, 6), (3, 5), (4,))
epsilon = 1e-06


def place():
    row = lax.axis_index("loader")
    y = lax.axis_index("split")
    return lax.div(row, 8), y, lax.rem(lax.div(row, 2), 4), lax.rem(row, 2)


def device(z, y, x, c):
    return ((z * 4 + x) * 2 + c, y)


def across(here, s):
    z, y, x, c = here
    return device(lax.rem(z + s, PLANES), y, x, c)


def within(here, j, sign):
    z, y, x, c = here
    dy, dx, dc = lax.rem(j, 4), lax.rem(lax.div(j, 4), 4), lax.div(j, 16)
    return device(
        z,
        lax.rem(y + 4 + sign * dy, 4),
        lax.rem(x + 4 + sign * dx, 4),
        lax.rem(c + dc, 2),
    )


def send(src, dst, sent, landed, to):
    return pltpu.make_async_remote_copy(
        src_ref=src,
        dst_ref=dst,
        send_sem=sent,
        recv_sem=landed,
        device_id=to,
        device_id_type=MESH,
    )


def product(a, b):
    return lax.dot_general(
        a, b, (((1,), (1,)), ((), ())), preferred_element_type=jnp.float32
    )


def iota(shape, dim):
    return lax.broadcasted_iota(jnp.int32, shape, dim)


def own_lanes(tiles_ref):
    group = iota((PLANES, SLOTS), 1) // CAP
    total = jnp.zeros((PLANES, SLOTS), jnp.float32)
    for j in range(PEERS):
        total = jnp.where(group == j, tiles_ref[j], total)
    return total


def kernel(
    emb_hbm, cid_ref, rank_ref, out_ref, flag_ref,
    raw, unit, meta_out, meta_in, rows_out, rows_in, dense, arrived, members,
    ranks_out, ranks_in, best_out, best_in, back_out, back_in,
    raw_sem, meta_sent, meta_landed, rows_sent, rows_landed, dense_sent, dense_landed,
    ranks_sent, ranks_landed, best_sent, best_landed, back_sent, back_landed,
):
    here = place()
    z, y, x, c = here
    loads = [
        pltpu.make_async_copy(
            emb_hbm.at[pl.ds(b * 128, 128)], raw.at[pl.ds(b * 128, 128)], raw_sem.at[b]
        )
        for b in range(BLOCKS)
    ]
    for load in loads:
        load.start()
    barrier = pltpu.get_barrier_semaphore()

    def greet_across(s, carry):
        pl.semaphore_signal(barrier, inc=1, device_id=across(here, s), device_id_type=MESH)
        return carry

    def greet_within(j, carry):
        pl.semaphore_signal(barrier, inc=1, device_id=within(here, j, 1), device_id_type=MESH)
        return carry

    lax.fori_loop(1, PLANES, greet_across, 0)
    lax.fori_loop(1, PEERS, greet_within, 0)

    cid = cid_ref[...]
    owner = cid & (PEERS - 1)
    step = ((cid >> 5) - z) & (PLANES - 1)
    peer = (
        (((owner >> 4) - c) & 1) * 16 + (((owner >> 2) - x) & 3) * 4 + ((owner - y) & 3)
    )
    turned = jnp.concatenate([cid, step], axis=0).T
    before = iota((128, 128), 0) < iota((128, 128), 1)
    slot_rows, pack_rows, over = [], [], jnp.zeros((1, 128), jnp.float32)
    for b in range(BLOCKS):
        same = jnp.zeros((128, 128), jnp.float32)
        along = jnp.zeros((128, 128), jnp.float32)
        for a in range(b + 1):
            alike = turned[:, a : a + 1] == cid[b : b + 1]
            aside = turned[:, BLOCKS + a : BLOCKS + a + 1] == step[b : b + 1]
            if a == b:
                alike, aside = alike & before, aside & before
            same += jnp.where(alike, 1.0, 0.0)
            along += jnp.where(aside, 1.0, 0.0)
        position = jnp.sum(same, axis=0, keepdims=True).astype(jnp.int32)
        count = jnp.sum(along, axis=0, keepdims=True).astype(jnp.int32)
        steps = step[b : b + 1] * SLOTS
        slot_rows.append(steps + peer[b : b + 1] * CAP + position)
        pack_rows.append(jnp.where(count < ROOM, steps + count, -1))
        over = jnp.maximum(over, jnp.where(count < ROOM, 0.0, 2 * EMPTY))
    over = jnp.max(over, axis=1, keepdims=True)
    slot_turned = jnp.concatenate(slot_rows + pack_rows, axis=0).T
    rank_turned = (rank_ref[...].astype(jnp.float32) - EMPTY).T
    lane = iota((128, 128), 1)
    for s in range(PLANES):
        name = jnp.zeros((128, 128), jnp.float32)
        rank = jnp.zeros((128, 128), jnp.float32)
        for b in range(BLOCKS):
            slots = slot_turned[:, b : b + 1]
            packs = slot_turned[:, BLOCKS + b : BLOCKS + b + 1]
            name = jnp.where(packs == s * SLOTS + lane, (slots - (s * SLOTS - 1)).astype(jnp.float32), name)
            rank = jnp.where(slots == s * SLOTS + lane, rank_turned[:, b : b + 1], rank)
        ref = meta_in if s == 0 else meta_out
        ref[s, 0:1] = jnp.sum(name, axis=0, keepdims=True) - 1.0
        ref[s, 1:2] = jnp.sum(rank, axis=0, keepdims=True) + (EMPTY + over)
    for b in range(BLOCKS):
        loads[b].wait()
        values = raw[b * 128 : (b + 1) * 128].astype(jnp.float32)
        scale = lax.rsqrt(jnp.sum(values * values, axis=1, keepdims=True) + epsilon)
        unit[b * 128 : (b + 1) * 128] = (values * scale).astype(jnp.bfloat16)

    pl.semaphore_wait(barrier, PLANES - 1 + PEERS - 1)
    metas, rows = {}, {}
    order = [s for group in GROUPS for s in group if s]
    for s in order:
        metas[s] = send(meta_out.at[s], meta_in.at[s], meta_sent.at[s], meta_landed.at[s], across(here, s))
        metas[s].start()
    pack = jnp.concatenate(pack_rows, axis=1)
    for group in GROUPS[1:] + GROUPS[:1]:
        chosen = jnp.concatenate(
            [jnp.where(pack == s * SLOTS + iota((ROOM, ROWS_DEV), 0), 1.0, 0.0) for s in group], axis=0
        ).astype(jnp.bfloat16)
        packed = jnp.dot(chosen, unit[...], preferred_element_type=jnp.float32).astype(jnp.bfloat16)
        for n, s in enumerate(group):
            ref = rows_in if s == 0 else rows_out
            ref[s] = packed[n * ROOM : (n + 1) * ROOM]
            if s:
                rows[s] = send(rows_out.at[s], rows_in.at[s], rows_sent.at[s], rows_landed.at[s], across(here, s))
                rows[s].start()

    def spread(s):
        chosen = jnp.where(
            meta_in[s, 0:1, :ROOM] == iota((SLOTS, ROOM), 0).astype(jnp.float32), 1.0, 0.0
        ).astype(jnp.bfloat16)
        placed = jnp.dot(chosen, rows_in[s], preferred_element_type=jnp.float32).astype(jnp.bfloat16)
        dense[s] = placed.reshape(PEERS, CAP, WIDTH)
        arrived[s, 0] = placed[:CAP]

        def deliver(j, carry):
            send(dense.at[s, j], arrived.at[s, j], dense_sent.at[s], dense_landed.at[s], within(here, j, 1)).start()
            return carry

        lax.fori_loop(1, PEERS, deliver, 0)

    for s in order:
        metas[s].wait_recv()
    for s in range(PLANES):
        ranks_out[s : s + 1] = meta_in[s, 1:2]
    ranks_in[0] = ranks_out[...]

    def deliver_ranks(j, carry):
        send(ranks_out, ranks_in.at[j], ranks_sent, ranks_landed, within(here, j, 1)).start()
        return carry

    lax.fori_loop(1, PEERS, deliver_ranks, 0)
    others = pl.ds(1, PEERS - 1)
    spread(0)

    best = [jnp.full((1, SLOTS), -1.0, jnp.float32)] * PLANES
    seen = []
    rank_row = rank_col = None
    for turn in range(1, len(GROUPS) + 1):
        if turn < len(GROUPS):
            for s in GROUPS[turn]:
                rows[s].wait_recv()
                spread(s)
        if turn == 1:
            send(ranks_in.at[others], ranks_in.at[others], ranks_sent, ranks_landed, within(here, 1, 1)).wait_recv()
            rank_row = own_lanes(ranks_in)
            rank_col = rank_row.T
            highest = jnp.full((PLANES, SLOTS), 0.0, jnp.float32)
            for j in range(PEERS):
                highest = jnp.maximum(highest, ranks_in[j])
            flag_ref[...] = jnp.where(highest >= 2 * EMPTY, 1.0, 0.0)
        group = GROUPS[turn - 1]
        known = len(seen)
        for s in group:
            send(dense.at[s, others], arrived.at[s, others], dense_sent.at[s], dense_landed.at[s], within(here, 1, 1)).wait_recv()
            members[len(seen) * SLOTS : (len(seen) + 1) * SLOTS] = arrived[s].reshape(SLOTS, WIDTH)
            seen.append(s)
        new = members[known * SLOTS : len(seen) * SLOTS]
        scores = product(members[: len(seen) * SLOTS], new)
        for n, q in enumerate(group):
            top = jnp.full((SLOTS, SLOTS), -1.0, jnp.float32)
            for k, m in enumerate(seen):
                part = scores[k * SLOTS : (k + 1) * SLOTS, n * SLOTS : (n + 1) * SLOTS]
                earlier = rank_col[:, m : m + 1] < rank_row[q : q + 1]
                top = jnp.maximum(top, jnp.where(earlier, part, -1.0))
            best[q] = jnp.maximum(best[q], jnp.max(top, axis=0, keepdims=True))
        if known:
            scores = product(new, members[: known * SLOTS])
            for k, q in enumerate(seen[:known]):
                top = jnp.full((SLOTS, SLOTS), -1.0, jnp.float32)
                for n, m in enumerate(group):
                    part = scores[n * SLOTS : (n + 1) * SLOTS, k * SLOTS : (k + 1) * SLOTS]
                    earlier = rank_col[:, m : m + 1] < rank_row[q : q + 1]
                    top = jnp.maximum(top, jnp.where(earlier, part, -1.0))
                best[q] = jnp.maximum(best[q], jnp.max(top, axis=0, keepdims=True))

    best_out[...] = jnp.concatenate(best, axis=0)

    def answer(j, carry):
        send(best_out, best_in.at[j], best_sent, best_landed, within(here, j, -1)).start()
        return carry

    lax.fori_loop(1, PEERS, answer, 0)
    best_in[0] = best_out[...]
    for s in order:
        metas[s].wait_send()
        rows[s].wait_send()
    for s in range(PLANES):
        send(dense.at[s, others], arrived.at[s, others], dense_sent.at[s], dense_landed.at[s], within(here, 1, 1)).wait_send()
    send(ranks_in.at[others], ranks_in.at[others], ranks_sent, ranks_landed, within(here, 1, 1)).wait_send()
    whole = send(best_in.at[others], best_in.at[others], best_sent, best_landed, within(here, 1, 1))
    whole.wait_recv()
    results = own_lanes(best_in)
    backs = []
    for s in range(PLANES):
        ref = back_in if s == 0 else back_out
        ref[s] = results[s : s + 1]
        if s:
            back = send(back_out.at[s], back_in.at[s], back_sent.at[s], back_landed.at[s], across(here, PLANES - s))
            back.start()
            backs.append(back)
    whole.wait_send()
    for back in backs:
        back.wait()
    result_col = jnp.concatenate([back_in[s] for s in range(PLANES)], axis=0).T
    slot = iota((SLOTS, 128), 0)
    for b in range(BLOCKS):
        found = jnp.zeros((SLOTS, 128), jnp.float32)
        for s in range(PLANES):
            found = jnp.where(slot_rows[b] == s * SLOTS + slot, result_col[:, s : s + 1], found)
        out_ref[b : b + 1] = jnp.sum(found, axis=0, keepdims=True)


def shards(embeddings, cluster_ids, ranks):
    dma = pltpu.SemaphoreType.DMA
    best, flag = pl.pallas_call(
        kernel,
        out_shape=(
            jax.ShapeDtypeStruct((BLOCKS, 128), jnp.float32),
            jax.ShapeDtypeStruct((PLANES, SLOTS), jnp.float32),
        ),
        in_specs=[
            pl.BlockSpec(memory_space=pl.ANY),
            pl.BlockSpec(memory_space=pltpu.VMEM),
            pl.BlockSpec(memory_space=pltpu.VMEM),
        ],
        out_specs=(pl.BlockSpec(memory_space=pltpu.VMEM),) * 2,
        scratch_shapes=[
            pltpu.VMEM((ROWS_DEV, WIDTH), jnp.bfloat16),
            pltpu.VMEM((ROWS_DEV, WIDTH), jnp.bfloat16),
            pltpu.VMEM((PLANES, 2, SLOTS), jnp.float32),
            pltpu.VMEM((PLANES, 2, SLOTS), jnp.float32),
            pltpu.VMEM((PLANES, ROOM, WIDTH), jnp.bfloat16),
            pltpu.VMEM((PLANES, ROOM, WIDTH), jnp.bfloat16),
            pltpu.VMEM((PLANES, PEERS, CAP, WIDTH), jnp.bfloat16),
            pltpu.VMEM((PLANES, PEERS, CAP, WIDTH), jnp.bfloat16),
            pltpu.VMEM((PLANES * SLOTS, WIDTH), jnp.bfloat16),
            pltpu.VMEM((PLANES, SLOTS), jnp.float32),
            pltpu.VMEM((PEERS, PLANES, SLOTS), jnp.float32),
            pltpu.VMEM((PLANES, SLOTS), jnp.float32),
            pltpu.VMEM((PEERS, PLANES, SLOTS), jnp.float32),
            pltpu.VMEM((PLANES, 1, SLOTS), jnp.float32),
            pltpu.VMEM((PLANES, 1, SLOTS), jnp.float32),
            dma((BLOCKS,)),
            dma((PLANES,)), dma((PLANES,)),
            dma((PLANES,)), dma((PLANES,)),
            dma((PLANES,)), dma((PLANES,)),
            dma, dma,
            dma, dma,
            dma((PLANES,)), dma((PLANES,)),
        ],
        compiler_params=pltpu.CompilerParams(
            collective_id=0, has_side_effects=True, vmem_limit_bytes=67043328
        ),
    )(embeddings, cluster_ids.reshape(BLOCKS, 128), ranks.reshape(BLOCKS, 128))
    return best.reshape(ROWS_DEV)


def solution(mesh):
    return jax.shard_map(
        shards,
        mesh=mesh,
        in_specs=(
            P(("loader", "split"), None),
            P(("loader", "split"), None),
            P(("loader", "split")),
        ),
        out_specs=P(("loader", "split")),
        check_vma=False,
    )
```

```python
import functools

import jax
import jax.numpy as jnp
from jax import lax
from jax.experimental import pallas as pl
from jax.experimental.pallas import tpu as pltpu
from jax.sharding import PartitionSpec as P

MESH = pl.DeviceIdType.MESH
CLUSTERS = 256
CAP = 4
WIDTH = 768
ROWS_DEV = 512
PLANES = 8
PEERS = 32
SLOTS = PEERS * CAP
BLOCKS = ROWS_DEV // 128
ROOM = 80
EMPTY = float(1 << 17)
GROUPS = ((0,), (1, 7), (2, 6), (3, 5), (4,))
epsilon = 1e-06


def place():
    row = lax.axis_index("loader")
    y = lax.axis_index("split")
    return lax.div(row, 8), y, lax.rem(lax.div(row, 2), 4), lax.rem(row, 2)


def device(z, y, x, c):
    return ((z * 4 + x) * 2 + c, y)


def across(here, s):
    z, y, x, c = here
    return device(lax.rem(z + s, PLANES), y, x, c)


def within(here, j, sign):
    z, y, x, c = here
    dy, dx, dc = lax.rem(j, 4), lax.rem(lax.div(j, 4), 4), lax.div(j, 16)
    return device(
        z,
        lax.rem(y + 4 + sign * dy, 4),
        lax.rem(x + 4 + sign * dx, 4),
        lax.rem(c + dc, 2),
    )


def send(src, dst, sent, landed, to):
    return pltpu.make_async_remote_copy(
        src_ref=src,
        dst_ref=dst,
        send_sem=sent,
        recv_sem=landed,
        device_id=to,
        device_id_type=MESH,
    )


def product(a, b):
    return lax.dot_general(
        a, b, (((1,), (1,)), ((), ())), preferred_element_type=jnp.float32
    )


def iota(shape, dim):
    return lax.broadcasted_iota(jnp.int32, shape, dim)


def own_lanes(tiles_ref):
    group = iota((PLANES, SLOTS), 1) // CAP
    total = jnp.zeros((PLANES, SLOTS), jnp.float32)
    for j in range(PEERS):
        total = jnp.where(group == j, tiles_ref[j], total)
    return total


def kernel(
    room, emb_hbm, cid_ref, rank_ref, out_ref, flag_ref,
    raw, unit, meta_out, meta_in, rows_out, rows_in, dense, arrived, members,
    ranks_out, ranks_in, best_out, best_in, back_out, back_in,
    raw_sem, meta_sent, meta_landed, rows_sent, rows_landed, dense_sent, dense_landed,
    ranks_sent, ranks_landed, best_sent, best_landed, back_sent, back_landed,
):
    here = place()
    z, y, x, c = here
    loads = [
        pltpu.make_async_copy(
            emb_hbm.at[pl.ds(b * 128, 128)], raw.at[pl.ds(b * 128, 128)], raw_sem.at[b]
        )
        for b in range(BLOCKS)
    ]
    for load in loads:
        load.start()
    barrier = pltpu.get_barrier_semaphore()

    def greet_across(s, carry):
        pl.semaphore_signal(barrier, inc=1, device_id=across(here, s), device_id_type=MESH)
        return carry

    def greet_within(j, carry):
        pl.semaphore_signal(barrier, inc=1, device_id=within(here, j, 1), device_id_type=MESH)
        return carry

    lax.fori_loop(1, PLANES, greet_across, 0)
    lax.fori_loop(1, PEERS, greet_within, 0)

    cid = cid_ref[...]
    owner = cid & (PEERS - 1)
    step = ((cid >> 5) - z) & (PLANES - 1)
    peer = (
        (((owner >> 4) - c) & 1) * 16 + (((owner >> 2) - x) & 3) * 4 + ((owner - y) & 3)
    )
    turned = jnp.concatenate([cid, step], axis=0).T
    before = iota((128, 128), 0) < iota((128, 128), 1)
    slot_rows, pack_rows, over = [], [], jnp.zeros((1, 128), jnp.float32)
    for b in range(BLOCKS):
        same = jnp.zeros((128, 128), jnp.float32)
        along = jnp.zeros((128, 128), jnp.float32)
        for a in range(b + 1):
            alike = turned[:, a : a + 1] == cid[b : b + 1]
            aside = turned[:, BLOCKS + a : BLOCKS + a + 1] == step[b : b + 1]
            if a == b:
                alike, aside = alike & before, aside & before
            same += jnp.where(alike, 1.0, 0.0)
            along += jnp.where(aside, 1.0, 0.0)
        position = jnp.sum(same, axis=0, keepdims=True).astype(jnp.int32)
        count = jnp.sum(along, axis=0, keepdims=True).astype(jnp.int32)
        steps = step[b : b + 1] * SLOTS
        slot_rows.append(steps + peer[b : b + 1] * CAP + position)
        pack_rows.append(jnp.where(count < room, steps + count, -1))
        over = jnp.maximum(over, jnp.where(count < room, 0.0, 2 * EMPTY))
    over = jnp.max(over, axis=1, keepdims=True)
    slot_turned = jnp.concatenate(slot_rows + pack_rows, axis=0).T
    rank_turned = (rank_ref[...].astype(jnp.float32) - EMPTY).T
    lane = iota((128, 128), 1)
    for s in range(PLANES):
        name = jnp.zeros((128, 128), jnp.float32)
        rank = jnp.zeros((128, 128), jnp.float32)
        for b in range(BLOCKS):
            slots = slot_turned[:, b : b + 1]
            packs = slot_turned[:, BLOCKS + b : BLOCKS + b + 1]
            name = jnp.where(packs == s * SLOTS + lane, (slots - (s * SLOTS - 1)).astype(jnp.float32), name)
            rank = jnp.where(slots == s * SLOTS + lane, rank_turned[:, b : b + 1], rank)
        ref = meta_in if s == 0 else meta_out
        ref[s, 0:1] = jnp.sum(name, axis=0, keepdims=True) - 1.0
        ref[s, 1:2] = jnp.sum(rank, axis=0, keepdims=True) + (EMPTY + over)
    for b in range(BLOCKS):
        loads[b].wait()
        values = raw[b * 128 : (b + 1) * 128].astype(jnp.float32)
        scale = lax.rsqrt(jnp.sum(values * values, axis=1, keepdims=True) + epsilon)
        unit[b * 128 : (b + 1) * 128] = (values * scale).astype(jnp.bfloat16)

    pl.semaphore_wait(barrier, PLANES - 1 + PEERS - 1)
    metas, rows = {}, {}
    order = [s for group in GROUPS for s in group if s]
    for s in order:
        metas[s] = send(meta_out.at[s], meta_in.at[s], meta_sent.at[s], meta_landed.at[s], across(here, s))
        metas[s].start()
    pack = jnp.concatenate(pack_rows, axis=1)
    for group in GROUPS[1:] + GROUPS[:1]:
        chosen = jnp.concatenate(
            [jnp.where(pack == s * SLOTS + iota((room, ROWS_DEV), 0), 1.0, 0.0) for s in group], axis=0
        ).astype(jnp.bfloat16)
        packed = jnp.dot(chosen, unit[...], preferred_element_type=jnp.float32).astype(jnp.bfloat16)
        for n, s in enumerate(group):
            ref = rows_in if s == 0 else rows_out
            ref[s] = packed[n * room : (n + 1) * room]
            if s:
                rows[s] = send(rows_out.at[s], rows_in.at[s], rows_sent.at[s], rows_landed.at[s], across(here, s))
                rows[s].start()

    def spread(s):
        chosen = jnp.where(
            meta_in[s, 0:1, :room] == iota((SLOTS, room), 0).astype(jnp.float32), 1.0, 0.0
        ).astype(jnp.bfloat16)
        placed = jnp.dot(chosen, rows_in[s], preferred_element_type=jnp.float32).astype(jnp.bfloat16)
        dense[s] = placed.reshape(PEERS, CAP, WIDTH)
        arrived[s, 0] = placed[:CAP]

        def deliver(j, carry):
            send(dense.at[s, j], arrived.at[s, j], dense_sent.at[s], dense_landed.at[s], within(here, j, 1)).start()
            return carry

        lax.fori_loop(1, PEERS, deliver, 0)

    for s in order:
        metas[s].wait_recv()
    for s in range(PLANES):
        ranks_out[s : s + 1] = meta_in[s, 1:2]
    ranks_in[0] = ranks_out[...]

    def deliver_ranks(j, carry):
        send(ranks_out, ranks_in.at[j], ranks_sent, ranks_landed, within(here, j, 1)).start()
        return carry

    lax.fori_loop(1, PEERS, deliver_ranks, 0)
    others = pl.ds(1, PEERS - 1)
    spread(0)

    best = [jnp.full((1, SLOTS), -1.0, jnp.float32)] * PLANES
    seen = []
    rank_row = rank_col = None
    for turn in range(1, len(GROUPS) + 1):
        if turn < len(GROUPS):
            for s in GROUPS[turn]:
                rows[s].wait_recv()
                spread(s)
        if turn == 1:
            send(ranks_in.at[others], ranks_in.at[others], ranks_sent, ranks_landed, within(here, 1, 1)).wait_recv()
            rank_row = own_lanes(ranks_in)
            rank_col = rank_row.T
            highest = jnp.full((PLANES, SLOTS), 0.0, jnp.float32)
            for j in range(PEERS):
                highest = jnp.maximum(highest, ranks_in[j])
            flag_ref[...] = jnp.full((PLANES, SLOTS), jnp.max(jnp.where(highest >= 2 * EMPTY, 1.0, 0.0)))
        group = GROUPS[turn - 1]
        known = len(seen)
        for s in group:
            send(dense.at[s, others], arrived.at[s, others], dense_sent.at[s], dense_landed.at[s], within(here, 1, 1)).wait_recv()
            members[len(seen) * SLOTS : (len(seen) + 1) * SLOTS] = arrived[s].reshape(SLOTS, WIDTH)
            seen.append(s)
        new = members[known * SLOTS : len(seen) * SLOTS]
        scores = product(members[: len(seen) * SLOTS], new)
        for n, q in enumerate(group):
            top = jnp.full((SLOTS, SLOTS), -1.0, jnp.float32)
            for k, m in enumerate(seen):
                part = scores[k * SLOTS : (k + 1) * SLOTS, n * SLOTS : (n + 1) * SLOTS]
                earlier = rank_col[:, m : m + 1] < rank_row[q : q + 1]
                top = jnp.maximum(top, jnp.where(earlier, part, -1.0))
            best[q] = jnp.maximum(best[q], jnp.max(top, axis=0, keepdims=True))
        if known:
            scores = product(new, members[: known * SLOTS])
            for k, q in enumerate(seen[:known]):
                top = jnp.full((SLOTS, SLOTS), -1.0, jnp.float32)
                for n, m in enumerate(group):
                    part = scores[n * SLOTS : (n + 1) * SLOTS, k * SLOTS : (k + 1) * SLOTS]
                    earlier = rank_col[:, m : m + 1] < rank_row[q : q + 1]
                    top = jnp.maximum(top, jnp.where(earlier, part, -1.0))
                best[q] = jnp.maximum(best[q], jnp.max(top, axis=0, keepdims=True))

    best_out[...] = jnp.concatenate(best, axis=0)

    def answer(j, carry):
        send(best_out, best_in.at[j], best_sent, best_landed, within(here, j, -1)).start()
        return carry

    lax.fori_loop(1, PEERS, answer, 0)
    best_in[0] = best_out[...]
    for s in order:
        metas[s].wait_send()
        rows[s].wait_send()
    for s in range(PLANES):
        send(dense.at[s, others], arrived.at[s, others], dense_sent.at[s], dense_landed.at[s], within(here, 1, 1)).wait_send()
    send(ranks_in.at[others], ranks_in.at[others], ranks_sent, ranks_landed, within(here, 1, 1)).wait_send()
    whole = send(best_in.at[others], best_in.at[others], best_sent, best_landed, within(here, 1, 1))
    whole.wait_recv()
    results = own_lanes(best_in)
    backs = []
    for s in range(PLANES):
        ref = back_in if s == 0 else back_out
        ref[s] = results[s : s + 1]
        if s:
            back = send(back_out.at[s], back_in.at[s], back_sent.at[s], back_landed.at[s], across(here, PLANES - s))
            back.start()
            backs.append(back)
    whole.wait_send()
    for back in backs:
        back.wait()
    result_col = jnp.concatenate([back_in[s] for s in range(PLANES)], axis=0).T
    slot = iota((SLOTS, 128), 0)
    for b in range(BLOCKS):
        found = jnp.zeros((SLOTS, 128), jnp.float32)
        for s in range(PLANES):
            found = jnp.where(slot_rows[b] == s * SLOTS + slot, result_col[:, s : s + 1], found)
        out_ref[b : b + 1] = jnp.sum(found, axis=0, keepdims=True)


def exchange(room, number, embeddings, cluster_ids, ranks):
    dma = pltpu.SemaphoreType.DMA
    return pl.pallas_call(
        functools.partial(kernel, room),
        out_shape=(
            jax.ShapeDtypeStruct((BLOCKS, 128), jnp.float32),
            jax.ShapeDtypeStruct((PLANES, SLOTS), jnp.float32),
        ),
        in_specs=[
            pl.BlockSpec(memory_space=pl.ANY),
            pl.BlockSpec(memory_space=pltpu.VMEM),
            pl.BlockSpec(memory_space=pltpu.VMEM),
        ],
        out_specs=(pl.BlockSpec(memory_space=pltpu.VMEM),) * 2,
        scratch_shapes=[
            pltpu.VMEM((ROWS_DEV, WIDTH), jnp.bfloat16),
            pltpu.VMEM((ROWS_DEV, WIDTH), jnp.bfloat16),
            pltpu.VMEM((PLANES, 2, SLOTS), jnp.float32),
            pltpu.VMEM((PLANES, 2, SLOTS), jnp.float32),
            pltpu.VMEM((PLANES, room, WIDTH), jnp.bfloat16),
            pltpu.VMEM((PLANES, room, WIDTH), jnp.bfloat16),
            pltpu.VMEM((PLANES, PEERS, CAP, WIDTH), jnp.bfloat16),
            pltpu.VMEM((PLANES, PEERS, CAP, WIDTH), jnp.bfloat16),
            pltpu.VMEM((PLANES * SLOTS, WIDTH), jnp.bfloat16),
            pltpu.VMEM((PLANES, SLOTS), jnp.float32),
            pltpu.VMEM((PEERS, PLANES, SLOTS), jnp.float32),
            pltpu.VMEM((PLANES, SLOTS), jnp.float32),
            pltpu.VMEM((PEERS, PLANES, SLOTS), jnp.float32),
            pltpu.VMEM((PLANES, 1, SLOTS), jnp.float32),
            pltpu.VMEM((PLANES, 1, SLOTS), jnp.float32),
            dma((BLOCKS,)),
            dma((PLANES,)), dma((PLANES,)),
            dma((PLANES,)), dma((PLANES,)),
            dma((PLANES,)), dma((PLANES,)),
            dma, dma,
            dma, dma,
            dma((PLANES,)), dma((PLANES,)),
        ],
        compiler_params=pltpu.CompilerParams(
            collective_id=number, has_side_effects=True, vmem_limit_bytes=67043328
        ),
    )(embeddings, cluster_ids, ranks)


def shards(embeddings, cluster_ids, ranks):
    given = embeddings, cluster_ids.reshape(BLOCKS, 128), ranks.reshape(BLOCKS, 128)
    nearest, over = exchange(ROOM, 0, *given)
    nearest = lax.cond(over[0, 0] > 0, lambda best: exchange(SLOTS, 1, *given)[0], lambda best: best, nearest)
    return nearest.reshape(ROWS_DEV)


def solution(mesh):
    return jax.shard_map(
        shards,
        mesh=mesh,
        in_specs=(
            P(("loader", "split"), None),
            P(("loader", "split"), None),
            P(("loader", "split")),
        ),
        out_specs=P(("loader", "split")),
        check_vma=False,
    )
```

```python
import functools

import jax
import jax.numpy as jnp
from jax import lax
from jax.experimental import pallas as pl
from jax.experimental.pallas import tpu as pltpu
from jax.sharding import PartitionSpec as P

MESH = pl.DeviceIdType.MESH
CLUSTERS = 256
CAP = 4
WIDTH = 768
ROWS_DEV = 512
PLANES = 8
PEERS = 32
SLOTS = PEERS * CAP
BLOCKS = ROWS_DEV // 128
ROOM = 80
EMPTY = float(1 << 17)
GROUPS = ((0,), (1, 7), (2, 6), (3, 5), (4,))
ORDER = (1, 7, 2, 6, 3, 5, 4)
epsilon = 1e-06


def place():
    row = lax.axis_index("loader")
    y = lax.axis_index("split")
    return lax.div(row, 8), y, lax.rem(lax.div(row, 2), 4), lax.rem(row, 2)


def device(z, y, x, c):
    return ((z * 4 + x) * 2 + c, y)


def across(here, s):
    z, y, x, c = here
    return device(lax.rem(z + s, PLANES), y, x, c)


def within(here, j, sign):
    z, y, x, c = here
    dy, dx, dc = j % 4, j // 4 % 4, j // 16
    return device(
        z,
        lax.rem(y + (4 + sign * dy) % 4, 4),
        lax.rem(x + (4 + sign * dx) % 4, 4),
        lax.rem(c + dc, 2),
    )


def hops(j):
    return min(j % 4, 4 - j % 4) + min(j // 4 % 4, 4 - j // 4 % 4)


FAR_FIRST = sorted(range(1, PEERS), key=lambda j: -hops(j))


def send(src, dst, sent, landed, to):
    return pltpu.make_async_remote_copy(
        src_ref=src,
        dst_ref=dst,
        send_sem=sent,
        recv_sem=landed,
        device_id=to,
        device_id_type=MESH,
    )


def product(a, b):
    return lax.dot_general(
        a, b, (((1,), (1,)), ((), ())), preferred_element_type=jnp.float32
    )


def iota(shape, dim):
    return lax.broadcasted_iota(jnp.int32, shape, dim)


def own_lanes(tiles_ref):
    group = iota((PLANES, SLOTS), 1) // CAP
    total = jnp.zeros((PLANES, SLOTS), jnp.float32)
    for j in range(PEERS):
        total = jnp.where(group == j, tiles_ref[j], total)
    return total


def kernel(
    room, emb_hbm, cid_hbm, rank_hbm, out_ref, flag_ref,
    raw, cid_ref, rank_ref, unit, meta_out, meta_in, rows_out, rows_in, dense, arrived, members,
    ranks_out, ranks_in, best_out, best_in, back_out, back_in,
    raw_sem, meta_sent, meta_landed, rows_sent, rows_landed, dense_sent, dense_landed,
    ranks_sent, ranks_landed, best_sent, best_landed, back_sent, back_landed,
):
    here = place()
    z, y, x, c = here
    load_cid = pltpu.make_async_copy(cid_hbm, cid_ref, raw_sem.at[BLOCKS])
    load_cid.start()
    loads = [
        pltpu.make_async_copy(
            emb_hbm.at[pl.ds(b * 128, 128)], raw.at[pl.ds(b * 128, 128)], raw_sem.at[b]
        )
        for b in range(BLOCKS)
    ]
    for load in loads:
        load.start()
    load_rank = pltpu.make_async_copy(rank_hbm, rank_ref, raw_sem.at[BLOCKS + 1])
    load_rank.start()
    barrier = pltpu.get_barrier_semaphore()
    for s in (4, 3, 5, 2, 6, 1, 7):
        pl.semaphore_signal(barrier, inc=1, device_id=across(here, s), device_id_type=MESH)
    for j in FAR_FIRST:
        pl.semaphore_signal(barrier, inc=1, device_id=within(here, j, 1), device_id_type=MESH)

    load_cid.wait()
    cid = cid_ref[...]
    owner = cid & (PEERS - 1)
    step = ((cid >> 5) - z) & (PLANES - 1)
    turned = jnp.concatenate([cid, step], axis=0).T
    before = iota((128, 128), 0) < iota((128, 128), 1)
    pack_rows, over = [], jnp.zeros((1, 128), jnp.float32)
    for b in range(BLOCKS):
        along = jnp.zeros((128, 128), jnp.float32)
        for a in range(b + 1):
            aside = turned[:, BLOCKS + a : BLOCKS + a + 1] == step[b : b + 1]
            along += jnp.where(aside & before if a == b else aside, 1.0, 0.0)
        count = jnp.sum(along, axis=0, keepdims=True).astype(jnp.int32)
        pack_rows.append(jnp.where(count < room, step[b : b + 1] * SLOTS + count, -1))
        over = jnp.maximum(over, jnp.where(count < room, 0.0, 2 * EMPTY))
    pack = jnp.concatenate(pack_rows, axis=1)
    for b in range(BLOCKS):
        loads[b].wait()
        values = raw[b * 128 : (b + 1) * 128].astype(jnp.float32)
        scale = lax.rsqrt(jnp.sum(values * values, axis=1, keepdims=True) + epsilon)
        unit[b * 128 : (b + 1) * 128] = (values * scale).astype(jnp.bfloat16)

    rows = {
        s: send(rows_out.at[s], rows_in.at[s], rows_sent.at[s], rows_landed.at[s], across(here, s))
        for s in range(1, PLANES)
    }
    metas = {
        s: send(meta_out.at[s], meta_in.at[s], meta_sent.at[s], meta_landed.at[s], across(here, s))
        for s in range(1, PLANES)
    }

    def gather_rows(group):
        chosen = jnp.concatenate(
            [jnp.where(pack == s * SLOTS + iota((room, ROWS_DEV), 0), 1.0, 0.0) for s in group], axis=0
        ).astype(jnp.bfloat16)
        packed = jnp.dot(chosen, unit[...], preferred_element_type=jnp.float32).astype(jnp.bfloat16)
        for n, s in enumerate(group):
            ref = rows_in if s == 0 else rows_out
            ref[s] = packed[n * room : (n + 1) * room]

    gather_rows((1, 7))
    pl.semaphore_wait(barrier, PLANES - 1 + PEERS - 1)
    rows[1].start()
    rows[7].start()

    peer = (
        (((owner >> 4) - c) & 1) * 16 + (((owner >> 2) - x) & 3) * 4 + ((owner - y) & 3)
    )
    slot_rows = []
    for b in range(BLOCKS):
        same = jnp.zeros((128, 128), jnp.float32)
        for a in range(b + 1):
            alike = turned[:, a : a + 1] == cid[b : b + 1]
            same += jnp.where(alike & before if a == b else alike, 1.0, 0.0)
        position = jnp.sum(same, axis=0, keepdims=True).astype(jnp.int32)
        slot_rows.append(step[b : b + 1] * SLOTS + peer[b : b + 1] * CAP + position)
    over = jnp.max(over, axis=1, keepdims=True)
    slot_turned = jnp.concatenate(slot_rows + pack_rows, axis=0).T
    load_rank.wait()
    rank_turned = (rank_ref[...].astype(jnp.float32) - EMPTY).T
    lane = iota((128, 128), 1)
    for s in range(PLANES):
        name = jnp.zeros((128, 128), jnp.float32)
        rank = jnp.zeros((128, 128), jnp.float32)
        for b in range(BLOCKS):
            slots = slot_turned[:, b : b + 1]
            packs = slot_turned[:, BLOCKS + b : BLOCKS + b + 1]
            name = jnp.where(packs == s * SLOTS + lane, (slots - (s * SLOTS - 1)).astype(jnp.float32), name)
            rank = jnp.where(slots == s * SLOTS + lane, rank_turned[:, b : b + 1], rank)
        ref = meta_in if s == 0 else meta_out
        ref[s, 0:1] = jnp.sum(name, axis=0, keepdims=True) - 1.0
        ref[s, 1:2] = jnp.sum(rank, axis=0, keepdims=True) + (EMPTY + over)
    for s in ORDER:
        metas[s].start()
    for group in ((2, 6), (3, 5), (4, 0)):
        gather_rows(group)
        for s in group:
            if s:
                rows[s].start()

    others = pl.ds(1, PEERS - 1)

    def spread(s):
        chosen = jnp.where(
            meta_in[s, 0:1, :room] == iota((SLOTS, room), 0).astype(jnp.float32), 1.0, 0.0
        ).astype(jnp.bfloat16)
        placed = jnp.dot(chosen, rows_in[s], preferred_element_type=jnp.float32).astype(jnp.bfloat16)
        dense[s] = placed.reshape(PEERS, CAP, WIDTH)
        arrived[s, 0] = placed[:CAP]
        for j in FAR_FIRST:
            send(dense.at[s, j], arrived.at[s, j], dense_sent.at[s], dense_landed.at[s], within(here, j, 1)).start()

    def all_dense(s):
        return send(dense.at[s, others], arrived.at[s, others], dense_sent.at[s], dense_landed.at[s], within(here, 1, 1))

    all_ranks = send(ranks_in.at[others], ranks_in.at[others], ranks_sent, ranks_landed, within(here, 1, 1))
    all_best = send(best_in.at[others], best_in.at[others], best_sent, best_landed, within(here, 1, 1))

    spread(0)
    for s in ORDER:
        metas[s].wait_recv()
    for s in range(PLANES):
        ranks_out[s : s + 1] = meta_in[s, 1:2]
    ranks_in[0] = ranks_out[...]
    for j in FAR_FIRST:
        send(ranks_out, ranks_in.at[j], ranks_sent, ranks_landed, within(here, j, 1)).start()
    for s in GROUPS[1]:
        rows[s].wait_recv()
        spread(s)

    all_ranks.wait_recv()
    rank_row = own_lanes(ranks_in)
    rank_col = rank_row.T
    highest = jnp.zeros((PLANES, SLOTS), jnp.float32)
    for j in range(PEERS):
        highest = jnp.maximum(highest, ranks_in[j])
    flag_ref[0] = jnp.max(jnp.where(highest >= 2 * EMPTY, 1, 0))

    best = [jnp.full((1, SLOTS), -1.0, jnp.float32)] * PLANES
    seen = []

    def compare(group):
        known = len(seen)
        for s in group:
            all_dense(s).wait_recv()
            members[len(seen) * SLOTS : (len(seen) + 1) * SLOTS] = arrived[s].reshape(SLOTS, WIDTH)
            seen.append(s)
        scores = product(members[known * SLOTS : len(seen) * SLOTS], members[: len(seen) * SLOTS])

        def part(n, k):
            return scores[n * SLOTS : (n + 1) * SLOTS, k * SLOTS : (k + 1) * SLOTS]

        for k, q in enumerate(seen):
            top = jnp.full((SLOTS, SLOTS), -1.0, jnp.float32)
            for n, m in enumerate(group):
                earlier = rank_col[:, m : m + 1] < rank_row[q : q + 1]
                top = jnp.maximum(top, jnp.where(earlier, part(n, k), -1.0))
            best[q] = jnp.maximum(best[q], jnp.max(top, axis=0, keepdims=True))
        for n, q in enumerate(group):
            if known:
                top = jnp.full((SLOTS, SLOTS), -1.0, jnp.float32)
                for k, m in enumerate(seen[:known]):
                    earlier = rank_row[m : m + 1] < rank_col[:, q : q + 1]
                    top = jnp.maximum(top, jnp.where(earlier, part(n, k), -1.0))
                best[q] = jnp.maximum(best[q], jnp.max(top.T, axis=0, keepdims=True))

    compare(GROUPS[0])
    for s in GROUPS[2]:
        rows[s].wait_recv()
        spread(s)
    compare(GROUPS[1])
    for s in GROUPS[3] + GROUPS[4]:
        rows[s].wait_recv()
        spread(s)
    for group in GROUPS[2:]:
        compare(group)

    best_out[...] = jnp.concatenate(best, axis=0)
    for j in FAR_FIRST:
        send(best_out, best_in.at[j], best_sent, best_landed, within(here, j, -1)).start()
    best_in[0] = best_out[...]
    for s in ORDER:
        metas[s].wait_send()
        rows[s].wait_send()
    for s in range(PLANES):
        all_dense(s).wait_send()
    all_ranks.wait_send()
    all_best.wait_recv()
    results = own_lanes(best_in)
    backs = []
    for s in (4, 3, 5, 2, 6, 1, 7):
        back_out[s] = results[s : s + 1]
        back = send(back_out.at[s], back_in.at[s], back_sent.at[s], back_landed.at[s], across(here, PLANES - s))
        back.start()
        backs.append(back)
    back_in[0] = results[0:1]
    all_best.wait_send()
    for back in backs:
        back.wait()
    result_col = jnp.concatenate([back_in[s] for s in range(PLANES)], axis=0).T
    slot = iota((SLOTS, 128), 0)
    for b in range(BLOCKS):
        found = jnp.zeros((SLOTS, 128), jnp.float32)
        for s in range(PLANES):
            found = jnp.where(slot_rows[b] == s * SLOTS + slot, result_col[:, s : s + 1], found)
        out_ref[b : b + 1] = jnp.sum(found, axis=0, keepdims=True)


def exchange(room, number, vmem, embeddings, cluster_ids, ranks):
    dma = pltpu.SemaphoreType.DMA
    return pl.pallas_call(
        functools.partial(kernel, room),
        out_shape=(
            jax.ShapeDtypeStruct((BLOCKS, 128), jnp.float32),
            jax.ShapeDtypeStruct((1,), jnp.int32),
        ),
        in_specs=[
            pl.BlockSpec(memory_space=pltpu.HBM),
            pl.BlockSpec(memory_space=pltpu.HBM),
            pl.BlockSpec(memory_space=pltpu.HBM),
        ],
        out_specs=(pl.BlockSpec(memory_space=pltpu.VMEM), pl.BlockSpec(memory_space=pltpu.SMEM)),
        scratch_shapes=[
            pltpu.VMEM((ROWS_DEV, WIDTH), jnp.bfloat16),
            pltpu.VMEM((BLOCKS, 128), jnp.int32),
            pltpu.VMEM((BLOCKS, 128), jnp.int32),
            pltpu.VMEM((ROWS_DEV, WIDTH), jnp.bfloat16),
            pltpu.VMEM((PLANES, 2, SLOTS), jnp.float32),
            pltpu.VMEM((PLANES, 2, SLOTS), jnp.float32),
            pltpu.VMEM((PLANES, room, WIDTH), jnp.bfloat16),
            pltpu.VMEM((PLANES, room, WIDTH), jnp.bfloat16),
            pltpu.VMEM((PLANES, PEERS, CAP, WIDTH), jnp.bfloat16),
            pltpu.VMEM((PLANES, PEERS, CAP, WIDTH), jnp.bfloat16),
            pltpu.VMEM((PLANES * SLOTS, WIDTH), jnp.bfloat16),
            pltpu.VMEM((PLANES, SLOTS), jnp.float32),
            pltpu.VMEM((PEERS, PLANES, SLOTS), jnp.float32),
            pltpu.VMEM((PLANES, SLOTS), jnp.float32),
            pltpu.VMEM((PEERS, PLANES, SLOTS), jnp.float32),
            pltpu.VMEM((PLANES, 1, SLOTS), jnp.float32),
            pltpu.VMEM((PLANES, 1, SLOTS), jnp.float32),
            dma((BLOCKS + 2,)),
            dma((PLANES,)), dma((PLANES,)),
            dma((PLANES,)), dma((PLANES,)),
            dma((PLANES,)), dma((PLANES,)),
            dma, dma,
            dma, dma,
            dma((PLANES,)), dma((PLANES,)),
        ],
        compiler_params=pltpu.CompilerParams(
            collective_id=number, has_side_effects=True, vmem_limit_bytes=vmem
        ),
    )(embeddings, cluster_ids, ranks)


def shards(embeddings, cluster_ids, ranks):
    given = embeddings, cluster_ids.reshape(BLOCKS, 128), ranks.reshape(BLOCKS, 128)
    nearest, over = exchange(ROOM, 0, 40 << 20, *given)
    nearest = lax.cond(over[0] > 0, lambda best: exchange(SLOTS, 1, 67043328, *given)[0], lambda best: best, nearest)
    return nearest.reshape(ROWS_DEV)


def solution(mesh):
    return jax.shard_map(
        shards,
        mesh=mesh,
        in_specs=(
            P(("loader", "split"), None),
            P(("loader", "split"), None),
            P(("loader", "split")),
        ),
        out_specs=P(("loader", "split")),
        check_vma=False,
    )
```

```python
import functools

import jax
import jax.numpy as jnp
from jax import lax
from jax.experimental import pallas as pl
from jax.experimental.pallas import tpu as pltpu
from jax.sharding import PartitionSpec as P

MESH = pl.DeviceIdType.MESH
scope = jax.named_scope
CLUSTERS = 256
CAP = 4
WIDTH = 768
ROWS_DEV = 512
PLANES = 8
PEERS = 32
SLOTS = PEERS * CAP
BLOCKS = ROWS_DEV // 128
ROOM = 80
EMPTY = float(1 << 17)
GROUPS = ((0,), (1, 7), (2, 6), (3, 5), (4,))
ORDER = sum(GROUPS[1:], ())
epsilon = 1e-06


def place():
    row = lax.axis_index("loader")
    y = lax.axis_index("split")
    return lax.div(row, 8), y, lax.rem(lax.div(row, 2), 4), lax.rem(row, 2)


def device(z, y, x, c):
    return ((z * 4 + x) * 2 + c, y)


def across(here, s):
    z, y, x, c = here
    return device(lax.rem(z + s, PLANES), y, x, c)


def within(here, j, sign):
    z, y, x, c = here
    dy, dx, dc = j % 4, j // 4 % 4, j // 16
    return device(
        z,
        lax.rem(y + (4 + sign * dy) % 4, 4),
        lax.rem(x + (4 + sign * dx) % 4, 4),
        lax.rem(c + dc, 2),
    )


def hops(j):
    return min(j % 4, 4 - j % 4) + min(j // 4 % 4, 4 - j // 4 % 4)


FAR_FIRST = sorted(range(1, PEERS), key=lambda j: -hops(j))


def send(src, dst, sent, landed, to):
    return pltpu.make_async_remote_copy(
        src_ref=src,
        dst_ref=dst,
        send_sem=sent,
        recv_sem=landed,
        device_id=to,
        device_id_type=MESH,
    )


def product(a, b):
    return lax.dot_general(
        a, b, (((1,), (1,)), ((), ())), preferred_element_type=jnp.float32
    )


def iota(shape, dim):
    return lax.broadcasted_iota(jnp.int32, shape, dim)


def own_lanes(tiles_ref):
    group = iota((PLANES, SLOTS), 1) // CAP
    total = jnp.zeros((PLANES, SLOTS), jnp.float32)
    for j in range(PEERS):
        total = jnp.where(group == j, tiles_ref[j], total)
    return total


def kernel(
    room, emb_hbm, cid_hbm, rank_hbm, out_ref, flag_ref,
    raw, cid_ref, rank_ref, unit, meta_out, meta_in, rows_out, rows_in, dense, arrived, members,
    ranks_out, ranks_in, best_out, best_in, back_out, back_in,
    raw_sem, meta_sent, meta_landed, rows_sent, rows_landed, dense_sent, dense_landed,
    ranks_sent, ranks_landed, best_sent, best_landed, back_sent, back_landed,
):
    here = place()
    z, y, x, c = here
    load_cid = pltpu.make_async_copy(cid_hbm, cid_ref, raw_sem.at[BLOCKS])
    load_cid.start()
    loads = [
        pltpu.make_async_copy(
            emb_hbm.at[pl.ds(b * 128, 128)], raw.at[pl.ds(b * 128, 128)], raw_sem.at[b]
        )
        for b in range(BLOCKS)
    ]
    for load in loads:
        load.start()
    load_rank = pltpu.make_async_copy(rank_hbm, rank_ref, raw_sem.at[BLOCKS + 1])
    load_rank.start()
    with scope("greet"):
        barrier = pltpu.get_barrier_semaphore()
        for s in (4, 3, 5, 2, 6, 1, 7):
            pl.semaphore_signal(barrier, inc=1, device_id=across(here, s), device_id_type=MESH)
        for j in FAR_FIRST:
            pl.semaphore_signal(barrier, inc=1, device_id=within(here, j, 1), device_id_type=MESH)

    with scope("count"):
        load_cid.wait()
        cid = cid_ref[...]
        owner = cid & (PEERS - 1)
        step = ((cid >> 5) - z) & (PLANES - 1)
        turned = jnp.concatenate([cid, step], axis=0).T
        before = iota((128, 128), 0) < iota((128, 128), 1)
        pack_rows, over = [], jnp.zeros((1, 128), jnp.float32)
        for b in range(BLOCKS):
            along = jnp.zeros((128, 128), jnp.float32)
            for a in range(b + 1):
                aside = turned[:, BLOCKS + a : BLOCKS + a + 1] == step[b : b + 1]
                along += jnp.where(aside & before if a == b else aside, 1.0, 0.0)
            count = jnp.sum(along, axis=0, keepdims=True).astype(jnp.int32)
            pack_rows.append(jnp.where(count < room, step[b : b + 1] * SLOTS + count, -1))
            over = jnp.maximum(over, jnp.where(count < room, 0.0, 2 * EMPTY))
        pack = jnp.concatenate(pack_rows, axis=1)
    with scope("norm"):
        for b in range(BLOCKS):
            loads[b].wait()
            values = raw[b * 128 : (b + 1) * 128].astype(jnp.float32)
            scale = lax.rsqrt(jnp.sum(values * values, axis=1, keepdims=True) + epsilon)
            unit[b * 128 : (b + 1) * 128] = (values * scale).astype(jnp.bfloat16)

    rows = {
        s: send(rows_out.at[s], rows_in.at[s], rows_sent.at[s], rows_landed.at[s], across(here, s))
        for s in range(1, PLANES)
    }
    metas = {
        s: send(meta_out.at[s], meta_in.at[s], meta_sent.at[s], meta_landed.at[s], across(here, s))
        for s in range(1, PLANES)
    }

    def gather_rows(group):
        chosen = jnp.concatenate(
            [jnp.where(pack == s * SLOTS + iota((room, ROWS_DEV), 0), 1.0, 0.0) for s in group], axis=0
        ).astype(jnp.bfloat16)
        packed = jnp.dot(chosen, unit[...], preferred_element_type=jnp.float32).astype(jnp.bfloat16)
        for n, s in enumerate(group):
            ref = rows_in if s == 0 else rows_out
            ref[s] = packed[n * room : (n + 1) * room]

    with scope("pack"):
        gather_rows(GROUPS[1])
    with scope("barrier_wait"):
        pl.semaphore_wait(barrier, PLANES - 1 + PEERS - 1)
    for s in GROUPS[1]:
        rows[s].start()

    with scope("slots"):
        peer = (
            (((owner >> 4) - c) & 1) * 16 + (((owner >> 2) - x) & 3) * 4 + ((owner - y) & 3)
        )
        slot_rows = []
        for b in range(BLOCKS):
            same = jnp.zeros((128, 128), jnp.float32)
            for a in range(b + 1):
                alike = turned[:, a : a + 1] == cid[b : b + 1]
                same += jnp.where(alike & before if a == b else alike, 1.0, 0.0)
            position = jnp.sum(same, axis=0, keepdims=True).astype(jnp.int32)
            slot_rows.append(step[b : b + 1] * SLOTS + peer[b : b + 1] * CAP + position)
        over = jnp.max(over, axis=1, keepdims=True)
        slot_turned = jnp.concatenate(slot_rows + pack_rows, axis=0).T
        load_rank.wait()
        rank_turned = (rank_ref[...].astype(jnp.float32) - EMPTY).T
        lane = iota((128, 128), 1)
        for s in range(PLANES):
            name = jnp.zeros((128, 128), jnp.float32)
            rank = jnp.zeros((128, 128), jnp.float32)
            for b in range(BLOCKS):
                slots = slot_turned[:, b : b + 1]
                packs = slot_turned[:, BLOCKS + b : BLOCKS + b + 1]
                name = jnp.where(packs == s * SLOTS + lane, (slots - (s * SLOTS - 1)).astype(jnp.float32), name)
                rank = jnp.where(slots == s * SLOTS + lane, rank_turned[:, b : b + 1], rank)
            ref = meta_in if s == 0 else meta_out
            ref[s, 0:1] = jnp.sum(name, axis=0, keepdims=True) - 1.0
            ref[s, 1:2] = jnp.sum(rank, axis=0, keepdims=True) + (EMPTY + over)
    for s in ORDER:
        metas[s].start()
    with scope("pack_rest"):
        for group in GROUPS[2:] + GROUPS[:1]:
            gather_rows(group)
            for s in group:
                if s:
                    rows[s].start()

    others = pl.ds(1, PEERS - 1)

    def spread(s):
        with scope(f"place#s={s}"):
            chosen = jnp.where(
                meta_in[s, 0:1, :room] == iota((SLOTS, room), 0).astype(jnp.float32), 1.0, 0.0
            ).astype(jnp.bfloat16)
            placed = jnp.dot(chosen, rows_in[s], preferred_element_type=jnp.float32).astype(jnp.bfloat16)
            dense[s] = placed.reshape(PEERS, CAP, WIDTH)
            arrived[s, 0] = placed[:CAP]
        with scope(f"deliver#s={s}"):
            for j in FAR_FIRST:
                send(dense.at[s, j], arrived.at[s, j], dense_sent.at[s], dense_landed.at[s], within(here, j, 1)).start()

    def all_dense(s):
        return send(dense.at[s, others], arrived.at[s, others], dense_sent.at[s], dense_landed.at[s], within(here, 1, 1))

    all_ranks = send(ranks_in.at[others], ranks_in.at[others], ranks_sent, ranks_landed, within(here, 1, 1))
    all_best = send(best_in.at[others], best_in.at[others], best_sent, best_landed, within(here, 1, 1))

    spread(0)
    for s in GROUPS[1]:
        with scope(f"rows_wait#s={s}"):
            metas[s].wait_recv()
            rows[s].wait_recv()
        spread(s)
    with scope("meta_wait"):
        for s in ORDER[len(GROUPS[1]) :]:
            metas[s].wait_recv()
    for s in range(PLANES):
        ranks_out[s : s + 1] = meta_in[s, 1:2]
    ranks_in[0] = ranks_out[...]
    for j in FAR_FIRST:
        send(ranks_out, ranks_in.at[j], ranks_sent, ranks_landed, within(here, j, 1)).start()

    for s in GROUPS[2]:
        with scope(f"rows_wait#s={s}"):
            rows[s].wait_recv()
        spread(s)
    with scope("ranks_wait"):
        all_ranks.wait_recv()
    rank_row = own_lanes(ranks_in)
    rank_col = rank_row.T
    highest = jnp.zeros((PLANES, SLOTS), jnp.float32)
    for j in range(PEERS):
        highest = jnp.maximum(highest, ranks_in[j])
    flag_ref[0] = jnp.max(jnp.where(highest >= 2 * EMPTY, 1, 0))

    best = [jnp.full((1, SLOTS), -1.0, jnp.float32)] * PLANES
    seen = []

    def compare(group):
        known = len(seen)
        for s in group:
            with scope(f"dense_wait#s={s}"):
                all_dense(s).wait_recv()
            members[len(seen) * SLOTS : (len(seen) + 1) * SLOTS] = arrived[s].reshape(SLOTS, WIDTH)
            seen.append(s)
        with scope(f"scores#n={len(seen)}"):
            scores = product(members[known * SLOTS : len(seen) * SLOTS], members[: len(seen) * SLOTS])

            def part(n, k):
                return scores[n * SLOTS : (n + 1) * SLOTS, k * SLOTS : (k + 1) * SLOTS]

            for k, q in enumerate(seen):
                top = jnp.full((SLOTS, SLOTS), -1.0, jnp.float32)
                for n, m in enumerate(group):
                    earlier = rank_col[:, m : m + 1] < rank_row[q : q + 1]
                    top = jnp.maximum(top, jnp.where(earlier, part(n, k), -1.0))
                best[q] = jnp.maximum(best[q], jnp.max(top, axis=0, keepdims=True))
            for n, q in enumerate(group):
                if known:
                    top = jnp.full((SLOTS, SLOTS), -1.0, jnp.float32)
                    for k, m in enumerate(seen[:known]):
                        earlier = rank_row[m : m + 1] < rank_col[:, q : q + 1]
                        top = jnp.maximum(top, jnp.where(earlier, part(n, k), -1.0))
                    best[q] = jnp.maximum(best[q], jnp.max(top.T, axis=0, keepdims=True))

    compare(GROUPS[0])
    compare(GROUPS[1])
    for s in GROUPS[3] + GROUPS[4]:
        with scope(f"rows_wait#s={s}"):
            rows[s].wait_recv()
        spread(s)
    compare(GROUPS[2])
    for s in GROUPS[3] + GROUPS[4]:
        compare((s,))

    lanes, peers = iota((PEERS, SLOTS), 1), iota((PEERS, SLOTS), 0)
    with scope("answer"):
        answers = jnp.zeros((PEERS, SLOTS), jnp.float32)
        for s in range(PLANES):
            line = jnp.broadcast_to(best[s], (PEERS, SLOTS))
            picked = jnp.take_along_axis(line, CAP * peers + (lanes & (CAP - 1)), axis=1)
            answers = jnp.where(lanes // CAP == s, picked, answers)
        best_out[...] = answers.reshape(PEERS, 1, SLOTS)
        for j in FAR_FIRST:
            send(best_out.at[j], best_in.at[j], best_sent, best_landed, within(here, j, -1)).start()
    best_in[0] = best_out[0]
    for s in ORDER:
        metas[s].wait_send()
        rows[s].wait_send()
    for s in range(PLANES):
        all_dense(s).wait_send()
    all_ranks.wait_send()
    with scope("best_wait"):
        all_best.wait_recv()
    with scope("back"):
        answers = best_in[...].reshape(PEERS, SLOTS)
        backs = []
        for s in (4, 3, 5, 2, 6, 1, 7, 0):
            picked = jnp.take_along_axis(answers, CAP * s + (lanes & (CAP - 1)), axis=1)
            line = jnp.sum(jnp.where(lanes // CAP == peers, picked, 0.0), axis=0, keepdims=True)
            if s == 0:
                back_in[0] = line
                continue
            back_out[s] = line
            back = send(back_out.at[s], back_in.at[s], back_sent.at[s], back_landed.at[s], across(here, PLANES - s))
            back.start()
            backs.append(back)
    all_best.wait_send()
    with scope("back_wait"):
        for back in backs:
            back.wait()
    with scope("final"):
        slot = jnp.concatenate(slot_rows * 2, axis=0)
        found = jnp.zeros((2 * BLOCKS, 128), jnp.float32)
        for s in range(PLANES):
            row = jnp.broadcast_to(back_in[s], (2 * BLOCKS, SLOTS))
            picked = jnp.take_along_axis(row, slot & (SLOTS - 1), axis=1)
            found = jnp.where(slot >> 7 == s, picked, found)
        out_ref[...] = found[:BLOCKS]


def exchange(room, number, vmem, embeddings, cluster_ids, ranks):
    dma = pltpu.SemaphoreType.DMA
    return pl.pallas_call(
        functools.partial(kernel, room),
        out_shape=(
            jax.ShapeDtypeStruct((BLOCKS, 128), jnp.float32),
            jax.ShapeDtypeStruct((1,), jnp.int32),
        ),
        in_specs=[
            pl.BlockSpec(memory_space=pltpu.HBM),
            pl.BlockSpec(memory_space=pltpu.HBM),
            pl.BlockSpec(memory_space=pltpu.HBM),
        ],
        out_specs=(pl.BlockSpec(memory_space=pltpu.VMEM), pl.BlockSpec(memory_space=pltpu.SMEM)),
        scratch_shapes=[
            pltpu.VMEM((ROWS_DEV, WIDTH), jnp.bfloat16),
            pltpu.VMEM((BLOCKS, 128), jnp.int32),
            pltpu.VMEM((BLOCKS, 128), jnp.int32),
            pltpu.VMEM((ROWS_DEV, WIDTH), jnp.bfloat16),
            pltpu.VMEM((PLANES, 2, SLOTS), jnp.float32),
            pltpu.VMEM((PLANES, 2, SLOTS), jnp.float32),
            pltpu.VMEM((PLANES, room, WIDTH), jnp.bfloat16),
            pltpu.VMEM((PLANES, room, WIDTH), jnp.bfloat16),
            pltpu.VMEM((PLANES, PEERS, CAP, WIDTH), jnp.bfloat16),
            pltpu.VMEM((PLANES, PEERS, CAP, WIDTH), jnp.bfloat16),
            pltpu.VMEM((PLANES * SLOTS, WIDTH), jnp.bfloat16),
            pltpu.VMEM((PLANES, SLOTS), jnp.float32),
            pltpu.VMEM((PEERS, PLANES, SLOTS), jnp.float32),
            pltpu.VMEM((PEERS, 1, SLOTS), jnp.float32),
            pltpu.VMEM((PEERS, 1, SLOTS), jnp.float32),
            pltpu.VMEM((PLANES, 1, SLOTS), jnp.float32),
            pltpu.VMEM((PLANES, 1, SLOTS), jnp.float32),
            dma((BLOCKS + 2,)),
            dma((PLANES,)), dma((PLANES,)),
            dma((PLANES,)), dma((PLANES,)),
            dma((PLANES,)), dma((PLANES,)),
            dma, dma,
            dma, dma,
            dma((PLANES,)), dma((PLANES,)),
        ],
        compiler_params=pltpu.CompilerParams(
            collective_id=number, has_side_effects=True, vmem_limit_bytes=vmem
        ),
    )(embeddings, cluster_ids, ranks)


def shards(embeddings, cluster_ids, ranks):
    given = embeddings, cluster_ids.reshape(BLOCKS, 128), ranks.reshape(BLOCKS, 128)
    nearest, over = exchange(ROOM, 0, 40 << 20, *given)
    nearest = lax.switch(over[0], (lambda best: best, lambda best: exchange(SLOTS, 1, 67043328, *given)[0]), nearest)
    return nearest.reshape(ROWS_DEV)


def solution(mesh):
    return jax.shard_map(
        shards,
        mesh=mesh,
        in_specs=(
            P(("loader", "split"), None),
            P(("loader", "split"), None),
            P(("loader", "split")),
        ),
        out_specs=P(("loader", "split")),
        check_vma=False,
    )
```

```python
import functools

import jax
import jax.numpy as jnp
from jax import lax
from jax.experimental import pallas as pl
from jax.experimental.pallas import tpu as pltpu
from jax.sharding import PartitionSpec as P

MESH = pl.DeviceIdType.MESH
scope = jax.named_scope
CLUSTERS = 256
CAP = 4
WIDTH = 768
ROWS_DEV = 512
PLANES = 8
PEERS = 32
SLOTS = PEERS * CAP
BLOCKS = ROWS_DEV // 128
ROOM = 80
EMPTY = float(1 << 17)
GROUPS = ((0,), (1, 7), (2, 6), (5, 3), (4,))
ORDER = sum(GROUPS[1:], ())
epsilon = 1e-06


def place():
    row = lax.axis_index("loader")
    y = lax.axis_index("split")
    return lax.div(row, 8), y, lax.rem(lax.div(row, 2), 4), lax.rem(row, 2)


def device(z, y, x, c):
    return ((z * 4 + x) * 2 + c, y)


def across(here, s):
    z, y, x, c = here
    return device(lax.rem(z + s, PLANES), y, x, c)


def within(here, j, sign):
    z, y, x, c = here
    dy, dx, dc = j % 4, j // 4 % 4, j // 16
    return device(
        z,
        lax.rem(y + (4 + sign * dy) % 4, 4),
        lax.rem(x + (4 + sign * dx) % 4, 4),
        lax.rem(c + dc, 2),
    )


def hops(j):
    return min(j % 4, 4 - j % 4) + min(j // 4 % 4, 4 - j // 4 % 4)


FIRST = [(z, y, x) for z in range(3) for y in range(4) for x in range(4) if z + min(y, 4 - y) + min(x, 4 - x) <= 2]
FAR_FIRST = sorted(range(1, PEERS), key=lambda j: -hops(j))


def is_first(z, y, x):
    return z + jnp.minimum(y, 4 - y) + jnp.minimum(x, 4 - x) <= 2


def send(src, dst, sent, landed, to):
    return pltpu.make_async_remote_copy(
        src_ref=src,
        dst_ref=dst,
        send_sem=sent,
        recv_sem=landed,
        device_id=to,
        device_id_type=MESH,
    )


def product(a, b):
    return lax.dot_general(
        a, b, (((1,), (1,)), ((), ())), preferred_element_type=jnp.float32
    )


def iota(shape, dim):
    return lax.broadcasted_iota(jnp.int32, shape, dim)


def own_lanes(tiles_ref):
    group = iota((PLANES, SLOTS), 1) // CAP
    total = jnp.zeros((PLANES, SLOTS), jnp.float32)
    for j in range(PEERS):
        total = jnp.where(group == j, tiles_ref[j], total)
    return total


def kernel(
    room, emb_hbm, cid_hbm, rank_hbm, out_ref, flag_ref,
    raw, cid_ref, rank_ref, unit, meta_out, meta_in, rows_out, rows_in, dense, arrived, members,
    ranks_out, ranks_in, best_out, best_rows, best_in, far_in, back_out, back_in,
    raw_sem, meta_sent, meta_landed, rows_sent, rows_landed, dense_sent, dense_landed,
    ranks_sent, ranks_landed, best_sent, best_landed, far_sent, far_landed, back_sent, back_landed,
):
    here = place()
    z, y, x, c = here
    load_cid = pltpu.make_async_copy(cid_hbm, cid_ref, raw_sem.at[BLOCKS])
    load_cid.start()
    loads = [
        pltpu.make_async_copy(
            emb_hbm.at[pl.ds(b * 128, 128)], raw.at[pl.ds(b * 128, 128)], raw_sem.at[b]
        )
        for b in range(BLOCKS)
    ]
    for load in loads:
        load.start()
    load_rank = pltpu.make_async_copy(rank_hbm, rank_ref, raw_sem.at[BLOCKS + 1])
    load_rank.start()
    with scope("greet"):
        barrier = pltpu.get_barrier_semaphore()
        for s in (4, 3, 5, 2, 6, 1, 7):
            pl.semaphore_signal(barrier, inc=1, device_id=across(here, s), device_id_type=MESH)
        for j in FAR_FIRST:
            pl.semaphore_signal(barrier, inc=1, device_id=within(here, j, 1), device_id_type=MESH)

    with scope("count"):
        load_cid.wait()
        cid = cid_ref[...]
        owner = cid & (PEERS - 1)
        step = ((cid >> 5) - z) & (PLANES - 1)
        turned = jnp.concatenate([cid, step], axis=0).T
        before = iota((128, 128), 0) < iota((128, 128), 1)
        pack_rows, over = [], jnp.zeros((1, 128), jnp.float32)
        for b in range(BLOCKS):
            along = jnp.zeros((128, 128), jnp.float32)
            for a in range(b + 1):
                aside = turned[:, BLOCKS + a : BLOCKS + a + 1] == step[b : b + 1]
                along += jnp.where(aside & before if a == b else aside, 1.0, 0.0)
            count = jnp.sum(along, axis=0, keepdims=True).astype(jnp.int32)
            pack_rows.append(jnp.where(count < room, step[b : b + 1] * SLOTS + count, -1))
            over = jnp.maximum(over, jnp.where(count < room, 0.0, 2 * EMPTY))
        pack = jnp.concatenate(pack_rows, axis=1)
    with scope("norm"):
        for b in range(BLOCKS):
            loads[b].wait()
            values = raw[b * 128 : (b + 1) * 128].astype(jnp.float32)
            scale = lax.rsqrt(jnp.sum(values * values, axis=1, keepdims=True) + epsilon)
            unit[b * 128 : (b + 1) * 128] = (values * scale).astype(jnp.bfloat16)

    rows = {
        s: send(rows_out.at[s], rows_in.at[s], rows_sent.at[s], rows_landed.at[s], across(here, s))
        for s in range(1, PLANES)
    }
    metas = {
        s: send(meta_out.at[s], meta_in.at[s], meta_sent.at[s], meta_landed.at[s], across(here, s))
        for s in range(1, PLANES)
    }

    def gather_rows(group):
        chosen = jnp.concatenate(
            [jnp.where(pack == s * SLOTS + iota((room, ROWS_DEV), 0), 1.0, 0.0) for s in group], axis=0
        ).astype(jnp.bfloat16)
        packed = jnp.dot(chosen, unit[...], preferred_element_type=jnp.float32).astype(jnp.bfloat16)
        for n, s in enumerate(group):
            ref = rows_in if s == 0 else rows_out
            ref[s] = packed[n * room : (n + 1) * room]

    with scope("pack"):
        gather_rows(GROUPS[1])
    with scope("barrier_wait"):
        pl.semaphore_wait(barrier, PLANES - 1 + PEERS - 1)
    for s in GROUPS[1]:
        rows[s].start()

    with scope("slots"):
        peer = (
            (((owner >> 4) - c) & 1) * 16 + (((owner >> 2) - x) & 3) * 4 + ((owner - y) & 3)
        )
        slot_rows = []
        for b in range(BLOCKS):
            same = jnp.zeros((128, 128), jnp.float32)
            for a in range(b + 1):
                alike = turned[:, a : a + 1] == cid[b : b + 1]
                same += jnp.where(alike & before if a == b else alike, 1.0, 0.0)
            position = jnp.sum(same, axis=0, keepdims=True).astype(jnp.int32)
            slot_rows.append(step[b : b + 1] * SLOTS + peer[b : b + 1] * CAP + position)
        over = jnp.max(over, axis=1, keepdims=True)
        slot_turned = jnp.concatenate(slot_rows + pack_rows, axis=0).T
        load_rank.wait()
        rank_turned = (rank_ref[...].astype(jnp.float32) - EMPTY).T
        lane = iota((128, 128), 1)
        for s in range(PLANES):
            name = jnp.zeros((128, 128), jnp.float32)
            rank = jnp.zeros((128, 128), jnp.float32)
            for b in range(BLOCKS):
                slots = slot_turned[:, b : b + 1]
                packs = slot_turned[:, BLOCKS + b : BLOCKS + b + 1]
                name = jnp.where(packs == s * SLOTS + lane, (slots - (s * SLOTS - 1)).astype(jnp.float32), name)
                rank = jnp.where(slots == s * SLOTS + lane, rank_turned[:, b : b + 1], rank)
            ref = meta_in if s == 0 else meta_out
            ref[s, 0:1] = jnp.sum(name, axis=0, keepdims=True) - 1.0
            ref[s, 1:2] = jnp.sum(rank, axis=0, keepdims=True) + (EMPTY + over)
    for s in ORDER:
        metas[s].start()
    with scope("pack_rest"):
        for group in GROUPS[2:] + GROUPS[:1]:
            gather_rows(group)
            for s in group:
                if s:
                    rows[s].start()

    others = pl.ds(1, PEERS - 1)

    def spread(s):
        with scope(f"place#s={s}"):
            chosen = jnp.where(
                meta_in[s, 0:1, :room] == iota((SLOTS, room), 0).astype(jnp.float32), 1.0, 0.0
            ).astype(jnp.bfloat16)
            placed = jnp.dot(chosen, rows_in[s], preferred_element_type=jnp.float32).astype(jnp.bfloat16)
            dense[s] = placed.reshape(PEERS, CAP, WIDTH)
            arrived[s, 0] = placed[:CAP]
        with scope(f"deliver#s={s}"):
            for j in FAR_FIRST:
                send(dense.at[s, j], arrived.at[s, j], dense_sent.at[s], dense_landed.at[s], within(here, j, 1)).start()

    def all_dense(s):
        return send(dense.at[s, others], arrived.at[s, others], dense_sent.at[s], dense_landed.at[s], within(here, 1, 1))

    all_ranks = send(ranks_in.at[others], ranks_in.at[others], ranks_sent, ranks_landed, within(here, 1, 1))
    all_best = send(best_in.at[others], best_in.at[others], best_sent, best_landed, within(here, 1, 1))

    spread(0)
    for s in GROUPS[1]:
        with scope(f"rows_wait#s={s}"):
            metas[s].wait_recv()
            rows[s].wait_recv()
        spread(s)
    with scope("meta_wait"):
        for s in ORDER[len(GROUPS[1]) :]:
            metas[s].wait_recv()
    for s in range(PLANES):
        ranks_out[s : s + 1] = meta_in[s, 1:2]
    ranks_in[0] = ranks_out[...]
    for j in FAR_FIRST:
        send(ranks_out, ranks_in.at[j], ranks_sent, ranks_landed, within(here, j, 1)).start()

    for s in GROUPS[2]:
        with scope(f"rows_wait#s={s}"):
            rows[s].wait_recv()
        spread(s)
    with scope("ranks_wait"):
        all_ranks.wait_recv()
    rank_row = own_lanes(ranks_in)
    rank_col = rank_row.T
    highest = jnp.zeros((PLANES, SLOTS), jnp.float32)
    for j in range(PEERS):
        highest = jnp.maximum(highest, ranks_in[j])
    flag_ref[0] = jnp.max(jnp.where(highest >= 2 * EMPTY, 1, 0))

    best = [jnp.full((1, SLOTS), -1.0, jnp.float32)] * PLANES
    seen = []

    def compare(group):
        known = len(seen)
        for s in group:
            with scope(f"dense_wait#s={s}"):
                all_dense(s).wait_recv()
            members[len(seen) * SLOTS : (len(seen) + 1) * SLOTS] = arrived[s].reshape(SLOTS, WIDTH)
            seen.append(s)
        with scope(f"scores#n={len(seen)}"):
            scores = product(members[known * SLOTS : len(seen) * SLOTS], members[: len(seen) * SLOTS])

            def part(n, k):
                return scores[n * SLOTS : (n + 1) * SLOTS, k * SLOTS : (k + 1) * SLOTS]

            for k, q in enumerate(seen):
                top = jnp.full((SLOTS, SLOTS), -1.0, jnp.float32)
                for n, m in enumerate(group):
                    earlier = rank_col[:, m : m + 1] < rank_row[q : q + 1]
                    top = jnp.maximum(top, jnp.where(earlier, part(n, k), -1.0))
                best[q] = jnp.maximum(best[q], jnp.max(top, axis=0, keepdims=True))
            for n, q in enumerate(group):
                if known:
                    top = jnp.full((SLOTS, SLOTS), -1.0, jnp.float32)
                    for k, m in enumerate(seen[:known]):
                        earlier = rank_row[m : m + 1] < rank_col[:, q : q + 1]
                        top = jnp.maximum(top, jnp.where(earlier, part(n, k), -1.0))
                    best[q] = jnp.maximum(best[q], jnp.max(top.T, axis=0, keepdims=True))

    compare(GROUPS[0])
    compare(GROUPS[1])
    for s in GROUPS[3] + GROUPS[4]:
        with scope(f"rows_wait#s={s}"):
            rows[s].wait_recv()
        spread(s)
    compare(GROUPS[2])
    for s in GROUPS[3] + GROUPS[4]:
        compare((s,))

    lanes, peers = iota((PEERS, SLOTS), 1), iota((PEERS, SLOTS), 0)
    straight = []
    for n, (a, b, d, e) in enumerate((*chip, core) for chip in FIRST for core in (1, 0)):
        up, j = lax.rem(z - a + PLANES, PLANES), lax.rem(c + e, 2) * 16 + lax.rem(x - d + 4, 4) * 4 + lax.rem(y - b + 4, 4)
        straight.append((up, send(best_rows.at[up], far_in.at[up, j], far_sent.at[n], far_landed, device(a, b, d, e))))
    with scope("answer"):
        for s in range(PLANES):
            best_rows[s] = best[s]
        for up, copy in straight:
            pl.when(up != 0)(copy.start)
        answers = jnp.zeros((PEERS, SLOTS), jnp.float32)
        for s in range(PLANES):
            line = jnp.broadcast_to(best[s], (PEERS, SLOTS))
            picked = jnp.take_along_axis(line, CAP * peers + (lanes & (CAP - 1)), axis=1)
            answers = jnp.where(lanes // CAP == s, picked, answers)
        best_out[...] = answers.reshape(PEERS, 1, SLOTS)
        for j in FAR_FIRST:
            send(best_out.at[j], best_in.at[j], best_sent, best_landed, within(here, j, -1)).start()
    best_in[0] = best_out[0]
    for s in ORDER:
        metas[s].wait_send()
        rows[s].wait_send()
    for s in range(PLANES):
        all_dense(s).wait_send()
    all_ranks.wait_send()
    with scope("best_wait"):
        all_best.wait_recv()
    with scope("back"):
        answers = best_in[...].reshape(PEERS, SLOTS)
        backs = []
        for s in (4, 3, 5, 2, 6, 1, 7, 0):
            picked = jnp.take_along_axis(answers, CAP * s + (lanes & (CAP - 1)), axis=1)
            line = jnp.sum(jnp.where(lanes // CAP == peers, picked, 0.0), axis=0, keepdims=True)
            if s == 0:
                back_in[0] = line
                continue
            back_out[s] = line
            back = send(back_out.at[s], back_in.at[s], back_sent.at[s], back_landed.at[s], across(here, PLANES - s))
            wanted = jnp.logical_not(is_first(lax.rem(z + PLANES - s, PLANES), y, x))
            pl.when(wanted)(back.start)
            backs.append((wanted, back))
    all_best.wait_send()
    for up, copy in straight:
        pl.when(up != 0)(copy.wait_send)
    for wanted, back in backs:
        pl.when(wanted)(back.wait_send)
    first = is_first(z, y, x)

    @pl.when(jnp.logical_not(first))
    def _():
        with scope("back_wait"):
            for _, back in backs:
                back.wait_recv()

    @pl.when(first)
    def _():
        steps = far_in.at[pl.ds(1, PLANES - 1)]
        with scope("far_wait"):
            send(steps, steps, far_sent.at[0], far_landed, across(here, 1)).wait_recv()
        for s in range(1, PLANES):
            tiles = far_in[s].reshape(PEERS, SLOTS)
            back_in[s] = jnp.sum(jnp.where(lanes // CAP == peers, tiles, 0.0), axis=0, keepdims=True)

    with scope("final"):
        slot = jnp.concatenate(slot_rows * 2, axis=0)
        found = jnp.zeros((2 * BLOCKS, 128), jnp.float32)
        for s in range(PLANES):
            row = jnp.broadcast_to(back_in[s], (2 * BLOCKS, SLOTS))
            picked = jnp.take_along_axis(row, slot & (SLOTS - 1), axis=1)
            found = jnp.where(slot >> 7 == s, picked, found)
        out_ref[...] = found[:BLOCKS]


def exchange(room, number, vmem, embeddings, cluster_ids, ranks):
    dma = pltpu.SemaphoreType.DMA
    return pl.pallas_call(
        functools.partial(kernel, room),
        out_shape=(
            jax.ShapeDtypeStruct((BLOCKS, 128), jnp.float32),
            jax.ShapeDtypeStruct((1,), jnp.int32),
        ),
        in_specs=[
            pl.BlockSpec(memory_space=pltpu.HBM),
            pl.BlockSpec(memory_space=pltpu.HBM),
            pl.BlockSpec(memory_space=pltpu.HBM),
        ],
        out_specs=(pl.BlockSpec(memory_space=pltpu.VMEM), pl.BlockSpec(memory_space=pltpu.SMEM)),
        scratch_shapes=[
            pltpu.VMEM((ROWS_DEV, WIDTH), jnp.bfloat16),
            pltpu.VMEM((BLOCKS, 128), jnp.int32),
            pltpu.VMEM((BLOCKS, 128), jnp.int32),
            pltpu.VMEM((ROWS_DEV, WIDTH), jnp.bfloat16),
            pltpu.VMEM((PLANES, 2, SLOTS), jnp.float32),
            pltpu.VMEM((PLANES, 2, SLOTS), jnp.float32),
            pltpu.VMEM((PLANES, room, WIDTH), jnp.bfloat16),
            pltpu.VMEM((PLANES, room, WIDTH), jnp.bfloat16),
            pltpu.VMEM((PLANES, PEERS, CAP, WIDTH), jnp.bfloat16),
            pltpu.VMEM((PLANES, PEERS, CAP, WIDTH), jnp.bfloat16),
            pltpu.VMEM((PLANES * SLOTS, WIDTH), jnp.bfloat16),
            pltpu.VMEM((PLANES, SLOTS), jnp.float32),
            pltpu.VMEM((PEERS, PLANES, SLOTS), jnp.float32),
            pltpu.VMEM((PEERS, 1, SLOTS), jnp.float32),
            pltpu.VMEM((PLANES, 1, SLOTS), jnp.float32),
            pltpu.VMEM((PEERS, 1, SLOTS), jnp.float32),
            pltpu.VMEM((PLANES, PEERS, 1, SLOTS), jnp.float32),
            pltpu.VMEM((PLANES, 1, SLOTS), jnp.float32),
            pltpu.VMEM((PLANES, 1, SLOTS), jnp.float32),
            dma((BLOCKS + 2,)),
            dma((PLANES,)), dma((PLANES,)),
            dma((PLANES,)), dma((PLANES,)),
            dma((PLANES,)), dma((PLANES,)),
            dma, dma,
            dma, dma,
            dma((2 * len(FIRST),)), dma,
            dma((PLANES,)), dma((PLANES,)),
        ],
        compiler_params=pltpu.CompilerParams(
            collective_id=number, has_side_effects=True, vmem_limit_bytes=vmem
        ),
    )(embeddings, cluster_ids, ranks)


def shards(embeddings, cluster_ids, ranks):
    given = embeddings, cluster_ids.reshape(BLOCKS, 128), ranks.reshape(BLOCKS, 128)
    nearest, over = exchange(ROOM, 0, 40 << 20, *given)
    nearest = lax.switch(over[0], (lambda best: best, lambda best: exchange(SLOTS, 1, 67043328, *given)[0]), nearest)
    return nearest.reshape(ROWS_DEV)


def solution(mesh):
    return jax.shard_map(
        shards,
        mesh=mesh,
        in_specs=(
            P(("loader", "split"), None),
            P(("loader", "split"), None),
            P(("loader", "split")),
        ),
        out_specs=P(("loader", "split")),
        check_vma=False,
    )
```

```python
import functools

import jax
import jax.numpy as jnp
from jax import lax
from jax.experimental import pallas as pl
from jax.experimental.pallas import tpu as pltpu
from jax.sharding import PartitionSpec as P

MESH = pl.DeviceIdType.MESH
scope = jax.named_scope
CLUSTERS = 256
CAP = 4
WIDTH = 768
ROWS_DEV = 512
PLANES = 8
PEERS = 32
SLOTS = PEERS * CAP
BLOCKS = ROWS_DEV // 128
ROOM = 80
EMPTY = float(1 << 17)
GROUPS = ((0,), (1, 7), (2, 6), (5, 3), (4,))
ORDER = sum(GROUPS[1:], ())
epsilon = 1e-06


def place():
    row = lax.axis_index("loader")
    y = lax.axis_index("split")
    return lax.div(row, 8), y, lax.rem(lax.div(row, 2), 4), lax.rem(row, 2)


def device(z, y, x, c):
    return ((z * 4 + x) * 2 + c, y)


def across(here, s):
    z, y, x, c = here
    return device(lax.rem(z + s, PLANES), y, x, c)


def within(here, j, sign):
    z, y, x, c = here
    dy, dx, dc = j % 4, j // 4 % 4, j // 16
    return device(
        z,
        lax.rem(y + (4 + sign * dy) % 4, 4),
        lax.rem(x + (4 + sign * dx) % 4, 4),
        lax.rem(c + dc, 2),
    )


def hops(j):
    return min(j % 4, 4 - j % 4) + min(j // 4 % 4, 4 - j // 4 % 4)


FIRST = [(z, y, x) for z in range(3) for y in range(4) for x in range(4) if z + min(y, 4 - y) + min(x, 4 - x) <= 2]
BESIDE = (1, 3, 4, 12, 16)
ROUNDS = ((1, 3), (4, 12), (4, 12), (16,))
FAR_FIRST = sorted(range(1, PEERS), key=lambda j: -hops(j))


def is_first(z, y, x):
    return z + jnp.minimum(y, 4 - y) + jnp.minimum(x, 4 - x) <= 2


def send(src, dst, sent, landed, to):
    return pltpu.make_async_remote_copy(
        src_ref=src,
        dst_ref=dst,
        send_sem=sent,
        recv_sem=landed,
        device_id=to,
        device_id_type=MESH,
    )


def product(a, b):
    return lax.dot_general(
        a, b, (((1,), (1,)), ((), ())), preferred_element_type=jnp.float32
    )


def iota(shape, dim):
    return lax.broadcasted_iota(jnp.int32, shape, dim)


def own_lanes(tiles_ref):
    group = iota((PLANES, SLOTS), 1) // CAP
    total = jnp.zeros((PLANES, SLOTS), jnp.float32)
    for j in range(PEERS):
        total = jnp.where(group == j, tiles_ref[j], total)
    return total


def kernel(
    room, emb_hbm, cid_hbm, rank_hbm, out_ref, flag_ref,
    raw, cid_ref, rank_ref, unit, meta_out, meta_in, rows_out, rows_in, dense, arrived, members,
    ranks_out, ranks_in, best_out, best_rows, best_in, far_in, back_out, back_in,
    raw_sem, meta_sent, meta_landed, rows_sent, rows_landed, dense_sent, dense_landed,
    ranks_sent, ranks_landed, best_sent, best_landed, far_sent, far_landed, back_sent, back_landed, met,
):
    here = place()
    z, y, x, c = here
    load_cid = pltpu.make_async_copy(cid_hbm, cid_ref, raw_sem.at[BLOCKS])
    load_cid.start()
    loads = [
        pltpu.make_async_copy(
            emb_hbm.at[pl.ds(b * 128, 128)], raw.at[pl.ds(b * 128, 128)], raw_sem.at[b]
        )
        for b in range(BLOCKS)
    ]
    for load in loads:
        load.start()
    load_rank = pltpu.make_async_copy(rank_hbm, rank_ref, raw_sem.at[BLOCKS + 1])
    load_rank.start()
    with scope("greet"):
        barrier = pltpu.get_barrier_semaphore()
        for s in (4, 3, 5, 2, 6, 1, 7):
            pl.semaphore_signal(barrier, inc=1, device_id=across(here, s), device_id_type=MESH)
        for j in BESIDE:
            pl.semaphore_signal(barrier, inc=1, device_id=within(here, j, 1), device_id_type=MESH)

    def tell(n):
        for j in ROUNDS[n]:
            pl.semaphore_signal(met.at[n], inc=1, device_id=within(here, j, 1), device_id_type=MESH)

    def hear(n):
        with scope(f"hear#n={n}"):
            pl.semaphore_wait(met.at[n], len(ROUNDS[n]))

    with scope("count"):
        load_cid.wait()
        cid = cid_ref[...]
        owner = cid & (PEERS - 1)
        step = ((cid >> 5) - z) & (PLANES - 1)
        turned = jnp.concatenate([cid, step], axis=0).T
        before = iota((128, 128), 0) < iota((128, 128), 1)
        pack_rows, over = [], jnp.zeros((1, 128), jnp.float32)
        for b in range(BLOCKS):
            along = jnp.zeros((128, 128), jnp.float32)
            for a in range(b + 1):
                aside = turned[:, BLOCKS + a : BLOCKS + a + 1] == step[b : b + 1]
                along += jnp.where(aside & before if a == b else aside, 1.0, 0.0)
            count = jnp.sum(along, axis=0, keepdims=True).astype(jnp.int32)
            pack_rows.append(jnp.where(count < room, step[b : b + 1] * SLOTS + count, -1))
            over = jnp.maximum(over, jnp.where(count < room, 0.0, 2 * EMPTY))
        pack = jnp.concatenate(pack_rows, axis=1)
    with scope("norm"):
        for b in range(BLOCKS):
            loads[b].wait()
            values = raw[b * 128 : (b + 1) * 128].astype(jnp.float32)
            scale = lax.rsqrt(jnp.sum(values * values, axis=1, keepdims=True) + epsilon)
            unit[b * 128 : (b + 1) * 128] = (values * scale).astype(jnp.bfloat16)

    rows = {
        s: send(rows_out.at[s], rows_in.at[s], rows_sent.at[s], rows_landed.at[s], across(here, s))
        for s in range(1, PLANES)
    }
    metas = {
        s: send(meta_out.at[s], meta_in.at[s], meta_sent.at[s], meta_landed.at[s], across(here, s))
        for s in range(1, PLANES)
    }

    def gather_rows(group):
        chosen = jnp.concatenate(
            [jnp.where(pack == s * SLOTS + iota((room, ROWS_DEV), 0), 1.0, 0.0) for s in group], axis=0
        ).astype(jnp.bfloat16)
        packed = jnp.dot(chosen, unit[...], preferred_element_type=jnp.float32).astype(jnp.bfloat16)
        for n, s in enumerate(group):
            ref = rows_in if s == 0 else rows_out
            ref[s] = packed[n * room : (n + 1) * room]

    with scope("pack"):
        gather_rows(GROUPS[1])
    with scope("barrier_wait"):
        pl.semaphore_wait(barrier, PLANES - 1 + len(BESIDE))
    for s in GROUPS[1]:
        rows[s].start()
    tell(0)

    with scope("slots"):
        peer = (
            (((owner >> 4) - c) & 1) * 16 + (((owner >> 2) - x) & 3) * 4 + ((owner - y) & 3)
        )
        slot_rows = []
        for b in range(BLOCKS):
            same = jnp.zeros((128, 128), jnp.float32)
            for a in range(b + 1):
                alike = turned[:, a : a + 1] == cid[b : b + 1]
                same += jnp.where(alike & before if a == b else alike, 1.0, 0.0)
            position = jnp.sum(same, axis=0, keepdims=True).astype(jnp.int32)
            slot_rows.append(step[b : b + 1] * SLOTS + peer[b : b + 1] * CAP + position)
        over = jnp.max(over, axis=1, keepdims=True)
        slot_turned = jnp.concatenate(slot_rows + pack_rows, axis=0).T
        load_rank.wait()
        rank_turned = (rank_ref[...].astype(jnp.float32) - EMPTY).T
        lane = iota((128, 128), 1)
        for s in range(PLANES):
            name = jnp.zeros((128, 128), jnp.float32)
            rank = jnp.zeros((128, 128), jnp.float32)
            for b in range(BLOCKS):
                slots = slot_turned[:, b : b + 1]
                packs = slot_turned[:, BLOCKS + b : BLOCKS + b + 1]
                name = jnp.where(packs == s * SLOTS + lane, (slots - (s * SLOTS - 1)).astype(jnp.float32), name)
                rank = jnp.where(slots == s * SLOTS + lane, rank_turned[:, b : b + 1], rank)
            ref = meta_in if s == 0 else meta_out
            ref[s, 0:1] = jnp.sum(name, axis=0, keepdims=True) - 1.0
            ref[s, 1:2] = jnp.sum(rank, axis=0, keepdims=True) + (EMPTY + over)
    for s in ORDER:
        metas[s].start()
    for n, group in enumerate(GROUPS[2:] + GROUPS[:1]):
        with scope("pack_rest"):
            gather_rows(group)
            for s in group:
                if s:
                    rows[s].start()
        if n < len(ROUNDS):
            hear(n)
            if n + 1 < len(ROUNDS):
                tell(n + 1)

    others = pl.ds(1, PEERS - 1)

    def spread(s):
        with scope(f"place#s={s}"):
            chosen = jnp.where(
                meta_in[s, 0:1, :room] == iota((SLOTS, room), 0).astype(jnp.float32), 1.0, 0.0
            ).astype(jnp.bfloat16)
            placed = jnp.dot(chosen, rows_in[s], preferred_element_type=jnp.float32).astype(jnp.bfloat16)
            dense[s] = placed.reshape(PEERS, CAP, WIDTH)
            arrived[s, 0] = placed[:CAP]
        with scope(f"deliver#s={s}"):
            for j in FAR_FIRST:
                send(dense.at[s, j], arrived.at[s, j], dense_sent.at[s], dense_landed.at[s], within(here, j, 1)).start()

    def all_dense(s):
        return send(dense.at[s, others], arrived.at[s, others], dense_sent.at[s], dense_landed.at[s], within(here, 1, 1))

    all_ranks = send(ranks_in.at[others], ranks_in.at[others], ranks_sent, ranks_landed, within(here, 1, 1))
    all_best = send(best_in.at[others], best_in.at[others], best_sent, best_landed, within(here, 1, 1))

    spread(0)
    for s in GROUPS[1]:
        with scope(f"rows_wait#s={s}"):
            metas[s].wait_recv()
            rows[s].wait_recv()
        spread(s)
    with scope("meta_wait"):
        for s in ORDER[len(GROUPS[1]) :]:
            metas[s].wait_recv()
    for s in range(PLANES):
        ranks_out[s : s + 1] = meta_in[s, 1:2]
    ranks_in[0] = ranks_out[...]
    for j in FAR_FIRST:
        send(ranks_out, ranks_in.at[j], ranks_sent, ranks_landed, within(here, j, 1)).start()

    for s in GROUPS[2]:
        with scope(f"rows_wait#s={s}"):
            rows[s].wait_recv()
        spread(s)
    best = [jnp.full((1, SLOTS), -1.0, jnp.float32)] * PLANES
    seen = []

    def compare(group):
        known = len(seen)
        for s in group:
            with scope(f"dense_wait#s={s}"):
                all_dense(s).wait_recv()
            members[len(seen) * SLOTS : (len(seen) + 1) * SLOTS] = arrived[s].reshape(SLOTS, WIDTH)
            seen.append(s)
        with scope(f"scores#n={len(seen)}"):
            scores = product(members[known * SLOTS : len(seen) * SLOTS], members[: len(seen) * SLOTS])

            def part(n, k):
                return scores[n * SLOTS : (n + 1) * SLOTS, k * SLOTS : (k + 1) * SLOTS]

            for k, q in enumerate(seen):
                top = jnp.full((SLOTS, SLOTS), -1.0, jnp.float32)
                for n, m in enumerate(group):
                    earlier = rank_col[:, m : m + 1] < rank_row[q : q + 1]
                    top = jnp.maximum(top, jnp.where(earlier, part(n, k), -1.0))
                best[q] = jnp.maximum(best[q], jnp.max(top, axis=0, keepdims=True))
            for n, q in enumerate(group):
                if known:
                    top = jnp.full((SLOTS, SLOTS), -1.0, jnp.float32)
                    for k, m in enumerate(seen[:known]):
                        earlier = rank_row[m : m + 1] < rank_col[:, q : q + 1]
                        top = jnp.maximum(top, jnp.where(earlier, part(n, k), -1.0))
                    best[q] = jnp.maximum(best[q], jnp.max(top.T, axis=0, keepdims=True))

    for s in GROUPS[3]:
        with scope(f"rows_wait#s={s}"):
            rows[s].wait_recv()
        spread(s)
    with scope("ranks_wait"):
        all_ranks.wait_recv()
    rank_row = own_lanes(ranks_in)
    rank_col = rank_row.T
    highest = jnp.zeros((PLANES, SLOTS), jnp.float32)
    for j in range(PEERS):
        highest = jnp.maximum(highest, ranks_in[j])
    flag_ref[0] = jnp.max(jnp.where(highest >= 2 * EMPTY, 1, 0))

    compare(GROUPS[0])
    compare(GROUPS[1])
    for s in GROUPS[4]:
        with scope(f"rows_wait#s={s}"):
            rows[s].wait_recv()
        spread(s)
    compare(GROUPS[2])
    for s in GROUPS[3] + GROUPS[4]:
        compare((s,))

    lanes, peers = iota((PEERS, SLOTS), 1), iota((PEERS, SLOTS), 0)
    straight = []
    for n, (a, b, d, e) in enumerate((*chip, core) for chip in FIRST for core in (1, 0)):
        up, j = lax.rem(z - a + PLANES, PLANES), lax.rem(c + e, 2) * 16 + lax.rem(x - d + 4, 4) * 4 + lax.rem(y - b + 4, 4)
        straight.append((up, send(best_rows.at[up], far_in.at[up, j], far_sent.at[n], far_landed, device(a, b, d, e))))
    with scope("answer"):
        for s in range(PLANES):
            best_rows[s] = best[s]
        for up, copy in straight:
            pl.when(up != 0)(copy.start)
        answers = jnp.zeros((PEERS, SLOTS), jnp.float32)
        for s in range(PLANES):
            line = jnp.broadcast_to(best[s], (PEERS, SLOTS))
            picked = jnp.take_along_axis(line, CAP * peers + (lanes & (CAP - 1)), axis=1)
            answers = jnp.where(lanes // CAP == s, picked, answers)
        best_out[...] = answers.reshape(PEERS, 1, SLOTS)
        for j in FAR_FIRST:
            send(best_out.at[j], best_in.at[j], best_sent, best_landed, within(here, j, -1)).start()
    best_in[0] = best_out[0]
    for s in ORDER:
        metas[s].wait_send()
        rows[s].wait_send()
    for s in range(PLANES):
        all_dense(s).wait_send()
    all_ranks.wait_send()
    with scope("best_wait"):
        all_best.wait_recv()
    with scope("back"):
        answers = best_in[...].reshape(PEERS, SLOTS)
        backs = []
        for s in (4, 3, 5, 2, 6, 1, 7, 0):
            picked = jnp.take_along_axis(answers, CAP * s + (lanes & (CAP - 1)), axis=1)
            line = jnp.sum(jnp.where(lanes // CAP == peers, picked, 0.0), axis=0, keepdims=True)
            if s == 0:
                back_in[0] = line
                continue
            back_out[s] = line
            back = send(back_out.at[s], back_in.at[s], back_sent.at[s], back_landed.at[s], across(here, PLANES - s))
            wanted = jnp.logical_not(is_first(lax.rem(z + PLANES - s, PLANES), y, x))
            pl.when(wanted)(back.start)
            backs.append((wanted, back))
    all_best.wait_send()
    for up, copy in straight:
        pl.when(up != 0)(copy.wait_send)
    for wanted, back in backs:
        pl.when(wanted)(back.wait_send)
    first = is_first(z, y, x)

    @pl.when(jnp.logical_not(first))
    def _():
        with scope("back_wait"):
            for _, back in backs:
                back.wait_recv()

    @pl.when(first)
    def _():
        steps = far_in.at[pl.ds(1, PLANES - 1)]
        with scope("far_wait"):
            send(steps, steps, far_sent.at[0], far_landed, across(here, 1)).wait_recv()
        for s in range(1, PLANES):
            tiles = far_in[s].reshape(PEERS, SLOTS)
            back_in[s] = jnp.sum(jnp.where(lanes // CAP == peers, tiles, 0.0), axis=0, keepdims=True)

    with scope("final"):
        slot = jnp.concatenate(slot_rows * 2, axis=0)
        found = jnp.zeros((2 * BLOCKS, 128), jnp.float32)
        for s in range(PLANES):
            row = jnp.broadcast_to(back_in[s], (2 * BLOCKS, SLOTS))
            picked = jnp.take_along_axis(row, slot & (SLOTS - 1), axis=1)
            found = jnp.where(slot >> 7 == s, picked, found)
        out_ref[...] = found[:BLOCKS]


def exchange(room, number, vmem, embeddings, cluster_ids, ranks):
    dma = pltpu.SemaphoreType.DMA
    return pl.pallas_call(
        functools.partial(kernel, room),
        out_shape=(
            jax.ShapeDtypeStruct((BLOCKS, 128), jnp.float32),
            jax.ShapeDtypeStruct((1,), jnp.int32),
        ),
        in_specs=[
            pl.BlockSpec(memory_space=pltpu.HBM),
            pl.BlockSpec(memory_space=pltpu.HBM),
            pl.BlockSpec(memory_space=pltpu.HBM),
        ],
        out_specs=(pl.BlockSpec(memory_space=pltpu.VMEM), pl.BlockSpec(memory_space=pltpu.SMEM)),
        scratch_shapes=[
            pltpu.VMEM((ROWS_DEV, WIDTH), jnp.bfloat16),
            pltpu.VMEM((BLOCKS, 128), jnp.int32),
            pltpu.VMEM((BLOCKS, 128), jnp.int32),
            pltpu.VMEM((ROWS_DEV, WIDTH), jnp.bfloat16),
            pltpu.VMEM((PLANES, 2, SLOTS), jnp.float32),
            pltpu.VMEM((PLANES, 2, SLOTS), jnp.float32),
            pltpu.VMEM((PLANES, room, WIDTH), jnp.bfloat16),
            pltpu.VMEM((PLANES, room, WIDTH), jnp.bfloat16),
            pltpu.VMEM((PLANES, PEERS, CAP, WIDTH), jnp.bfloat16),
            pltpu.VMEM((PLANES, PEERS, CAP, WIDTH), jnp.bfloat16),
            pltpu.VMEM((PLANES * SLOTS, WIDTH), jnp.bfloat16),
            pltpu.VMEM((PLANES, SLOTS), jnp.float32),
            pltpu.VMEM((PEERS, PLANES, SLOTS), jnp.float32),
            pltpu.VMEM((PEERS, 1, SLOTS), jnp.float32),
            pltpu.VMEM((PLANES, 1, SLOTS), jnp.float32),
            pltpu.VMEM((PEERS, 1, SLOTS), jnp.float32),
            pltpu.VMEM((PLANES, PEERS, 1, SLOTS), jnp.float32),
            pltpu.VMEM((PLANES, 1, SLOTS), jnp.float32),
            pltpu.VMEM((PLANES, 1, SLOTS), jnp.float32),
            dma((BLOCKS + 2,)),
            dma((PLANES,)), dma((PLANES,)),
            dma((PLANES,)), dma((PLANES,)),
            dma((PLANES,)), dma((PLANES,)),
            dma, dma,
            dma, dma,
            dma((2 * len(FIRST),)), dma,
            dma((PLANES,)), dma((PLANES,)),
            pltpu.SemaphoreType.REGULAR((len(ROUNDS),)),
        ],
        compiler_params=pltpu.CompilerParams(
            collective_id=number, has_side_effects=True, vmem_limit_bytes=vmem
        ),
    )(embeddings, cluster_ids, ranks)


def shards(embeddings, cluster_ids, ranks):
    given = embeddings, cluster_ids.reshape(BLOCKS, 128), ranks.reshape(BLOCKS, 128)
    nearest, over = exchange(ROOM, 0, 40 << 20, *given)
    nearest = lax.switch(over[0], (lambda best: best, lambda best: exchange(SLOTS, 1, 67043328, *given)[0]), nearest)
    return nearest.reshape(ROWS_DEV)


def solution(mesh):
    return jax.shard_map(
        shards,
        mesh=mesh,
        in_specs=(
            P(("loader", "split"), None),
            P(("loader", "split"), None),
            P(("loader", "split")),
        ),
        out_specs=P(("loader", "split")),
        check_vma=False,
    )
```

```python
import functools

import jax
import jax.numpy as jnp
from jax import lax
from jax.experimental import pallas as pl
from jax.experimental.pallas import tpu as pltpu
from jax.sharding import PartitionSpec as P

MESH = pl.DeviceIdType.MESH
scope = jax.named_scope
CLUSTERS = 256
CAP = 4
WIDTH = 768
ROWS_DEV = 512
PLANES = 8
PEERS = 32
SLOTS = PEERS * CAP
BLOCKS = ROWS_DEV // 128
ROOM = 80
EMPTY = float(1 << 17)
GROUPS = ((0,), (1, 7), (2, 6), (5, 3), (4,))
ORDER = sum(GROUPS[1:], ())
epsilon = 1e-06


def place():
    row = lax.axis_index("loader")
    y = lax.axis_index("split")
    return lax.div(row, 8), y, lax.rem(lax.div(row, 2), 4), lax.rem(row, 2)


def device(z, y, x, c):
    return ((z * 4 + x) * 2 + c, y)


def across(here, s):
    z, y, x, c = here
    return device(lax.rem(z + s, PLANES), y, x, c)


def within(here, j, sign):
    z, y, x, c = here
    dy, dx, dc = j % 4, j // 4 % 4, j // 16
    return device(
        z,
        lax.rem(y + (4 + sign * dy) % 4, 4),
        lax.rem(x + (4 + sign * dx) % 4, 4),
        lax.rem(c + dc, 2),
    )


def hops(j):
    return min(j % 4, 4 - j % 4) + min(j // 4 % 4, 4 - j // 4 % 4)


FIRST = [(z, y, x) for z in range(3) for y in range(4) for x in range(4) if z + min(y, 4 - y) + min(x, 4 - x) <= 2]
BESIDE = (1, 3, 4, 12, 16)
ROUNDS = ((1, 3), (4, 12), (4, 12), (16,))
FAR_FIRST = sorted(range(1, PEERS), key=lambda j: -hops(j))


def is_first(z, y, x):
    return z + jnp.minimum(y, 4 - y) + jnp.minimum(x, 4 - x) <= 2


def send(src, dst, sent, landed, to):
    return pltpu.make_async_remote_copy(
        src_ref=src,
        dst_ref=dst,
        send_sem=sent,
        recv_sem=landed,
        device_id=to,
        device_id_type=MESH,
    )


def product(a, b):
    return lax.dot_general(
        a, b, (((1,), (1,)), ((), ())), preferred_element_type=jnp.float32
    )


def iota(shape, dim):
    return lax.broadcasted_iota(jnp.int32, shape, dim)


def own_lanes(tiles_ref):
    group = iota((PLANES, SLOTS), 1) // CAP
    total = jnp.zeros((PLANES, SLOTS), jnp.float32)
    for j in range(PEERS):
        total = jnp.where(group == j, tiles_ref[j], total)
    return total


def kernel(
    room, emb_hbm, cid_hbm, rank_hbm, out_ref, flag_hbm, flag_ref,
    raw, cid_ref, rank_ref, unit, meta_out, meta_in, rows_out, rows_in, dense, arrived, members,
    ranks_out, ranks_in, best_out, best_rows, best_in, far_in, back_out, back_in,
    raw_sem, cid_sem, rank_sem, meta_sent, meta_landed, rows_sent, rows_landed, dense_sent, dense_landed,
    ranks_sent, ranks_landed, best_sent, best_landed, far_sent, far_landed, back_sent, back_landed, met,
):
    here = place()
    z, y, x, c = here
    load_cid = pltpu.make_async_copy(cid_hbm, cid_ref, cid_sem)
    load_cid.start()
    load = pltpu.make_async_copy(emb_hbm, raw, raw_sem)
    load.start()
    load_rank = pltpu.make_async_copy(rank_hbm, rank_ref, rank_sem)
    load_rank.start()
    with scope("greet"):
        barrier = pltpu.get_barrier_semaphore()
        for s in (4, 3, 5, 2, 6, 1, 7):
            pl.semaphore_signal(barrier, inc=1, device_id=across(here, s), device_id_type=MESH)
        for j in BESIDE:
            pl.semaphore_signal(barrier, inc=1, device_id=within(here, j, 1), device_id_type=MESH)

    def tell(n):
        for j in ROUNDS[n]:
            pl.semaphore_signal(met.at[n], inc=1, device_id=within(here, j, 1), device_id_type=MESH)

    def hear(n):
        with scope(f"hear#n={n}"):
            pl.semaphore_wait(met.at[n], len(ROUNDS[n]))

    with scope("count"):
        load_cid.wait()
        cid = cid_ref[...]
        owner = cid & (PEERS - 1)
        step = ((cid >> 5) - z) & (PLANES - 1)
        turned = jnp.concatenate([cid, step], axis=0).T
        before = iota((128, 128), 0) < iota((128, 128), 1)
        pack_rows, over = [], jnp.zeros((1, 128), jnp.float32)
        for b in range(BLOCKS):
            along = jnp.zeros((128, 128), jnp.float32)
            for a in range(b + 1):
                aside = turned[:, BLOCKS + a : BLOCKS + a + 1] == step[b : b + 1]
                along += jnp.where(aside & before if a == b else aside, 1.0, 0.0)
            count = jnp.sum(along, axis=0, keepdims=True).astype(jnp.int32)
            pack_rows.append(jnp.where(count < room, step[b : b + 1] * SLOTS + count, -1))
            over = jnp.maximum(over, jnp.where(count < room, 0.0, 2 * EMPTY))
        pack = jnp.concatenate(pack_rows, axis=1)
    with scope("norm"):
        load.wait()
        for b in range(BLOCKS):
            values = raw[b * 128 : (b + 1) * 128].astype(jnp.float32)
            scale = lax.rsqrt(jnp.sum(values * values, axis=1, keepdims=True) + epsilon)
            unit[b * 128 : (b + 1) * 128] = (values * scale).astype(jnp.bfloat16)

    rows = {
        s: send(rows_out.at[s], rows_in.at[s], rows_sent, rows_landed.at[s - 1], across(here, s))
        for s in range(1, PLANES)
    }
    metas = {
        s: send(meta_out.at[s], meta_in.at[s], meta_sent, meta_landed.at[0 if s in GROUPS[1] else 1], across(here, s))
        for s in range(1, PLANES)
    }

    def gather_rows(group):
        chosen = jnp.concatenate(
            [jnp.where(pack == s * SLOTS + iota((room, ROWS_DEV), 0), 1.0, 0.0) for s in group], axis=0
        ).astype(jnp.bfloat16)
        packed = jnp.dot(chosen, unit[...], preferred_element_type=jnp.float32).astype(jnp.bfloat16)
        for n, s in enumerate(group):
            ref = rows_in if s == 0 else rows_out
            ref[s] = packed[n * room : (n + 1) * room]

    with scope("pack"):
        gather_rows(GROUPS[1])
    with scope("barrier_wait"):
        pl.semaphore_wait(barrier, PLANES - 1 + len(BESIDE))
    for s in GROUPS[1]:
        rows[s].start()
    tell(0)

    with scope("slots"):
        peer = (
            (((owner >> 4) - c) & 1) * 16 + (((owner >> 2) - x) & 3) * 4 + ((owner - y) & 3)
        )
        slot_rows = []
        for b in range(BLOCKS):
            same = jnp.zeros((128, 128), jnp.float32)
            for a in range(b + 1):
                alike = turned[:, a : a + 1] == cid[b : b + 1]
                same += jnp.where(alike & before if a == b else alike, 1.0, 0.0)
            position = jnp.sum(same, axis=0, keepdims=True).astype(jnp.int32)
            slot_rows.append(step[b : b + 1] * SLOTS + peer[b : b + 1] * CAP + position)
        over = jnp.max(over, axis=1, keepdims=True)
        slot_turned = jnp.concatenate(slot_rows + pack_rows, axis=0).T
        load_rank.wait()
        rank_turned = (rank_ref[...].astype(jnp.float32) - EMPTY).T
        lane = iota((128, 128), 1)
        for s in range(PLANES):
            name = jnp.zeros((128, 128), jnp.float32)
            rank = jnp.zeros((128, 128), jnp.float32)
            for b in range(BLOCKS):
                slots = slot_turned[:, b : b + 1]
                packs = slot_turned[:, BLOCKS + b : BLOCKS + b + 1]
                name = jnp.where(packs == s * SLOTS + lane, (slots - (s * SLOTS - 1)).astype(jnp.float32), name)
                rank = jnp.where(slots == s * SLOTS + lane, rank_turned[:, b : b + 1], rank)
            ref = meta_in if s == 0 else meta_out
            ref[s, 0:1] = jnp.sum(name, axis=0, keepdims=True) - 1.0
            ref[s, 1:2] = jnp.sum(rank, axis=0, keepdims=True) + (EMPTY + over)
    for s in ORDER:
        metas[s].start()
    for n, group in enumerate(GROUPS[2:] + GROUPS[:1]):
        with scope("pack_rest"):
            gather_rows(group)
            for s in group:
                if s:
                    rows[s].start()
        if n < len(ROUNDS):
            hear(n)
            if n + 1 < len(ROUNDS):
                tell(n + 1)

    others = pl.ds(1, PEERS - 1)

    def spread(s):
        with scope(f"place#s={s}"):
            chosen = jnp.where(
                meta_in[s, 0:1, :room] == iota((SLOTS, room), 0).astype(jnp.float32), 1.0, 0.0
            ).astype(jnp.bfloat16)
            placed = jnp.dot(chosen, rows_in[s], preferred_element_type=jnp.float32).astype(jnp.bfloat16)
            dense[s] = placed.reshape(PEERS, CAP, WIDTH)
            arrived[s, 0] = placed[:CAP]
        with scope(f"deliver#s={s}"):
            for j in FAR_FIRST:
                send(dense.at[s, j], arrived.at[s, j], dense_sent, dense_landed.at[s], within(here, j, 1)).start()

    def all_dense(s):
        return send(dense.at[s, others], arrived.at[s, others], dense_sent, dense_landed.at[s], within(here, 1, 1))

    all_ranks = send(ranks_in.at[others], ranks_in.at[others], ranks_sent, ranks_landed, within(here, 1, 1))
    all_best = send(best_in.at[others], best_in.at[others], best_sent, best_landed, within(here, 1, 1))

    spread(0)
    def metas_in(n, count):
        some = meta_in.at[pl.ds(0, count)]
        return send(some, some, meta_sent, meta_landed.at[n], across(here, 1))

    metas_in(0, len(GROUPS[1])).wait_recv()
    for s in GROUPS[1]:
        with scope(f"rows_wait#s={s}"):
            rows[s].wait_recv()
        spread(s)
    with scope("meta_wait"):
        metas_in(1, PLANES - 1 - len(GROUPS[1])).wait_recv()
    for s in range(PLANES):
        ranks_out[s : s + 1] = meta_in[s, 1:2]
    ranks_in[0] = ranks_out[...]
    for j in FAR_FIRST:
        send(ranks_out, ranks_in.at[j], ranks_sent, ranks_landed, within(here, j, 1)).start()

    for s in GROUPS[2]:
        with scope(f"rows_wait#s={s}"):
            rows[s].wait_recv()
        spread(s)
    best = [jnp.full((1, SLOTS), -1.0, jnp.float32)] * PLANES
    seen = []

    def compare(group):
        known = len(seen)
        for s in group:
            with scope(f"dense_wait#s={s}"):
                all_dense(s).wait_recv()
            members[len(seen) * SLOTS : (len(seen) + 1) * SLOTS] = arrived[s].reshape(SLOTS, WIDTH)
            seen.append(s)
        with scope(f"scores#n={len(seen)}"):
            scores = product(members[known * SLOTS : len(seen) * SLOTS], members[: len(seen) * SLOTS])

            def part(n, k):
                return scores[n * SLOTS : (n + 1) * SLOTS, k * SLOTS : (k + 1) * SLOTS]

            for k, q in enumerate(seen):
                top = jnp.full((SLOTS, SLOTS), -1.0, jnp.float32)
                for n, m in enumerate(group):
                    earlier = rank_col[:, m : m + 1] < rank_row[q : q + 1]
                    top = jnp.maximum(top, jnp.where(earlier, part(n, k), -1.0))
                best[q] = jnp.maximum(best[q], jnp.max(top, axis=0, keepdims=True))
            for n, q in enumerate(group):
                if known:
                    top = jnp.full((SLOTS, SLOTS), -1.0, jnp.float32)
                    for k, m in enumerate(seen[:known]):
                        earlier = rank_row[m : m + 1] < rank_col[:, q : q + 1]
                        top = jnp.maximum(top, jnp.where(earlier, part(n, k), -1.0))
                    best[q] = jnp.maximum(best[q], jnp.max(top.T, axis=0, keepdims=True))

    for s in GROUPS[3]:
        with scope(f"rows_wait#s={s}"):
            rows[s].wait_recv()
        spread(s)
    with scope("ranks_wait"):
        all_ranks.wait_recv()
    rank_row = own_lanes(ranks_in)
    rank_col = rank_row.T
    highest = jnp.zeros((PLANES, SLOTS), jnp.float32)
    for j in range(PEERS):
        highest = jnp.maximum(highest, ranks_in[j])
    flag_ref[0] = jnp.max(jnp.where(highest >= 2 * EMPTY, 1, 0))
    save_flag = pltpu.make_async_copy(flag_ref, flag_hbm, cid_sem)
    save_flag.start()

    compare(GROUPS[0])
    compare(GROUPS[1])
    for s in GROUPS[4]:
        with scope(f"rows_wait#s={s}"):
            rows[s].wait_recv()
        spread(s)
    compare(GROUPS[2])
    for s in GROUPS[3] + GROUPS[4]:
        compare((s,))

    lanes, peers = iota((PEERS, SLOTS), 1), iota((PEERS, SLOTS), 0)
    straight = []
    for a, b, d, e in [(*chip, core) for chip in FIRST for core in (1, 0)]:
        up, j = lax.rem(z - a + PLANES, PLANES), lax.rem(c + e, 2) * 16 + lax.rem(x - d + 4, 4) * 4 + lax.rem(y - b + 4, 4)
        straight.append((up, send(best_rows.at[up], far_in.at[up, j], far_sent.at[e], far_landed, device(a, b, d, e))))
    with scope("answer"):
        for s in range(PLANES):
            best_rows[s] = best[s]
        for up, copy in straight:
            pl.when(up != 0)(copy.start)
        answers = jnp.zeros((PEERS, SLOTS), jnp.float32)
        for s in range(PLANES):
            line = jnp.broadcast_to(best[s], (PEERS, SLOTS))
            picked = jnp.take_along_axis(line, CAP * peers + (lanes & (CAP - 1)), axis=1)
            answers = jnp.where(lanes // CAP == s, picked, answers)
        best_out[...] = answers.reshape(PEERS, 1, SLOTS)
        for j in FAR_FIRST:
            send(best_out.at[j], best_in.at[j], best_sent, best_landed, within(here, j, -1)).start()
    best_in[0] = best_out[0]
    metas_in(0, PLANES - 1).wait_send()
    steps = pl.ds(1, PLANES - 1)
    send(rows_out.at[steps], rows_out.at[steps], rows_sent, rows_landed.at[0], across(here, 1)).wait_send()
    send(dense.at[:, others], dense.at[:, others], dense_sent, dense_landed.at[0], across(here, 1)).wait_send()
    all_ranks.wait_send()
    save_flag.wait()
    with scope("best_wait"):
        all_best.wait_recv()
    with scope("back"):
        answers = best_in[...].reshape(PEERS, SLOTS)
        backs = []
        for s in (4, 3, 5, 2, 6, 1, 7, 0):
            picked = jnp.take_along_axis(answers, CAP * s + (lanes & (CAP - 1)), axis=1)
            line = jnp.sum(jnp.where(lanes // CAP == peers, picked, 0.0), axis=0, keepdims=True)
            if s == 0:
                back_in[0] = line
                continue
            back_out[s] = line
            back = send(back_out.at[s], back_in.at[s], back_sent, back_landed, across(here, PLANES - s))
            wanted = jnp.logical_not(is_first(lax.rem(z + PLANES - s, PLANES), y, x))
            pl.when(wanted)(back.start)
            backs.append((wanted, back))
    all_best.wait_send()
    for a in range(PLANES):
        count = len([chip for chip in FIRST if chip[0] != a])

        @pl.when(z == a)
        def _():
            for e in range(2):
                some = best_in.at[pl.ds(0, count)]
                send(some, some, far_sent.at[e], far_landed, across(here, 1)).wait_send()

    sent = sum(wanted.astype(jnp.int32) for wanted, _ in backs)
    for count in range(4, PLANES):

        @pl.when(sent == count)
        def _():
            some = back_out.at[pl.ds(0, count)]
            send(some, some, back_sent, back_landed, across(here, 1)).wait_send()

    first = is_first(z, y, x)

    @pl.when(jnp.logical_not(first))
    def _():
        with scope("back_wait"):
            send(back_in.at[steps], back_in.at[steps], back_sent, back_landed, across(here, 1)).wait_recv()

    @pl.when(first)
    def _():
        with scope("far_wait"):
            send(far_in.at[steps], far_in.at[steps], far_sent.at[0], far_landed, across(here, 1)).wait_recv()
        for s in range(1, PLANES):
            tiles = far_in[s].reshape(PEERS, SLOTS)
            back_in[s] = jnp.sum(jnp.where(lanes // CAP == peers, tiles, 0.0), axis=0, keepdims=True)

    with scope("final"):
        slot = jnp.concatenate(slot_rows * 2, axis=0)
        found = jnp.zeros((2 * BLOCKS, 128), jnp.float32)
        for s in range(PLANES):
            row = jnp.broadcast_to(back_in[s], (2 * BLOCKS, SLOTS))
            picked = jnp.take_along_axis(row, slot & (SLOTS - 1), axis=1)
            found = jnp.where(slot >> 7 == s, picked, found)
        out_ref[...] = found[:BLOCKS]


def exchange(room, number, vmem, embeddings, cluster_ids, ranks):
    dma = pltpu.SemaphoreType.DMA
    return pl.pallas_call(
        functools.partial(kernel, room),
        out_shape=(
            jax.ShapeDtypeStruct((BLOCKS, 128), jnp.float32),
            jax.ShapeDtypeStruct((1,), jnp.int32),
        ),
        in_specs=[
            pl.BlockSpec(memory_space=pltpu.HBM),
            pl.BlockSpec(memory_space=pltpu.HBM),
            pl.BlockSpec(memory_space=pltpu.HBM),
        ],
        out_specs=(pl.BlockSpec(memory_space=pltpu.VMEM), pl.BlockSpec(memory_space=pltpu.HBM)),
        scratch_shapes=[
            pltpu.SMEM((1,), jnp.int32),
            pltpu.VMEM((ROWS_DEV, WIDTH), jnp.bfloat16),
            pltpu.VMEM((BLOCKS, 128), jnp.int32),
            pltpu.VMEM((BLOCKS, 128), jnp.int32),
            pltpu.VMEM((ROWS_DEV, WIDTH), jnp.bfloat16),
            pltpu.VMEM((PLANES, 2, SLOTS), jnp.float32),
            pltpu.VMEM((PLANES, 2, SLOTS), jnp.float32),
            pltpu.VMEM((PLANES, room, WIDTH), jnp.bfloat16),
            pltpu.VMEM((PLANES, room, WIDTH), jnp.bfloat16),
            pltpu.VMEM((PLANES, PEERS, CAP, WIDTH), jnp.bfloat16),
            pltpu.VMEM((PLANES, PEERS, CAP, WIDTH), jnp.bfloat16),
            pltpu.VMEM((PLANES * SLOTS, WIDTH), jnp.bfloat16),
            pltpu.VMEM((PLANES, SLOTS), jnp.float32),
            pltpu.VMEM((PEERS, PLANES, SLOTS), jnp.float32),
            pltpu.VMEM((PEERS, 1, SLOTS), jnp.float32),
            pltpu.VMEM((PLANES, 1, SLOTS), jnp.float32),
            pltpu.VMEM((PEERS, 1, SLOTS), jnp.float32),
            pltpu.VMEM((PLANES, PEERS, 1, SLOTS), jnp.float32),
            pltpu.VMEM((PLANES, 1, SLOTS), jnp.float32),
            pltpu.VMEM((PLANES, 1, SLOTS), jnp.float32),
            dma, dma, dma,
            dma, dma((2,)),
            dma, dma((PLANES - 1,)),
            dma, dma((PLANES,)),
            dma, dma,
            dma, dma,
            dma((2,)), dma,
            dma, dma,
            pltpu.SemaphoreType.REGULAR((len(ROUNDS),)),
        ],
        compiler_params=pltpu.CompilerParams(
            collective_id=number, has_side_effects=True, vmem_limit_bytes=vmem
        ),
    )(embeddings, cluster_ids, ranks)


def shards(embeddings, cluster_ids, ranks):
    given = embeddings, cluster_ids.reshape(BLOCKS, 128), ranks.reshape(BLOCKS, 128)
    nearest, over = exchange(ROOM, 0, 40 << 20, *given)
    nearest = lax.switch(over[0], (lambda best: best, lambda best: exchange(SLOTS, 1, 67043328, *given)[0]), nearest)
    return nearest.reshape(ROWS_DEV)


def solution(mesh):
    return jax.shard_map(
        shards,
        mesh=mesh,
        in_specs=(
            P(("loader", "split"), None),
            P(("loader", "split"), None),
            P(("loader", "split")),
        ),
        out_specs=P(("loader", "split")),
        check_vma=False,
    )
```

```python
import functools

import jax
import jax.numpy as jnp
from jax import lax
from jax.experimental import pallas as pl
from jax.experimental.pallas import tpu as pltpu
from jax.sharding import PartitionSpec as P

MESH = pl.DeviceIdType.MESH
scope = jax.named_scope
CLUSTERS = 256
CAP = 4
WIDTH = 768
ROWS_DEV = 512
PLANES = 8
PEERS = 32
SLOTS = PEERS * CAP
BLOCKS = ROWS_DEV // 128
ROOM = 80
EMPTY = float(1 << 17)
GROUPS = ((0,), (1, 7), (2, 6), (5, 3), (4,))
ORDER = sum(GROUPS[1:], ())
epsilon = 1e-06


def place():
    row = lax.axis_index("loader")
    y = lax.axis_index("split")
    return lax.div(row, 8), y, lax.rem(lax.div(row, 2), 4), lax.rem(row, 2)


def device(z, y, x, c):
    return ((z * 4 + x) * 2 + c, y)


def across(here, s):
    z, y, x, c = here
    return device(lax.rem(z + s, PLANES), y, x, c)


def within(here, j, sign):
    z, y, x, c = here
    dy, dx, dc = j % 4, j // 4 % 4, j // 16
    return device(
        z,
        lax.rem(y + (4 + sign * dy) % 4, 4),
        lax.rem(x + (4 + sign * dx) % 4, 4),
        lax.rem(c + dc, 2),
    )


def hops(j):
    return min(j % 4, 4 - j % 4) + min(j // 4 % 4, 4 - j // 4 % 4)


FIRST = [(z, y, x) for z in range(3) for y in range(4) for x in range(4) if z + min(y, 4 - y) + min(x, 4 - x) <= 2]
BESIDE = (1, 3, 4, 12, 16)
CLOSE = (1, 7)
ROUNDS = ((1, 3), (4, 12), (4, 12), (16,))
FAR_FIRST = sorted(range(1, PEERS), key=lambda j: -hops(j))


def is_first(z, y, x):
    return z + jnp.minimum(y, 4 - y) + jnp.minimum(x, 4 - x) <= 2


def send(src, dst, sent, landed, to):
    return pltpu.make_async_remote_copy(
        src_ref=src,
        dst_ref=dst,
        send_sem=sent,
        recv_sem=landed,
        device_id=to,
        device_id_type=MESH,
    )


def product(a, b):
    return lax.dot_general(
        a, b, (((1,), (1,)), ((), ())), preferred_element_type=jnp.float32
    )


def iota(shape, dim):
    return lax.broadcasted_iota(jnp.int32, shape, dim)


def own_lanes(tiles_ref):
    group = iota((PLANES, SLOTS), 1) // CAP
    total = jnp.zeros((PLANES, SLOTS), jnp.float32)
    for j in range(PEERS):
        total = jnp.where(group == j, tiles_ref[j], total)
    return total


def kernel(
    room, emb_hbm, cid_hbm, rank_hbm, out_ref, flag_hbm, flag_ref,
    raw, cid_ref, rank_ref, meta_out, meta_in, rows_out, rows_in, dense, arrived, members,
    ranks_out, ranks_in, best_out, best_rows, best_in, far_in, back_out, back_in,
    raw_sem, cid_sem, rank_sem, meta_sent, meta_landed, rows_sent, rows_landed, dense_sent, dense_landed,
    ranks_sent, ranks_landed, best_sent, best_landed, far_sent, far_landed, back_sent, back_landed, linked, met,
):
    here = place()
    z, y, x, c = here
    load_cid = pltpu.make_async_copy(cid_hbm, cid_ref, cid_sem)
    load_cid.start()
    load = pltpu.make_async_copy(emb_hbm, raw, raw_sem)
    load.start()
    load_rank = pltpu.make_async_copy(rank_hbm, rank_ref, rank_sem)
    load_rank.start()
    with scope("greet"):
        barrier = pltpu.get_barrier_semaphore()
        for s in CLOSE:
            pl.semaphore_signal(barrier, inc=1, device_id=across(here, s), device_id_type=MESH)
        for j in BESIDE:
            pl.semaphore_signal(barrier, inc=1, device_id=within(here, j, 1), device_id_type=MESH)

    def tell(n):
        for j in ROUNDS[n]:
            pl.semaphore_signal(met.at[n], inc=1, device_id=within(here, j, 1), device_id_type=MESH)

    def hear(n):
        with scope(f"hear#n={n}"):
            pl.semaphore_wait(met.at[n], len(ROUNDS[n]))

    def tell_across(n):
        for s in (1, PLANES - 1):
            pl.semaphore_signal(linked.at[n], inc=1, device_id=across(here, s), device_id_type=MESH)

    def hear_across(n):
        with scope(f"hear_across#n={n}"):
            pl.semaphore_wait(linked.at[n], 2)

    with scope("count"):
        load_cid.wait()
        cid = cid_ref[...]
        owner = cid & (PEERS - 1)
        step = ((cid >> 5) - z) & (PLANES - 1)
        turned = jnp.concatenate([cid, step], axis=0).T
        before = iota((128, 128), 0) < iota((128, 128), 1)
        pack_rows, over = [], jnp.zeros((1, 128), jnp.float32)
        for b in range(BLOCKS):
            along = jnp.zeros((128, 128), jnp.float32)
            for a in range(b + 1):
                aside = turned[:, BLOCKS + a : BLOCKS + a + 1] == step[b : b + 1]
                along += jnp.where(aside & before if a == b else aside, 1.0, 0.0)
            count = jnp.sum(along, axis=0, keepdims=True).astype(jnp.int32)
            pack_rows.append(jnp.where(count < room, step[b : b + 1] * SLOTS + count, -1))
            over = jnp.maximum(over, jnp.where(count < room, 0.0, 2 * EMPTY))
        pack = jnp.concatenate(pack_rows, axis=1)
    with scope("load"):
        load.wait()

    rows = {
        s: send(rows_out.at[s], rows_in.at[s], rows_sent, rows_landed.at[s - 1], across(here, s))
        for s in range(1, PLANES)
    }
    metas = {
        s: send(meta_out.at[s], meta_in.at[s], meta_sent, meta_landed.at[0 if s in GROUPS[1] else 2 if s in GROUPS[4] else 1], across(here, s))
        for s in range(1, PLANES)
    }

    def gather_rows(group):
        chosen = jnp.concatenate(
            [jnp.where(pack == s * SLOTS + iota((room, ROWS_DEV), 0), 1.0, 0.0) for s in group], axis=0
        ).astype(jnp.bfloat16)
        picked = jnp.dot(chosen, raw[...], preferred_element_type=jnp.float32)
        scale = lax.rsqrt(jnp.sum(picked * picked, axis=1, keepdims=True) + epsilon)
        packed = (picked * scale).astype(jnp.bfloat16)
        for n, s in enumerate(group):
            ref = rows_in if s == 0 else rows_out
            ref[s] = packed[n * room : (n + 1) * room]

    with scope("pack"):
        gather_rows(GROUPS[1])
    with scope("barrier_wait"):
        pl.semaphore_wait(barrier, len(CLOSE) + len(BESIDE))
    pl.when(z == 1)(lambda: pl.delay(800))
    pl.when(z == 2)(lambda: pl.delay(1200))
    for s in GROUPS[1]:
        rows[s].start()
    tell_across(0)
    tell(0)

    with scope("slots"):
        peer = (
            (((owner >> 4) - c) & 1) * 16 + (((owner >> 2) - x) & 3) * 4 + ((owner - y) & 3)
        )
        slot_rows = []
        for b in range(BLOCKS):
            same = jnp.zeros((128, 128), jnp.float32)
            for a in range(b + 1):
                alike = turned[:, a : a + 1] == cid[b : b + 1]
                same += jnp.where(alike & before if a == b else alike, 1.0, 0.0)
            position = jnp.sum(same, axis=0, keepdims=True).astype(jnp.int32)
            slot_rows.append(step[b : b + 1] * SLOTS + peer[b : b + 1] * CAP + position)
    hear_across(0)
    tell_across(1)
    hear(0)
    tell(1)
    with scope("names"):
        over = jnp.max(over, axis=1, keepdims=True)
        slot_turned = jnp.concatenate(slot_rows + pack_rows, axis=0).T
        load_rank.wait()
        rank_turned = (rank_ref[...].astype(jnp.float32) - EMPTY).T
        lane = iota((128, 128), 1)
        for s in range(PLANES):
            name = jnp.zeros((128, 128), jnp.float32)
            rank = jnp.zeros((128, 128), jnp.float32)
            for b in range(BLOCKS):
                slots = slot_turned[:, b : b + 1]
                packs = slot_turned[:, BLOCKS + b : BLOCKS + b + 1]
                name = jnp.where(packs == s * SLOTS + lane, (slots - (s * SLOTS - 1)).astype(jnp.float32), name)
                rank = jnp.where(slots == s * SLOTS + lane, rank_turned[:, b : b + 1], rank)
            ref = meta_in if s == 0 else meta_out
            ref[s, 0:1] = jnp.sum(name, axis=0, keepdims=True) - 1.0
            ref[s, 1:2] = jnp.sum(rank, axis=0, keepdims=True) + (EMPTY + over)
    with scope("pack_rest"):
        gather_rows(GROUPS[2])
    hear_across(1)
    tell_across(2)
    for s in GROUPS[1] + GROUPS[2] + GROUPS[3]:
        metas[s].start()
    for s in GROUPS[2]:
        rows[s].start()
    hear(1)
    tell(2)
    with scope("pack_rest"):
        gather_rows(GROUPS[3])
    with scope("pack_rest"):
        gather_rows(GROUPS[4] + GROUPS[0])
    hear_across(2)
    for s in GROUPS[4]:
        metas[s].start()
    hear(2)
    tell(3)
    hear(3)

    others = pl.ds(1, PEERS - 1)

    def spread(s):
        with scope(f"place#s={s}"):
            chosen = jnp.where(
                meta_in[s, 0:1, :room] == iota((SLOTS, room), 0).astype(jnp.float32), 1.0, 0.0
            ).astype(jnp.bfloat16)
            placed = jnp.dot(chosen, rows_in[s], preferred_element_type=jnp.float32).astype(jnp.bfloat16)
            dense[s] = placed.reshape(PEERS, CAP, WIDTH)
            arrived[s, 0] = placed[:CAP]
        with scope(f"deliver#s={s}"):
            for j in FAR_FIRST:
                send(dense.at[s, j], arrived.at[s, j], dense_sent, dense_landed.at[s], within(here, j, 1)).start()

    def all_dense(s):
        return send(dense.at[s, others], arrived.at[s, others], dense_sent, dense_landed.at[s], within(here, 1, 1))

    all_ranks = send(ranks_in.at[others], ranks_in.at[others], ranks_sent, ranks_landed, within(here, 1, 1))
    all_best = send(best_in.at[others], best_in.at[others], best_sent, best_landed, within(here, 1, 1))

    spread(0)
    def metas_in(n, count):
        some = meta_in.at[pl.ds(0, count)]
        return send(some, some, meta_sent, meta_landed.at[n], across(here, 1))

    metas_in(0, len(GROUPS[1])).wait_recv()
    for s in GROUPS[1]:
        with scope(f"rows_wait#s={s}"):
            rows[s].wait_recv()
    for s in GROUPS[3]:
        rows[s].start()
    for s in GROUPS[1]:
        spread(s)
    with scope("meta_wait"):
        metas_in(1, len(GROUPS[2] + GROUPS[3])).wait_recv()
    for s in GROUPS[2]:
        with scope(f"rows_wait#s={s}"):
            rows[s].wait_recv()
        spread(s)
    for s in GROUPS[4]:
        rows[s].start()
    metas_in(2, len(GROUPS[4])).wait_recv()
    for s in range(PLANES):
        ranks_out[s : s + 1] = meta_in[s, 1:2]
    ranks_in[0] = ranks_out[...]
    for j in FAR_FIRST:
        send(ranks_out, ranks_in.at[j], ranks_sent, ranks_landed, within(here, j, 1)).start()

    best = [jnp.full((1, SLOTS), -1.0, jnp.float32)] * PLANES
    seen = []

    def compare(group):
        known = len(seen)
        for s in group:
            with scope(f"dense_wait#s={s}"):
                all_dense(s).wait_recv()
            members[len(seen) * SLOTS : (len(seen) + 1) * SLOTS] = arrived[s].reshape(SLOTS, WIDTH)
            seen.append(s)
        with scope(f"scores#n={len(seen)}"):
            scores = product(members[known * SLOTS : len(seen) * SLOTS], members[: len(seen) * SLOTS])

            def part(n, k):
                return scores[n * SLOTS : (n + 1) * SLOTS, k * SLOTS : (k + 1) * SLOTS]

            for k, q in enumerate(seen):
                top = jnp.full((SLOTS, SLOTS), -1.0, jnp.float32)
                for n, m in enumerate(group):
                    earlier = rank_col[:, m : m + 1] < rank_row[q : q + 1]
                    top = jnp.maximum(top, jnp.where(earlier, part(n, k), -1.0))
                best[q] = jnp.maximum(best[q], jnp.max(top, axis=0, keepdims=True))
            for n, q in enumerate(group):
                if known:
                    top = jnp.full((SLOTS, SLOTS), -1.0, jnp.float32)
                    for k, m in enumerate(seen[:known]):
                        earlier = rank_row[m : m + 1] < rank_col[:, q : q + 1]
                        top = jnp.maximum(top, jnp.where(earlier, part(n, k), -1.0))
                    best[q] = jnp.maximum(best[q], jnp.max(top.T, axis=0, keepdims=True))

    for s in GROUPS[3]:
        with scope(f"rows_wait#s={s}"):
            rows[s].wait_recv()
        spread(s)
    for s in GROUPS[4]:
        with scope(f"rows_wait#s={s}"):
            rows[s].wait_recv()
        spread(s)
    with scope("ranks_wait"):
        all_ranks.wait_recv()
    rank_row = own_lanes(ranks_in)
    rank_col = rank_row.T
    highest = jnp.zeros((PLANES, SLOTS), jnp.float32)
    for j in range(PEERS):
        highest = jnp.maximum(highest, ranks_in[j])
    flag_ref[0] = jnp.max(jnp.where(highest >= 2 * EMPTY, 1, 0))
    save_flag = pltpu.make_async_copy(flag_ref, flag_hbm, cid_sem)
    save_flag.start()

    compare(GROUPS[0])
    compare(GROUPS[1])
    compare(GROUPS[2])
    for s in GROUPS[3] + GROUPS[4]:
        compare((s,))

    lanes, peers = iota((PEERS, SLOTS), 1), iota((PEERS, SLOTS), 0)
    straight = []
    for a, b, d, e in [(*chip, core) for chip in FIRST for core in (1, 0)]:
        up, j = lax.rem(z - a + PLANES, PLANES), lax.rem(c + e, 2) * 16 + lax.rem(x - d + 4, 4) * 4 + lax.rem(y - b + 4, 4)
        straight.append((up, send(best_rows.at[up], far_in.at[up, j], far_sent.at[e], far_landed, device(a, b, d, e))))
    with scope("answer"):
        for s in range(PLANES):
            best_rows[s] = best[s]
        for up, copy in straight:
            pl.when(up != 0)(copy.start)
        answers = jnp.zeros((PEERS, SLOTS), jnp.float32)
        for s in range(PLANES):
            line = jnp.broadcast_to(best[s], (PEERS, SLOTS))
            picked = jnp.take_along_axis(line, CAP * peers + (lanes & (CAP - 1)), axis=1)
            answers = jnp.where(lanes // CAP == s, picked, answers)
        best_out[...] = answers.reshape(PEERS, 1, SLOTS)
        for j in FAR_FIRST:
            send(best_out.at[j], best_in.at[j], best_sent, best_landed, within(here, j, -1)).start()
    best_in[0] = best_out[0]
    metas_in(0, PLANES - 1).wait_send()
    steps = pl.ds(1, PLANES - 1)
    send(rows_out.at[steps], rows_out.at[steps], rows_sent, rows_landed.at[0], across(here, 1)).wait_send()
    send(dense.at[:, others], dense.at[:, others], dense_sent, dense_landed.at[0], across(here, 1)).wait_send()
    all_ranks.wait_send()
    save_flag.wait()
    with scope("best_wait"):
        all_best.wait_recv()
    with scope("back"):
        answers = best_in[...].reshape(PEERS, SLOTS)
        backs = []
        for s in (4, 3, 5, 2, 6, 1, 7, 0):
            picked = jnp.take_along_axis(answers, CAP * s + (lanes & (CAP - 1)), axis=1)
            line = jnp.sum(jnp.where(lanes // CAP == peers, picked, 0.0), axis=0, keepdims=True)
            if s == 0:
                back_in[0] = line
                continue
            back_out[s] = line
            back = send(back_out.at[s], back_in.at[s], back_sent, back_landed, across(here, PLANES - s))
            wanted = jnp.logical_not(is_first(lax.rem(z + PLANES - s, PLANES), y, x))
            pl.when(wanted)(back.start)
            backs.append((wanted, back))
    all_best.wait_send()
    for a in range(PLANES):
        count = len([chip for chip in FIRST if chip[0] != a])

        @pl.when(z == a)
        def _():
            for e in range(2):
                some = best_in.at[pl.ds(0, count)]
                send(some, some, far_sent.at[e], far_landed, across(here, 1)).wait_send()

    sent = sum(wanted.astype(jnp.int32) for wanted, _ in backs)
    for count in range(4, PLANES):

        @pl.when(sent == count)
        def _():
            some = back_out.at[pl.ds(0, count)]
            send(some, some, back_sent, back_landed, across(here, 1)).wait_send()

    first = is_first(z, y, x)

    @pl.when(jnp.logical_not(first))
    def _():
        with scope("back_wait"):
            send(back_in.at[steps], back_in.at[steps], back_sent, back_landed, across(here, 1)).wait_recv()

    @pl.when(first)
    def _():
        with scope("far_wait"):
            send(far_in.at[steps], far_in.at[steps], far_sent.at[0], far_landed, across(here, 1)).wait_recv()
        for s in range(1, PLANES):
            tiles = far_in[s].reshape(PEERS, SLOTS)
            back_in[s] = jnp.sum(jnp.where(lanes // CAP == peers, tiles, 0.0), axis=0, keepdims=True)

    with scope("final"):
        slot = jnp.concatenate(slot_rows * 2, axis=0)
        found = jnp.zeros((2 * BLOCKS, 128), jnp.float32)
        for s in range(PLANES):
            row = jnp.broadcast_to(back_in[s], (2 * BLOCKS, SLOTS))
            picked = jnp.take_along_axis(row, slot & (SLOTS - 1), axis=1)
            found = jnp.where(slot >> 7 == s, picked, found)
        out_ref[...] = found[:BLOCKS]


def exchange(room, number, vmem, embeddings, cluster_ids, ranks):
    dma = pltpu.SemaphoreType.DMA
    return pl.pallas_call(
        functools.partial(kernel, room),
        out_shape=(
            jax.ShapeDtypeStruct((BLOCKS, 128), jnp.float32),
            jax.ShapeDtypeStruct((1,), jnp.int32),
        ),
        in_specs=[
            pl.BlockSpec(memory_space=pltpu.HBM),
            pl.BlockSpec(memory_space=pltpu.HBM),
            pl.BlockSpec(memory_space=pltpu.HBM),
        ],
        out_specs=(pl.BlockSpec(memory_space=pltpu.VMEM), pl.BlockSpec(memory_space=pltpu.HBM)),
        scratch_shapes=[
            pltpu.SMEM((1,), jnp.int32),
            pltpu.VMEM((ROWS_DEV, WIDTH), jnp.bfloat16),
            pltpu.VMEM((BLOCKS, 128), jnp.int32),
            pltpu.VMEM((BLOCKS, 128), jnp.int32),
            pltpu.VMEM((PLANES, 2, SLOTS), jnp.float32),
            pltpu.VMEM((PLANES, 2, SLOTS), jnp.float32),
            pltpu.VMEM((PLANES, room, WIDTH), jnp.bfloat16),
            pltpu.VMEM((PLANES, room, WIDTH), jnp.bfloat16),
            pltpu.VMEM((PLANES, PEERS, CAP, WIDTH), jnp.bfloat16),
            pltpu.VMEM((PLANES, PEERS, CAP, WIDTH), jnp.bfloat16),
            pltpu.VMEM((PLANES * SLOTS, WIDTH), jnp.bfloat16),
            pltpu.VMEM((PLANES, SLOTS), jnp.float32),
            pltpu.VMEM((PEERS, PLANES, SLOTS), jnp.float32),
            pltpu.VMEM((PEERS, 1, SLOTS), jnp.float32),
            pltpu.VMEM((PLANES, 1, SLOTS), jnp.float32),
            pltpu.VMEM((PEERS, 1, SLOTS), jnp.float32),
            pltpu.VMEM((PLANES, PEERS, 1, SLOTS), jnp.float32),
            pltpu.VMEM((PLANES, 1, SLOTS), jnp.float32),
            pltpu.VMEM((PLANES, 1, SLOTS), jnp.float32),
            dma, dma, dma,
            dma, dma((3,)),
            dma, dma((PLANES - 1,)),
            dma, dma((PLANES,)),
            dma, dma,
            dma, dma,
            dma((2,)), dma,
            dma, dma,
            pltpu.SemaphoreType.REGULAR((3,)),
            pltpu.SemaphoreType.REGULAR((len(ROUNDS),)),
        ],
        compiler_params=pltpu.CompilerParams(
            collective_id=number, has_side_effects=True, vmem_limit_bytes=vmem
        ),
    )(embeddings, cluster_ids, ranks)


def shards(embeddings, cluster_ids, ranks):
    given = embeddings, cluster_ids.reshape(BLOCKS, 128), ranks.reshape(BLOCKS, 128)
    nearest, over = exchange(ROOM, 0, 40 << 20, *given)
    nearest = lax.switch(over[0], (lambda best: best, lambda best: exchange(SLOTS, 1, 67043328, *given)[0]), nearest)
    return nearest.reshape(ROWS_DEV)


def solution(mesh):
    return jax.shard_map(
        shards,
        mesh=mesh,
        in_specs=(
            P(("loader", "split"), None),
            P(("loader", "split"), None),
            P(("loader", "split")),
        ),
        out_specs=P(("loader", "split")),
        check_vma=False,
    )
```

```python
import functools

import jax
import jax.numpy as jnp
from jax import lax
from jax.experimental import pallas as pl
from jax.experimental.pallas import tpu as pltpu
from jax.sharding import PartitionSpec as P

MESH = pl.DeviceIdType.MESH
scope = jax.named_scope
CLUSTERS = 256
CAP = 4
WIDTH = 768
ROWS_DEV = 512
PLANES = 8
PEERS = 32
SLOTS = PEERS * CAP
BLOCKS = ROWS_DEV // 128
ROOM = 80
EMPTY = float(1 << 17)
GROUPS = ((0,), (1, 7), (2, 6), (5, 3), (4,))
ORDER = sum(GROUPS[1:], ())
TOGETHER = (GROUPS[0] + GROUPS[1], GROUPS[2]) + tuple((s,) for s in GROUPS[3] + GROUPS[4])
SHARED = {s: n for n, steps in enumerate(TOGETHER) for s in steps}
epsilon = 1e-06


def place():
    row = lax.axis_index("loader")
    y = lax.axis_index("split")
    return lax.div(row, 8), y, lax.rem(lax.div(row, 2), 4), lax.rem(row, 2)


def device(z, y, x, c):
    return ((z * 4 + x) * 2 + c, y)


def across(here, s):
    z, y, x, c = here
    return device(lax.rem(z + s, PLANES), y, x, c)


def within(here, j, sign):
    z, y, x, c = here
    dy, dx, dc = j % 4, j // 4 % 4, j // 16
    return device(
        z,
        lax.rem(y + (4 + sign * dy) % 4, 4),
        lax.rem(x + (4 + sign * dx) % 4, 4),
        lax.rem(c + dc, 2),
    )


def hops(j):
    return min(j % 4, 4 - j % 4) + min(j // 4 % 4, 4 - j // 4 % 4)


FIRST = [(z, y, x) for z in range(3) for y in range(4) for x in range(4) if z + min(y, 4 - y) + min(x, 4 - x) <= 2]
BESIDE = (1, 3, 4, 12, 16)
CLOSE = (1, 7)
ROUNDS = ((1, 3), (4, 12), (4, 12), (16,))
FAR_FIRST = sorted(range(1, PEERS), key=lambda j: -hops(j))


def is_first(z, y, x):
    return z + jnp.minimum(y, 4 - y) + jnp.minimum(x, 4 - x) <= 2


def send(src, dst, sent, landed, to):
    return pltpu.make_async_remote_copy(
        src_ref=src,
        dst_ref=dst,
        send_sem=sent,
        recv_sem=landed,
        device_id=to,
        device_id_type=MESH,
    )


def product(a, b):
    return lax.dot_general(
        a, b, (((1,), (1,)), ((), ())), preferred_element_type=jnp.float32
    )


def iota(shape, dim):
    return lax.broadcasted_iota(jnp.int32, shape, dim)


def own_lanes(tiles_ref):
    group = iota((PLANES, SLOTS), 1) // CAP
    total = jnp.zeros((PLANES, SLOTS), jnp.float32)
    for j in range(PEERS):
        total = jnp.where(group == j, tiles_ref[j], total)
    return total


def kernel(
    room, emb_hbm, cid_hbm, rank_hbm, out_ref, flag_hbm, flag_ref,
    raw, cid_ref, rank_ref, meta_out, meta_in, rows_out, rows_in, dense, arrived, members,
    ranks_out, ranks_in, best_out, best_rows, best_in, far_in, back_out, back_in,
    raw_sem, cid_sem, meta_landed, rows_sent, rows_landed, dense_sent, dense_landed,
    small_sent, ranks_landed, far_sent, far_landed, best_landed, back_landed, linked, met,
):
    here = place()
    z, y, x, c = here
    load_cid = pltpu.make_async_copy(cid_hbm, cid_ref, cid_sem)
    load_cid.start()
    load = pltpu.make_async_copy(emb_hbm, raw, raw_sem)
    load.start()
    with scope("greet"):
        barrier = pltpu.get_barrier_semaphore()
        for s in CLOSE:
            pl.semaphore_signal(barrier, inc=1, device_id=across(here, s), device_id_type=MESH)
        for j in BESIDE:
            pl.semaphore_signal(barrier, inc=1, device_id=within(here, j, 1), device_id_type=MESH)

    def tell(n):
        for j in ROUNDS[n]:
            pl.semaphore_signal(met.at[(0, 1, 0, 2)[n]], inc=1, device_id=within(here, j, 1), device_id_type=MESH)

    def hear(n):
        with scope(f"hear#n={n}"):
            pl.semaphore_wait(met.at[(0, 1, 0, 2)[n]], len(ROUNDS[n]))

    def tell_across(n):
        for s in (1, PLANES - 1):
            pl.semaphore_signal(linked.at[n % 2], inc=1, device_id=across(here, s), device_id_type=MESH)

    def hear_across(n):
        with scope(f"hear_across#n={n}"):
            pl.semaphore_wait(linked.at[n % 2], 2)

    with scope("count"):
        load_cid.wait()
        cid = cid_ref[...]
        owner = cid & (PEERS - 1)
        step = ((cid >> 5) - z) & (PLANES - 1)
        turned = jnp.concatenate([cid, step], axis=0).T
        before = iota((128, 128), 0) < iota((128, 128), 1)
        pack_rows, over = [], jnp.zeros((1, 128), jnp.float32)
        for b in range(BLOCKS):
            along = jnp.zeros((128, 128), jnp.float32)
            for a in range(b + 1):
                aside = turned[:, BLOCKS + a : BLOCKS + a + 1] == step[b : b + 1]
                along += jnp.where(aside & before if a == b else aside, 1.0, 0.0)
            count = jnp.sum(along, axis=0, keepdims=True).astype(jnp.int32)
            pack_rows.append(jnp.where(count < room, step[b : b + 1] * SLOTS + count, -1))
            over = jnp.maximum(over, jnp.where(count < room, 0.0, 2 * EMPTY))
        pack = jnp.concatenate(pack_rows, axis=1)
    load_rank = pltpu.make_async_copy(rank_hbm, rank_ref, cid_sem)
    load_rank.start()
    with scope("load"):
        load.wait()

    rows = {
        s: send(rows_out.at[s], rows_in.at[s], rows_sent, rows_landed.at[0 if s in GROUPS[1] else ORDER.index(s) - 1], across(here, s))
        for s in range(1, PLANES)
    }
    metas = {
        s: send(meta_out.at[s], meta_in.at[s], small_sent, meta_landed.at[0 if s in GROUPS[1] else 2 if s in GROUPS[4] else 1], across(here, s))
        for s in range(1, PLANES)
    }

    def gather_rows(group):
        chosen = jnp.concatenate(
            [jnp.where(pack == s * SLOTS + iota((room, ROWS_DEV), 0), 1.0, 0.0) for s in group], axis=0
        ).astype(jnp.bfloat16)
        picked = jnp.dot(chosen, raw[...], preferred_element_type=jnp.float32)
        scale = lax.rsqrt(jnp.sum(picked * picked, axis=1, keepdims=True) + epsilon)
        packed = (picked * scale).astype(jnp.bfloat16)
        for n, s in enumerate(group):
            ref = rows_in if s == 0 else rows_out
            ref[s] = packed[n * room : (n + 1) * room]

    with scope("pack"):
        gather_rows(GROUPS[1])
    with scope("barrier_wait"):
        pl.semaphore_wait(barrier, len(CLOSE) + len(BESIDE))
    pl.when(z == 1)(lambda: pl.delay(800))
    pl.when(z == 2)(lambda: pl.delay(1200))
    for s in GROUPS[1]:
        rows[s].start()
    tell_across(0)
    tell(0)

    with scope("slots"):
        peer = (
            (((owner >> 4) - c) & 1) * 16 + (((owner >> 2) - x) & 3) * 4 + ((owner - y) & 3)
        )
        slot_rows = []
        for b in range(BLOCKS):
            same = jnp.zeros((128, 128), jnp.float32)
            for a in range(b + 1):
                alike = turned[:, a : a + 1] == cid[b : b + 1]
                same += jnp.where(alike & before if a == b else alike, 1.0, 0.0)
            position = jnp.sum(same, axis=0, keepdims=True).astype(jnp.int32)
            slot_rows.append(step[b : b + 1] * SLOTS + peer[b : b + 1] * CAP + position)
    hear_across(0)
    tell_across(1)
    hear(0)
    tell(1)
    with scope("names"):
        over = jnp.max(over, axis=1, keepdims=True)
        slot_turned = jnp.concatenate(slot_rows + pack_rows, axis=0).T
        load_rank.wait()
        rank_turned = (rank_ref[...].astype(jnp.float32) - EMPTY).T
        lane = iota((128, 128), 1)
        for s in range(PLANES):
            name = jnp.zeros((128, 128), jnp.float32)
            rank = jnp.zeros((128, 128), jnp.float32)
            for b in range(BLOCKS):
                slots = slot_turned[:, b : b + 1]
                packs = slot_turned[:, BLOCKS + b : BLOCKS + b + 1]
                name = jnp.where(packs == s * SLOTS + lane, (slots - (s * SLOTS - 1)).astype(jnp.float32), name)
                rank = jnp.where(slots == s * SLOTS + lane, rank_turned[:, b : b + 1], rank)
            ref = meta_in if s == 0 else meta_out
            ref[s, 0:1] = jnp.sum(name, axis=0, keepdims=True) - 1.0
            ref[s, 1:2] = jnp.sum(rank, axis=0, keepdims=True) + (EMPTY + over)
    with scope("pack_rest"):
        gather_rows(GROUPS[2])
    hear_across(1)
    tell_across(2)
    for s in GROUPS[1] + GROUPS[2] + GROUPS[3]:
        metas[s].start()
    for s in GROUPS[2]:
        rows[s].start()
    hear(1)
    tell(2)
    with scope("pack_rest"):
        gather_rows(GROUPS[3])
    with scope("pack_rest"):
        gather_rows(GROUPS[4] + GROUPS[0])
    hear_across(2)
    for s in GROUPS[4]:
        metas[s].start()
    with scope("rows_wait#s=1"):
        first_two = rows_in.at[pl.ds(0, len(GROUPS[1]))]
        send(first_two, first_two, rows_sent, rows_landed.at[0], across(here, 1)).wait_recv()
    for s in GROUPS[3]:
        rows[s].start()
    hear(2)
    tell(3)
    hear(3)

    others = pl.ds(1, PEERS - 1)

    def spread(s):
        with scope(f"place#s={s}"):
            chosen = jnp.where(
                meta_in[s, 0:1, :room] == iota((SLOTS, room), 0).astype(jnp.float32), 1.0, 0.0
            ).astype(jnp.bfloat16)
            placed = jnp.dot(chosen, rows_in[s], preferred_element_type=jnp.float32).astype(jnp.bfloat16)
            dense[s] = placed.reshape(PEERS, CAP, WIDTH)
            arrived[s, 0] = placed[:CAP]
        with scope(f"deliver#s={s}"):
            for j in FAR_FIRST:
                send(dense.at[s, j], arrived.at[s, j], dense_sent, dense_landed.at[SHARED[s]], within(here, j, 1)).start()

    def all_dense(n):
        some = arrived.at[pl.ds(0, len(TOGETHER[n])), others]
        return send(some, some, dense_sent, dense_landed.at[n], within(here, 1, 1))

    all_ranks = send(ranks_in.at[others], ranks_in.at[others], small_sent, ranks_landed, within(here, 1, 1))
    all_best = send(best_in.at[others], best_in.at[others], small_sent, best_landed, within(here, 1, 1))

    spread(0)
    def metas_in(n, count):
        some = meta_in.at[pl.ds(0, count)]
        return send(some, some, small_sent, meta_landed.at[n], across(here, 1))

    metas_in(0, len(GROUPS[1])).wait_recv()
    for s in GROUPS[1]:
        spread(s)
    with scope("meta_wait"):
        metas_in(1, len(GROUPS[2] + GROUPS[3])).wait_recv()
    for s in GROUPS[2]:
        with scope(f"rows_wait#s={s}"):
            rows[s].wait_recv()
        spread(s)
    for s in GROUPS[4]:
        rows[s].start()
    metas_in(2, len(GROUPS[4])).wait_recv()
    metas_in(0, PLANES - 1).wait_send()
    for s in range(PLANES):
        ranks_out[s : s + 1] = meta_in[s, 1:2]
    ranks_in[0] = ranks_out[...]
    for j in FAR_FIRST:
        send(ranks_out, ranks_in.at[j], small_sent, ranks_landed, within(here, j, 1)).start()

    best = [jnp.full((1, SLOTS), -1.0, jnp.float32)] * PLANES
    seen = []

    def compare(group):
        known = len(seen)
        for s in group:
            if s == TOGETHER[SHARED[s]][0]:
                with scope(f"dense_wait#s={s}"):
                    all_dense(SHARED[s]).wait_recv()
            members[len(seen) * SLOTS : (len(seen) + 1) * SLOTS] = arrived[s].reshape(SLOTS, WIDTH)
            seen.append(s)
        with scope(f"scores#n={len(seen)}"):
            scores = product(members[known * SLOTS : len(seen) * SLOTS], members[: len(seen) * SLOTS])

            def part(n, k):
                return scores[n * SLOTS : (n + 1) * SLOTS, k * SLOTS : (k + 1) * SLOTS]

            for k, q in enumerate(seen):
                top = jnp.full((SLOTS, SLOTS), -1.0, jnp.float32)
                for n, m in enumerate(group):
                    earlier = rank_col[:, m : m + 1] < rank_row[q : q + 1]
                    top = jnp.maximum(top, jnp.where(earlier, part(n, k), -1.0))
                best[q] = jnp.maximum(best[q], jnp.max(top, axis=0, keepdims=True))
            for n, q in enumerate(group):
                if known:
                    top = jnp.full((SLOTS, SLOTS), -1.0, jnp.float32)
                    for k, m in enumerate(seen[:known]):
                        earlier = rank_row[m : m + 1] < rank_col[:, q : q + 1]
                        top = jnp.maximum(top, jnp.where(earlier, part(n, k), -1.0))
                    best[q] = jnp.maximum(best[q], jnp.max(top.T, axis=0, keepdims=True))

    for s in GROUPS[3]:
        with scope(f"rows_wait#s={s}"):
            rows[s].wait_recv()
        spread(s)
    for s in GROUPS[4]:
        with scope(f"rows_wait#s={s}"):
            rows[s].wait_recv()
        spread(s)
    with scope("ranks_wait"):
        all_ranks.wait_recv()
    rank_row = own_lanes(ranks_in)
    rank_col = rank_row.T
    highest = jnp.zeros((PLANES, SLOTS), jnp.float32)
    for j in range(PEERS):
        highest = jnp.maximum(highest, ranks_in[j])
    flag_ref[0] = jnp.max(jnp.where(highest >= 2 * EMPTY, 1, 0))
    save_flag = pltpu.make_async_copy(flag_ref, flag_hbm, cid_sem)
    save_flag.start()

    compare(GROUPS[0])
    compare(GROUPS[1])
    compare(GROUPS[2])
    for s in GROUPS[3] + GROUPS[4]:
        compare((s,))

    all_ranks.wait_send()

    lanes, peers = iota((PEERS, SLOTS), 1), iota((PEERS, SLOTS), 0)
    straight = []
    for a, b, d, e in [(*chip, core) for chip in FIRST for core in (1, 0)]:
        up, j = lax.rem(z - a + PLANES, PLANES), lax.rem(c + e, 2) * 16 + lax.rem(x - d + 4, 4) * 4 + lax.rem(y - b + 4, 4)
        straight.append((up, send(best_rows.at[up], far_in.at[up, j], far_sent.at[e], far_landed, device(a, b, d, e))))
    with scope("answer"):
        for s in range(PLANES):
            best_rows[s] = best[s]
        for up, copy in straight:
            pl.when(up != 0)(copy.start)
        answers = jnp.zeros((PEERS, SLOTS), jnp.float32)
        for s in range(PLANES):
            line = jnp.broadcast_to(best[s], (PEERS, SLOTS))
            picked = jnp.take_along_axis(line, CAP * peers + (lanes & (CAP - 1)), axis=1)
            answers = jnp.where(lanes // CAP == s, picked, answers)
        best_out[...] = answers.reshape(PEERS, 1, SLOTS)
        for j in FAR_FIRST:
            send(best_out.at[j], best_in.at[j], small_sent, best_landed, within(here, j, -1)).start()
    best_in[0] = best_out[0]
    steps = pl.ds(1, PLANES - 1)
    send(rows_out.at[steps], rows_out.at[steps], rows_sent, rows_landed.at[0], across(here, 1)).wait_send()
    send(dense.at[:, others], dense.at[:, others], dense_sent, dense_landed.at[0], across(here, 1)).wait_send()
    save_flag.wait()
    with scope("best_wait"):
        all_best.wait_recv()
    with scope("back"):
        all_best.wait_send()
        answers = best_in[...].reshape(PEERS, SLOTS)
        backs = []
        for s in (4, 3, 5, 2, 6, 1, 7, 0):
            picked = jnp.take_along_axis(answers, CAP * s + (lanes & (CAP - 1)), axis=1)
            line = jnp.sum(jnp.where(lanes // CAP == peers, picked, 0.0), axis=0, keepdims=True)
            if s == 0:
                back_in[0] = line
                continue
            back_out[s] = line
            back = send(back_out.at[s], back_in.at[s], small_sent, back_landed, across(here, PLANES - s))
            wanted = jnp.logical_not(is_first(lax.rem(z + PLANES - s, PLANES), y, x))
            pl.when(wanted)(back.start)
            backs.append((wanted, back))
    for a in range(PLANES):
        count = len([chip for chip in FIRST if chip[0] != a])

        @pl.when(z == a)
        def _():
            for e in range(2):
                some = best_in.at[pl.ds(0, count)]
                send(some, some, far_sent.at[e], far_landed, across(here, 1)).wait_send()

    sent = sum(wanted.astype(jnp.int32) for wanted, _ in backs)
    for count in range(4, PLANES):

        @pl.when(sent == count)
        def _():
            some = back_out.at[pl.ds(0, count)]
            send(some, some, small_sent, back_landed, across(here, 1)).wait_send()

    first = is_first(z, y, x)

    @pl.when(jnp.logical_not(first))
    def _():
        with scope("back_wait"):
            send(back_in.at[steps], back_in.at[steps], small_sent, back_landed, across(here, 1)).wait_recv()

    @pl.when(first)
    def _():
        with scope("far_wait"):
            send(far_in.at[steps], far_in.at[steps], far_sent.at[0], far_landed, across(here, 1)).wait_recv()
        for s in range(1, PLANES):
            tiles = far_in[s].reshape(PEERS, SLOTS)
            back_in[s] = jnp.sum(jnp.where(lanes // CAP == peers, tiles, 0.0), axis=0, keepdims=True)

    with scope("final"):
        slot = jnp.concatenate(slot_rows * 2, axis=0)
        found = jnp.zeros((2 * BLOCKS, 128), jnp.float32)
        for s in range(PLANES):
            row = jnp.broadcast_to(back_in[s], (2 * BLOCKS, SLOTS))
            picked = jnp.take_along_axis(row, slot & (SLOTS - 1), axis=1)
            found = jnp.where(slot >> 7 == s, picked, found)
        out_ref[...] = found[:BLOCKS]


def exchange(room, number, vmem, embeddings, cluster_ids, ranks):
    dma = pltpu.SemaphoreType.DMA
    return pl.pallas_call(
        functools.partial(kernel, room),
        out_shape=(
            jax.ShapeDtypeStruct((BLOCKS, 128), jnp.float32),
            jax.ShapeDtypeStruct((1,), jnp.int32),
        ),
        in_specs=[
            pl.BlockSpec(memory_space=pltpu.HBM),
            pl.BlockSpec(memory_space=pltpu.HBM),
            pl.BlockSpec(memory_space=pltpu.HBM),
        ],
        out_specs=(pl.BlockSpec(memory_space=pltpu.VMEM), pl.BlockSpec(memory_space=pltpu.HBM)),
        scratch_shapes=[
            pltpu.SMEM((1,), jnp.int32),
            pltpu.VMEM((ROWS_DEV, WIDTH), jnp.bfloat16),
            pltpu.VMEM((BLOCKS, 128), jnp.int32),
            pltpu.VMEM((BLOCKS, 128), jnp.int32),
            pltpu.VMEM((PLANES, 2, SLOTS), jnp.float32),
            pltpu.VMEM((PLANES, 2, SLOTS), jnp.float32),
            pltpu.VMEM((PLANES, room, WIDTH), jnp.bfloat16),
            pltpu.VMEM((PLANES, room, WIDTH), jnp.bfloat16),
            pltpu.VMEM((PLANES, PEERS, CAP, WIDTH), jnp.bfloat16),
            pltpu.VMEM((PLANES, PEERS, CAP, WIDTH), jnp.bfloat16),
            pltpu.VMEM((PLANES * SLOTS, WIDTH), jnp.bfloat16),
            pltpu.VMEM((PLANES, SLOTS), jnp.float32),
            pltpu.VMEM((PEERS, PLANES, SLOTS), jnp.float32),
            pltpu.VMEM((PEERS, 1, SLOTS), jnp.float32),
            pltpu.VMEM((PLANES, 1, SLOTS), jnp.float32),
            pltpu.VMEM((PEERS, 1, SLOTS), jnp.float32),
            pltpu.VMEM((PLANES, PEERS, 1, SLOTS), jnp.float32),
            pltpu.VMEM((PLANES, 1, SLOTS), jnp.float32),
            pltpu.VMEM((PLANES, 1, SLOTS), jnp.float32),
            dma, dma,
            dma((3,)),
            dma, dma((PLANES - 2,)),
            dma, dma((len(TOGETHER),)),
            dma, dma,
            dma((2,)), dma,
            dma, dma,
            pltpu.SemaphoreType.REGULAR((2,)),
            pltpu.SemaphoreType.REGULAR((3,)),
        ],
        compiler_params=pltpu.CompilerParams(
            collective_id=number, has_side_effects=True, vmem_limit_bytes=vmem
        ),
    )(embeddings, cluster_ids, ranks)


def shards(embeddings, cluster_ids, ranks):
    given = embeddings, cluster_ids.reshape(BLOCKS, 128), ranks.reshape(BLOCKS, 128)
    nearest, over = exchange(ROOM, 0, 40 << 20, *given)
    nearest = lax.switch(over[0], (lambda best: best, lambda best: exchange(SLOTS, 1, 67043328, *given)[0]), nearest)
    return nearest.reshape(ROWS_DEV)


def solution(mesh):
    return jax.shard_map(
        shards,
        mesh=mesh,
        in_specs=(
            P(("loader", "split"), None),
            P(("loader", "split"), None),
            P(("loader", "split")),
        ),
        out_specs=P(("loader", "split")),
        check_vma=False,
    )
```

```python
import functools

import jax
import jax.numpy as jnp
from jax import lax
from jax.experimental import pallas as pl
from jax.experimental.pallas import tpu as pltpu
from jax.sharding import PartitionSpec as P

MESH = pl.DeviceIdType.MESH
scope = jax.named_scope
CLUSTERS = 256
CAP = 4
WIDTH = 768
ROWS_DEV = 512
PLANES = 8
PEERS = 32
SLOTS = PEERS * CAP
BLOCKS = ROWS_DEV // 128
ROOM = 80
EMPTY = float(1 << 17)
GROUPS = ((0,), (1, 7), (2, 6), (5, 3), (4,))
ORDER = sum(GROUPS[1:], ())
TOGETHER = (GROUPS[0] + GROUPS[1], GROUPS[2]) + tuple((s,) for s in GROUPS[3] + GROUPS[4])
SHARED = {s: n for n, steps in enumerate(TOGETHER) for s in steps}
epsilon = 1e-06


def place():
    row = lax.axis_index("loader")
    y = lax.axis_index("split")
    return lax.div(row, 8), y, lax.rem(lax.div(row, 2), 4), lax.rem(row, 2)


def device(z, y, x, c):
    return ((z * 4 + x) * 2 + c, y)


def across(here, s):
    z, y, x, c = here
    return device(lax.rem(z + s, PLANES), y, x, c)


def within(here, j, sign):
    z, y, x, c = here
    dy, dx, dc = j % 4, j // 4 % 4, j // 16
    return device(
        z,
        lax.rem(y + (4 + sign * dy) % 4, 4),
        lax.rem(x + (4 + sign * dx) % 4, 4),
        lax.rem(c + dc, 2),
    )


def hops(j):
    return min(j % 4, 4 - j % 4) + min(j // 4 % 4, 4 - j // 4 % 4)


FIRST = [(z, y, x) for z in range(3) for y in range(4) for x in range(4) if z + min(y, 4 - y) + min(x, 4 - x) <= 2]
BESIDE = (1, 3, 4, 12, 16)
CLOSE = (1, 7)
ROUNDS = ((1, 3), (4, 12), (4, 12), (16,))
FAR_FIRST = sorted(range(1, PEERS), key=lambda j: -hops(j))


def is_first(z, y, x):
    return z + jnp.minimum(y, 4 - y) + jnp.minimum(x, 4 - x) <= 2


def send(src, dst, sent, landed, to):
    return pltpu.make_async_remote_copy(
        src_ref=src,
        dst_ref=dst,
        send_sem=sent,
        recv_sem=landed,
        device_id=to,
        device_id_type=MESH,
    )


def product(a, b):
    return lax.dot_general(
        a, b, (((1,), (1,)), ((), ())), preferred_element_type=jnp.float32
    )


def iota(shape, dim):
    return lax.broadcasted_iota(jnp.int32, shape, dim)


def own_lanes(tiles_ref):
    group = iota((PLANES, SLOTS), 1) // CAP
    total = jnp.zeros((PLANES, SLOTS), jnp.float32)
    for j in range(PEERS):
        total = jnp.where(group == j, tiles_ref[j], total)
    return total


def kernel(
    room, emb_hbm, cid_hbm, rank_hbm, out_ref, flag_hbm, flag_ref,
    raw, cid_ref, rank_ref, meta_out, meta_in, rows_out, rows_in, dense, arrived, members,
    ranks_out, ranks_in, best_out, best_rows, best_in, far_in, back_out, back_in,
    raw_sem, cid_sem, meta_landed, rows_sent, rows_landed, dense_sent, dense_landed,
    small_sent, ranks_landed, far_sent, far_landed, best_landed, back_landed, linked, met,
):
    here = place()
    z, y, x, c = here
    load_cid = pltpu.make_async_copy(cid_hbm, cid_ref, cid_sem)
    load_cid.start()
    load = pltpu.make_async_copy(emb_hbm, raw, raw_sem)
    load.start()
    with scope("greet"):
        barrier = pltpu.get_barrier_semaphore()
        for s in CLOSE:
            pl.semaphore_signal(barrier, inc=1, device_id=across(here, s), device_id_type=MESH)
        for j in BESIDE:
            pl.semaphore_signal(barrier, inc=1, device_id=within(here, j, 1), device_id_type=MESH)

    def tell(n):
        for j in ROUNDS[n]:
            pl.semaphore_signal(met.at[(0, 1, 0, 2)[n]], inc=1, device_id=within(here, j, 1), device_id_type=MESH)

    def hear(n):
        with scope(f"hear#n={n}"):
            pl.semaphore_wait(met.at[(0, 1, 0, 2)[n]], len(ROUNDS[n]))

    def tell_across(n):
        for s in (1, PLANES - 1):
            pl.semaphore_signal(linked.at[n % 2], inc=1, device_id=across(here, s), device_id_type=MESH)

    def hear_across(n):
        with scope(f"hear_across#n={n}"):
            pl.semaphore_wait(linked.at[n % 2], 2)

    with scope("count"):
        load_cid.wait()
        cid = cid_ref[...]
        owner = cid & (PEERS - 1)
        step = ((cid >> 5) - z) & (PLANES - 1)
        turned = jnp.concatenate([cid, step], axis=0).T
        before = iota((128, 128), 0) < iota((128, 128), 1)
        pack_rows, over = [], jnp.zeros((1, 128), jnp.float32)
        for b in range(BLOCKS):
            along = jnp.zeros((128, 128), jnp.float32)
            for a in range(b + 1):
                aside = turned[:, BLOCKS + a : BLOCKS + a + 1] == step[b : b + 1]
                along += jnp.where(aside & before if a == b else aside, 1.0, 0.0)
            count = jnp.sum(along, axis=0, keepdims=True).astype(jnp.int32)
            pack_rows.append(jnp.where(count < room, step[b : b + 1] * SLOTS + count, -1))
            over = jnp.maximum(over, jnp.where(count < room, 0.0, 2 * EMPTY))
        pack = jnp.concatenate(pack_rows, axis=1)
    load_rank = pltpu.make_async_copy(rank_hbm, rank_ref, cid_sem)
    load_rank.start()
    with scope("load"):
        load.wait()

    rows = {
        s: send(rows_out.at[s], rows_in.at[s], rows_sent, rows_landed.at[0 if s in GROUPS[1] else ORDER.index(s) - 1], across(here, s))
        for s in range(1, PLANES)
    }
    metas = {
        s: send(meta_out.at[s], meta_in.at[s], small_sent, meta_landed.at[0 if s in GROUPS[1] else 2 if s in GROUPS[4] else 1], across(here, s))
        for s in range(1, PLANES)
    }

    def gather_rows(group):
        chosen = jnp.concatenate(
            [jnp.where(pack == s * SLOTS + iota((room, ROWS_DEV), 0), 1.0, 0.0) for s in group], axis=0
        ).astype(jnp.bfloat16)
        picked = jnp.dot(chosen, raw[...], preferred_element_type=jnp.float32)
        scale = lax.rsqrt(jnp.sum(picked * picked, axis=1, keepdims=True) + epsilon)
        packed = (picked * scale).astype(jnp.bfloat16)
        for n, s in enumerate(group):
            ref = rows_in if s == 0 else rows_out
            ref[s] = packed[n * room : (n + 1) * room]

    with scope("pack"):
        gather_rows(GROUPS[1])
    with scope("barrier_wait"):
        pl.semaphore_wait(barrier, len(CLOSE) + len(BESIDE))
    pl.when(z == 1)(lambda: pl.delay(800))
    pl.when(z == 2)(lambda: pl.delay(1200))
    for s in GROUPS[1]:
        rows[s].start()
    tell_across(0)
    tell(0)

    with scope("slots"):
        peer = (
            (((owner >> 4) - c) & 1) * 16 + (((owner >> 2) - x) & 3) * 4 + ((owner - y) & 3)
        )
        slot_rows = []
        for b in range(BLOCKS):
            same = jnp.zeros((128, 128), jnp.float32)
            for a in range(b + 1):
                alike = turned[:, a : a + 1] == cid[b : b + 1]
                same += jnp.where(alike & before if a == b else alike, 1.0, 0.0)
            position = jnp.sum(same, axis=0, keepdims=True).astype(jnp.int32)
            slot_rows.append(step[b : b + 1] * SLOTS + peer[b : b + 1] * CAP + position)
    hear_across(0)
    tell_across(1)
    hear(0)
    tell(1)
    with scope("names"):
        over = jnp.max(over, axis=1, keepdims=True)
        slot_turned = jnp.concatenate(slot_rows + pack_rows, axis=0).T
        load_rank.wait()
        rank_turned = (rank_ref[...].astype(jnp.float32) - EMPTY).T
        lane = iota((128, 128), 1)
        for s in range(PLANES):
            name = jnp.zeros((128, 128), jnp.float32)
            rank = jnp.zeros((128, 128), jnp.float32)
            for b in range(BLOCKS):
                slots = slot_turned[:, b : b + 1]
                packs = slot_turned[:, BLOCKS + b : BLOCKS + b + 1]
                name = jnp.where(packs == s * SLOTS + lane, (slots - (s * SLOTS - 1)).astype(jnp.float32), name)
                rank = jnp.where(slots == s * SLOTS + lane, rank_turned[:, b : b + 1], rank)
            ref = meta_in if s == 0 else meta_out
            ref[s, 0:1] = jnp.sum(name, axis=0, keepdims=True) - 1.0
            ref[s, 1:2] = jnp.sum(rank, axis=0, keepdims=True) + (EMPTY + over)
    with scope("pack_rest"):
        gather_rows(GROUPS[2])
    hear_across(1)
    tell_across(2)
    for s in GROUPS[1] + GROUPS[2] + GROUPS[3]:
        metas[s].start()
    for s in GROUPS[2]:
        rows[s].start()
    hear(1)
    tell(2)
    with scope("pack_rest"):
        gather_rows(GROUPS[3])
    with scope("pack_rest"):
        gather_rows(GROUPS[4] + GROUPS[0])
    hear_across(2)
    for s in GROUPS[4]:
        metas[s].start()
    with scope("rows_wait#s=1"):
        first_two = rows_in.at[pl.ds(0, len(GROUPS[1]))]
        send(first_two, first_two, rows_sent, rows_landed.at[0], across(here, 1)).wait_recv()
    tell_across(3)
    hear_across(3)
    for s in GROUPS[3]:
        rows[s].start()
    hear(2)
    tell(3)
    hear(3)

    others = pl.ds(1, PEERS - 1)

    def spread(s):
        with scope(f"place#s={s}"):
            chosen = jnp.where(
                meta_in[s, 0:1, :room] == iota((SLOTS, room), 0).astype(jnp.float32), 1.0, 0.0
            ).astype(jnp.bfloat16)
            placed = jnp.dot(chosen, rows_in[s], preferred_element_type=jnp.float32).astype(jnp.bfloat16)
            dense[s] = placed.reshape(PEERS, CAP, WIDTH)
            arrived[s, 0] = placed[:CAP]
        with scope(f"deliver#s={s}"):
            for j in FAR_FIRST:
                send(dense.at[s, j], arrived.at[s, j], dense_sent, dense_landed.at[SHARED[s]], within(here, j, 1)).start()

    def all_dense(n):
        some = arrived.at[pl.ds(0, len(TOGETHER[n])), others]
        return send(some, some, dense_sent, dense_landed.at[n], within(here, 1, 1))

    all_ranks = send(ranks_in.at[others], ranks_in.at[others], small_sent, ranks_landed, within(here, 1, 1))
    all_best = send(best_in.at[others], best_in.at[others], small_sent, best_landed, within(here, 1, 1))

    spread(0)
    def metas_in(n, count):
        some = meta_in.at[pl.ds(0, count)]
        return send(some, some, small_sent, meta_landed.at[n], across(here, 1))

    metas_in(0, len(GROUPS[1])).wait_recv()
    for s in GROUPS[1]:
        spread(s)
    with scope("meta_wait"):
        metas_in(1, len(GROUPS[2] + GROUPS[3])).wait_recv()
    for s in GROUPS[2]:
        with scope(f"rows_wait#s={s}"):
            rows[s].wait_recv()
        if s == GROUPS[2][0]:
            for far in GROUPS[4]:
                rows[far].start()
        spread(s)
    metas_in(2, len(GROUPS[4])).wait_recv()
    metas_in(0, PLANES - 1).wait_send()
    for s in range(PLANES):
        ranks_out[s : s + 1] = meta_in[s, 1:2]
    ranks_in[0] = ranks_out[...]
    for j in FAR_FIRST:
        send(ranks_out, ranks_in.at[j], small_sent, ranks_landed, within(here, j, 1)).start()

    best = [jnp.full((1, SLOTS), -1.0, jnp.float32)] * PLANES
    seen = []

    def compare(group):
        known = len(seen)
        for s in group:
            if s == TOGETHER[SHARED[s]][0]:
                with scope(f"dense_wait#s={s}"):
                    all_dense(SHARED[s]).wait_recv()
            members[len(seen) * SLOTS : (len(seen) + 1) * SLOTS] = arrived[s].reshape(SLOTS, WIDTH)
            seen.append(s)
        with scope(f"scores#n={len(seen)}"):
            scores = product(members[known * SLOTS : len(seen) * SLOTS], members[: len(seen) * SLOTS])

            def part(n, k):
                return scores[n * SLOTS : (n + 1) * SLOTS, k * SLOTS : (k + 1) * SLOTS]

            for k, q in enumerate(seen):
                top = jnp.full((SLOTS, SLOTS), -1.0, jnp.float32)
                for n, m in enumerate(group):
                    earlier = rank_col[:, m : m + 1] < rank_row[q : q + 1]
                    top = jnp.maximum(top, jnp.where(earlier, part(n, k), -1.0))
                best[q] = jnp.maximum(best[q], jnp.max(top, axis=0, keepdims=True))
            for n, q in enumerate(group):
                if known:
                    top = jnp.full((SLOTS, SLOTS), -1.0, jnp.float32)
                    for k, m in enumerate(seen[:known]):
                        earlier = rank_row[m : m + 1] < rank_col[:, q : q + 1]
                        top = jnp.maximum(top, jnp.where(earlier, part(n, k), -1.0))
                    best[q] = jnp.maximum(best[q], jnp.max(top.T, axis=0, keepdims=True))

    for s in GROUPS[3]:
        with scope(f"rows_wait#s={s}"):
            rows[s].wait_recv()
        spread(s)
    for s in GROUPS[4]:
        with scope(f"rows_wait#s={s}"):
            rows[s].wait_recv()
        spread(s)
    with scope("ranks_wait"):
        all_ranks.wait_recv()
    rank_row = own_lanes(ranks_in)
    rank_col = rank_row.T
    highest = jnp.zeros((PLANES, SLOTS), jnp.float32)
    for j in range(PEERS):
        highest = jnp.maximum(highest, ranks_in[j])
    flag_ref[0] = jnp.max(jnp.where(highest >= 2 * EMPTY, 1, 0))
    save_flag = pltpu.make_async_copy(flag_ref, flag_hbm, cid_sem)
    save_flag.start()

    compare(GROUPS[0])
    compare(GROUPS[1])
    compare(GROUPS[2])
    for s in GROUPS[3] + GROUPS[4]:
        compare((s,))

    all_ranks.wait_send()

    lanes, peers = iota((PEERS, SLOTS), 1), iota((PEERS, SLOTS), 0)
    straight = []
    for a, b, d, e in [(*chip, core) for chip in FIRST for core in (1, 0)]:
        up, j = lax.rem(z - a + PLANES, PLANES), lax.rem(c + e, 2) * 16 + lax.rem(x - d + 4, 4) * 4 + lax.rem(y - b + 4, 4)
        straight.append((up, send(best_rows.at[up], far_in.at[up, j], far_sent.at[e], far_landed, device(a, b, d, e))))
    with scope("answer"):
        for s in range(PLANES):
            best_rows[s] = best[s]
        for up, copy in straight:
            pl.when(up != 0)(copy.start)
        answers = jnp.zeros((PEERS, SLOTS), jnp.float32)
        for s in range(PLANES):
            line = jnp.broadcast_to(best[s], (PEERS, SLOTS))
            picked = jnp.take_along_axis(line, CAP * peers + (lanes & (CAP - 1)), axis=1)
            answers = jnp.where(lanes // CAP == s, picked, answers)
        best_out[...] = answers.reshape(PEERS, 1, SLOTS)
        for j in FAR_FIRST:
            send(best_out.at[j], best_in.at[j], small_sent, best_landed, within(here, j, -1)).start()
    best_in[0] = best_out[0]
    steps = pl.ds(1, PLANES - 1)
    send(rows_out.at[steps], rows_out.at[steps], rows_sent, rows_landed.at[0], across(here, 1)).wait_send()
    send(dense.at[:, others], dense.at[:, others], dense_sent, dense_landed.at[0], across(here, 1)).wait_send()
    save_flag.wait()
    with scope("best_wait"):
        all_best.wait_recv()
    with scope("back"):
        all_best.wait_send()
        answers = best_in[...].reshape(PEERS, SLOTS)
        backs = []
        for s in (4, 3, 5, 2, 6, 1, 7, 0):
            picked = jnp.take_along_axis(answers, CAP * s + (lanes & (CAP - 1)), axis=1)
            line = jnp.sum(jnp.where(lanes // CAP == peers, picked, 0.0), axis=0, keepdims=True)
            if s == 0:
                back_in[0] = line
                continue
            back_out[s] = line
            back = send(back_out.at[s], back_in.at[s], small_sent, back_landed, across(here, PLANES - s))
            wanted = jnp.logical_not(is_first(lax.rem(z + PLANES - s, PLANES), y, x))
            pl.when(wanted)(back.start)
            backs.append((wanted, back))
    for a in range(PLANES):
        count = len([chip for chip in FIRST if chip[0] != a])

        @pl.when(z == a)
        def _():
            for e in range(2):
                some = best_in.at[pl.ds(0, count)]
                send(some, some, far_sent.at[e], far_landed, across(here, 1)).wait_send()

    sent = sum(wanted.astype(jnp.int32) for wanted, _ in backs)
    for count in range(4, PLANES):

        @pl.when(sent == count)
        def _():
            some = back_out.at[pl.ds(0, count)]
            send(some, some, small_sent, back_landed, across(here, 1)).wait_send()

    first = is_first(z, y, x)

    @pl.when(jnp.logical_not(first))
    def _():
        with scope("back_wait"):
            send(back_in.at[steps], back_in.at[steps], small_sent, back_landed, across(here, 1)).wait_recv()

    @pl.when(first)
    def _():
        with scope("far_wait"):
            send(far_in.at[steps], far_in.at[steps], far_sent.at[0], far_landed, across(here, 1)).wait_recv()
        for s in range(1, PLANES):
            tiles = far_in[s].reshape(PEERS, SLOTS)
            back_in[s] = jnp.sum(jnp.where(lanes // CAP == peers, tiles, 0.0), axis=0, keepdims=True)

    with scope("final"):
        slot = jnp.concatenate(slot_rows * 2, axis=0)
        found = jnp.zeros((2 * BLOCKS, 128), jnp.float32)
        for s in range(PLANES):
            row = jnp.broadcast_to(back_in[s], (2 * BLOCKS, SLOTS))
            picked = jnp.take_along_axis(row, slot & (SLOTS - 1), axis=1)
            found = jnp.where(slot >> 7 == s, picked, found)
        out_ref[...] = found[:BLOCKS]


def exchange(room, number, vmem, embeddings, cluster_ids, ranks):
    dma = pltpu.SemaphoreType.DMA
    return pl.pallas_call(
        functools.partial(kernel, room),
        out_shape=(
            jax.ShapeDtypeStruct((BLOCKS, 128), jnp.float32),
            jax.ShapeDtypeStruct((1,), jnp.int32),
        ),
        in_specs=[
            pl.BlockSpec(memory_space=pltpu.HBM),
            pl.BlockSpec(memory_space=pltpu.HBM),
            pl.BlockSpec(memory_space=pltpu.HBM),
        ],
        out_specs=(pl.BlockSpec(memory_space=pltpu.VMEM), pl.BlockSpec(memory_space=pltpu.HBM)),
        scratch_shapes=[
            pltpu.SMEM((1,), jnp.int32),
            pltpu.VMEM((ROWS_DEV, WIDTH), jnp.bfloat16),
            pltpu.VMEM((BLOCKS, 128), jnp.int32),
            pltpu.VMEM((BLOCKS, 128), jnp.int32),
            pltpu.VMEM((PLANES, 2, SLOTS), jnp.float32),
            pltpu.VMEM((PLANES, 2, SLOTS), jnp.float32),
            pltpu.VMEM((PLANES, room, WIDTH), jnp.bfloat16),
            pltpu.VMEM((PLANES, room, WIDTH), jnp.bfloat16),
            pltpu.VMEM((PLANES, PEERS, CAP, WIDTH), jnp.bfloat16),
            pltpu.VMEM((PLANES, PEERS, CAP, WIDTH), jnp.bfloat16),
            pltpu.VMEM((PLANES * SLOTS, WIDTH), jnp.bfloat16),
            pltpu.VMEM((PLANES, SLOTS), jnp.float32),
            pltpu.VMEM((PEERS, PLANES, SLOTS), jnp.float32),
            pltpu.VMEM((PEERS, 1, SLOTS), jnp.float32),
            pltpu.VMEM((PLANES, 1, SLOTS), jnp.float32),
            pltpu.VMEM((PEERS, 1, SLOTS), jnp.float32),
            pltpu.VMEM((PLANES, PEERS, 1, SLOTS), jnp.float32),
            pltpu.VMEM((PLANES, 1, SLOTS), jnp.float32),
            pltpu.VMEM((PLANES, 1, SLOTS), jnp.float32),
            dma, dma,
            dma((3,)),
            dma, dma((PLANES - 2,)),
            dma, dma((len(TOGETHER),)),
            dma, dma,
            dma((2,)), dma,
            dma, dma,
            pltpu.SemaphoreType.REGULAR((2,)),
            pltpu.SemaphoreType.REGULAR((3,)),
        ],
        compiler_params=pltpu.CompilerParams(
            collective_id=number, has_side_effects=True, vmem_limit_bytes=vmem
        ),
    )(embeddings, cluster_ids, ranks)


def shards(embeddings, cluster_ids, ranks):
    given = embeddings, cluster_ids.reshape(BLOCKS, 128), ranks.reshape(BLOCKS, 128)
    nearest, over = exchange(ROOM, 0, 40 << 20, *given)
    nearest = lax.switch(over[0], (lambda best: best, lambda best: exchange(SLOTS, 1, 67043328, *given)[0]), nearest)
    return nearest.reshape(ROWS_DEV)


def solution(mesh):
    return jax.shard_map(
        shards,
        mesh=mesh,
        in_specs=(
            P(("loader", "split"), None),
            P(("loader", "split"), None),
            P(("loader", "split")),
        ),
        out_specs=P(("loader", "split")),
        check_vma=False,
    )
```

```python
import functools

import jax
import jax.numpy as jnp
from jax import lax
from jax.experimental import pallas as pl
from jax.experimental.pallas import tpu as pltpu
from jax.sharding import PartitionSpec as P

MESH = pl.DeviceIdType.MESH
scope = jax.named_scope
CLUSTERS = 256
CAP = 4
WIDTH = 768
ROWS_DEV = 512
PLANES = 8
PEERS = 32
SLOTS = PEERS * CAP
BLOCKS = ROWS_DEV // 128
ROOM = 80
EMPTY = float(1 << 17)
GROUPS = ((0,), (1, 7), (2, 6), (5, 3), (4,))
ORDER = sum(GROUPS[1:], ())
TOGETHER = (GROUPS[0] + GROUPS[1], GROUPS[2]) + tuple((s,) for s in GROUPS[3] + GROUPS[4])
SHARED = {s: n for n, steps in enumerate(TOGETHER) for s in steps}
epsilon = 1e-06


def place():
    row = lax.axis_index("loader")
    y = lax.axis_index("split")
    return lax.div(row, 8), y, lax.rem(lax.div(row, 2), 4), lax.rem(row, 2)


def device(z, y, x, c):
    return ((z * 4 + x) * 2 + c, y)


def across(here, s):
    z, y, x, c = here
    return device(lax.rem(z + s, PLANES), y, x, c)


def within(here, j, sign):
    z, y, x, c = here
    dy, dx, dc = j % 4, j // 4 % 4, j // 16
    return device(
        z,
        lax.rem(y + (4 + sign * dy) % 4, 4),
        lax.rem(x + (4 + sign * dx) % 4, 4),
        lax.rem(c + dc, 2),
    )


def hops(j):
    return min(j % 4, 4 - j % 4) + min(j // 4 % 4, 4 - j // 4 % 4)


FIRST = [(z, y, x) for z in range(3) for y in range(4) for x in range(4) if z + min(y, 4 - y) + min(x, 4 - x) <= 2]
BESIDE = (1, 3, 4, 12, 16)
CLOSE = (1, 7)
ROUNDS = ((1, 3), (4, 12), (4, 12), (16,))
FAR_FIRST = sorted(range(1, PEERS), key=lambda j: -hops(j))


def is_first(z, y, x):
    return z + jnp.minimum(y, 4 - y) + jnp.minimum(x, 4 - x) <= 2


def send(src, dst, sent, landed, to):
    return pltpu.make_async_remote_copy(
        src_ref=src,
        dst_ref=dst,
        send_sem=sent,
        recv_sem=landed,
        device_id=to,
        device_id_type=MESH,
    )


def product(a, b):
    return lax.dot_general(
        a, b, (((1,), (1,)), ((), ())), preferred_element_type=jnp.float32
    )


def iota(shape, dim):
    return lax.broadcasted_iota(jnp.int32, shape, dim)


def own_lanes(tiles_ref):
    group = iota((PLANES, SLOTS), 1) // CAP
    total = jnp.zeros((PLANES, SLOTS), jnp.float32)
    for j in range(PEERS):
        total = jnp.where(group == j, tiles_ref[j], total)
    return total


def kernel(
    room, emb_hbm, cid_hbm, rank_hbm, out_ref, flag_hbm, flag_ref,
    raw, cid_ref, rank_ref, meta_out, meta_in, rows_out, rows_in, dense, arrived, members,
    ranks_out, ranks_in, best_out, best_rows, best_in, far_in, back_out, back_in,
    raw_sem, cid_sem, meta_landed, rows_sent, rows_landed, dense_sent, dense_landed,
    small_sent, ranks_landed, far_sent, far_landed, best_landed, back_landed, linked, met,
):
    here = place()
    z, y, x, c = here
    load_cid = pltpu.make_async_copy(cid_hbm, cid_ref, cid_sem)
    load_cid.start()
    load = pltpu.make_async_copy(emb_hbm, raw, raw_sem)
    load.start()
    with scope("greet"):
        barrier = pltpu.get_barrier_semaphore()
        for s in CLOSE:
            pl.semaphore_signal(barrier, inc=1, device_id=across(here, s), device_id_type=MESH)
        for j in BESIDE:
            pl.semaphore_signal(barrier, inc=1, device_id=within(here, j, 1), device_id_type=MESH)

    def tell(n):
        for j in ROUNDS[n]:
            pl.semaphore_signal(met.at[(0, 1, 0, 2)[n]], inc=1, device_id=within(here, j, 1), device_id_type=MESH)

    def hear(n):
        with scope(f"hear#n={n}"):
            pl.semaphore_wait(met.at[(0, 1, 0, 2)[n]], len(ROUNDS[n]))

    def tell_across(n):
        for s in (1, PLANES - 1):
            pl.semaphore_signal(linked.at[n % 2], inc=1, device_id=across(here, s), device_id_type=MESH)

    def hear_across(n):
        with scope(f"hear_across#n={n}"):
            pl.semaphore_wait(linked.at[n % 2], 2)

    with scope("count"):
        load_cid.wait()
        cid = cid_ref[...]
        owner = cid & (PEERS - 1)
        step = ((cid >> 5) - z) & (PLANES - 1)
        turned = jnp.concatenate([cid, step], axis=0).T
        before = iota((128, 128), 0) < iota((128, 128), 1)
        pack_rows, over = [], jnp.zeros((1, 128), jnp.float32)
        for b in range(BLOCKS):
            along = jnp.zeros((128, 128), jnp.float32)
            for a in range(b + 1):
                aside = turned[:, BLOCKS + a : BLOCKS + a + 1] == step[b : b + 1]
                along += jnp.where(aside & before if a == b else aside, 1.0, 0.0)
            count = jnp.sum(along, axis=0, keepdims=True).astype(jnp.int32)
            pack_rows.append(jnp.where(count < room, step[b : b + 1] * SLOTS + count, -1))
            over = jnp.maximum(over, jnp.where(count < room, 0.0, 2 * EMPTY))
        pack = jnp.concatenate(pack_rows, axis=1)
    load_rank = pltpu.make_async_copy(rank_hbm, rank_ref, cid_sem)
    load_rank.start()
    with scope("load"):
        load.wait()

    rows = {
        s: send(rows_out.at[s], rows_in.at[s], rows_sent, rows_landed.at[0 if s in GROUPS[1] else ORDER.index(s) - 1], across(here, s))
        for s in range(1, PLANES)
    }
    metas = {
        s: send(meta_out.at[s], meta_in.at[s], small_sent, meta_landed.at[0 if s in GROUPS[1] else 2 if s in GROUPS[4] else 1], across(here, s))
        for s in range(1, PLANES)
    }

    def gather_rows(group):
        chosen = jnp.concatenate(
            [jnp.where(pack == s * SLOTS + iota((room, ROWS_DEV), 0), 1.0, 0.0) for s in group], axis=0
        ).astype(jnp.bfloat16)
        picked = jnp.dot(chosen, raw[...], preferred_element_type=jnp.float32)
        scale = lax.rsqrt(jnp.sum(picked * picked, axis=1, keepdims=True) + epsilon)
        packed = (picked * scale).astype(jnp.bfloat16)
        for n, s in enumerate(group):
            ref = rows_in if s == 0 else rows_out
            ref[s] = packed[n * room : (n + 1) * room]

    with scope("pack"):
        gather_rows(GROUPS[1])
    with scope("barrier_wait"):
        pl.semaphore_wait(barrier, len(CLOSE) + len(BESIDE))
    for s in GROUPS[1]:
        rows[s].start()
    tell_across(0)
    tell(0)

    with scope("slots"):
        peer = (
            (((owner >> 4) - c) & 1) * 16 + (((owner >> 2) - x) & 3) * 4 + ((owner - y) & 3)
        )
        slot_rows = []
        for b in range(BLOCKS):
            same = jnp.zeros((128, 128), jnp.float32)
            for a in range(b + 1):
                alike = turned[:, a : a + 1] == cid[b : b + 1]
                same += jnp.where(alike & before if a == b else alike, 1.0, 0.0)
            position = jnp.sum(same, axis=0, keepdims=True).astype(jnp.int32)
            slot_rows.append(step[b : b + 1] * SLOTS + peer[b : b + 1] * CAP + position)
    over = jnp.max(over, axis=1, keepdims=True)
    slot_turned = jnp.concatenate(slot_rows + pack_rows, axis=0).T
    load_rank.wait()
    rank_turned = (rank_ref[...].astype(jnp.float32) - EMPTY).T
    lane = iota((128, 128), 1)

    def write_names(group):
        with scope("names"):
            for s in group:
                name = jnp.zeros((128, 128), jnp.float32)
                rank = jnp.zeros((128, 128), jnp.float32)
                for b in range(BLOCKS):
                    slots = slot_turned[:, b : b + 1]
                    packs = slot_turned[:, BLOCKS + b : BLOCKS + b + 1]
                    name = jnp.where(packs == s * SLOTS + lane, (slots - (s * SLOTS - 1)).astype(jnp.float32), name)
                    rank = jnp.where(slots == s * SLOTS + lane, rank_turned[:, b : b + 1], rank)
                ref = meta_in if s == 0 else meta_out
                ref[s, 0:1] = jnp.sum(name, axis=0, keepdims=True) - 1.0
                ref[s, 1:2] = jnp.sum(rank, axis=0, keepdims=True) + (EMPTY + over)

    hear_across(0)
    tell_across(1)
    write_names(GROUPS[1])
    for s in GROUPS[1]:
        metas[s].start()
    with scope("pack_rest"):
        gather_rows(GROUPS[2])
    hear_across(1)
    tell_across(2)
    for s in GROUPS[2]:
        rows[s].start()
    hear(0)
    tell(1)
    write_names(GROUPS[2] + GROUPS[3] + GROUPS[4] + GROUPS[0])
    for s in GROUPS[2] + GROUPS[3]:
        metas[s].start()
    hear(1)
    tell(2)
    with scope("pack_rest"):
        gather_rows(GROUPS[3])
    with scope("pack_rest"):
        gather_rows(GROUPS[4] + GROUPS[0])
    hear_across(2)
    for s in GROUPS[4]:
        metas[s].start()
    with scope("rows_wait#s=1"):
        first_two = rows_in.at[pl.ds(0, len(GROUPS[1]))]
        send(first_two, first_two, rows_sent, rows_landed.at[0], across(here, 1)).wait_recv()
    for s in GROUPS[3]:
        rows[s].start()
    hear(2)
    tell(3)
    hear(3)

    others = pl.ds(1, PEERS - 1)

    def spread(s):
        with scope(f"place#s={s}"):
            chosen = jnp.where(
                meta_in[s, 0:1, :room] == iota((SLOTS, room), 0).astype(jnp.float32), 1.0, 0.0
            ).astype(jnp.bfloat16)
            placed = jnp.dot(chosen, rows_in[s], preferred_element_type=jnp.float32).astype(jnp.bfloat16)
            dense[s] = placed.reshape(PEERS, CAP, WIDTH)
            arrived[s, 0] = placed[:CAP]
        with scope(f"deliver#s={s}"):
            for j in FAR_FIRST:
                send(dense.at[s, j], arrived.at[s, j], dense_sent, dense_landed.at[SHARED[s]], within(here, j, 1)).start()

    def all_dense(n):
        some = arrived.at[pl.ds(0, len(TOGETHER[n])), others]
        return send(some, some, dense_sent, dense_landed.at[n], within(here, 1, 1))

    all_ranks = send(ranks_in.at[others], ranks_in.at[others], small_sent, ranks_landed, within(here, 1, 1))
    all_best = send(best_in.at[others], best_in.at[others], small_sent, best_landed, within(here, 1, 1))

    spread(0)
    def metas_in(n, count):
        some = meta_in.at[pl.ds(0, count)]
        return send(some, some, small_sent, meta_landed.at[n], across(here, 1))

    metas_in(0, len(GROUPS[1])).wait_recv()
    for s in GROUPS[1]:
        spread(s)
    with scope("meta_wait"):
        metas_in(1, len(GROUPS[2] + GROUPS[3])).wait_recv()
    for s in GROUPS[2]:
        with scope(f"rows_wait#s={s}"):
            rows[s].wait_recv()
        if s == GROUPS[2][0]:
            for far in GROUPS[4]:
                rows[far].start()
        spread(s)
    metas_in(2, len(GROUPS[4])).wait_recv()
    metas_in(0, PLANES - 1).wait_send()
    for s in range(PLANES):
        ranks_out[s : s + 1] = meta_in[s, 1:2]
    ranks_in[0] = ranks_out[...]
    for j in FAR_FIRST:
        send(ranks_out, ranks_in.at[j], small_sent, ranks_landed, within(here, j, 1)).start()

    best = [jnp.full((1, SLOTS), -1.0, jnp.float32)] * PLANES
    seen = []

    def compare(group):
        known = len(seen)
        for s in group:
            if s == TOGETHER[SHARED[s]][0]:
                with scope(f"dense_wait#s={s}"):
                    all_dense(SHARED[s]).wait_recv()
            members[len(seen) * SLOTS : (len(seen) + 1) * SLOTS] = arrived[s].reshape(SLOTS, WIDTH)
            seen.append(s)
        with scope(f"scores#n={len(seen)}"):
            scores = product(members[known * SLOTS : len(seen) * SLOTS], members[: len(seen) * SLOTS])

            def part(n, k):
                return scores[n * SLOTS : (n + 1) * SLOTS, k * SLOTS : (k + 1) * SLOTS]

            for k, q in enumerate(seen):
                top = jnp.full((SLOTS, SLOTS), -1.0, jnp.float32)
                for n, m in enumerate(group):
                    earlier = rank_col[:, m : m + 1] < rank_row[q : q + 1]
                    top = jnp.maximum(top, jnp.where(earlier, part(n, k), -1.0))
                best[q] = jnp.maximum(best[q], jnp.max(top, axis=0, keepdims=True))
            for n, q in enumerate(group):
                if known:
                    top = jnp.full((SLOTS, SLOTS), -1.0, jnp.float32)
                    for k, m in enumerate(seen[:known]):
                        earlier = rank_row[m : m + 1] < rank_col[:, q : q + 1]
                        top = jnp.maximum(top, jnp.where(earlier, part(n, k), -1.0))
                    best[q] = jnp.maximum(best[q], jnp.max(top.T, axis=0, keepdims=True))

    for s in GROUPS[3]:
        with scope(f"rows_wait#s={s}"):
            rows[s].wait_recv()
        spread(s)
    for s in GROUPS[4]:
        with scope(f"rows_wait#s={s}"):
            rows[s].wait_recv()
        spread(s)
    with scope("ranks_wait"):
        all_ranks.wait_recv()
    rank_row = own_lanes(ranks_in)
    rank_col = rank_row.T
    highest = jnp.zeros((PLANES, SLOTS), jnp.float32)
    for j in range(PEERS):
        highest = jnp.maximum(highest, ranks_in[j])
    flag_ref[0] = jnp.max(jnp.where(highest >= 2 * EMPTY, 1, 0))
    save_flag = pltpu.make_async_copy(flag_ref, flag_hbm, cid_sem)
    save_flag.start()

    compare(GROUPS[0])
    compare(GROUPS[1])
    compare(GROUPS[2])
    for s in GROUPS[3] + GROUPS[4]:
        compare((s,))

    all_ranks.wait_send()

    lanes, peers = iota((PEERS, SLOTS), 1), iota((PEERS, SLOTS), 0)
    straight = []
    for a, b, d, e in [(*chip, core) for chip in FIRST for core in (1, 0)]:
        up, j = lax.rem(z - a + PLANES, PLANES), lax.rem(c + e, 2) * 16 + lax.rem(x - d + 4, 4) * 4 + lax.rem(y - b + 4, 4)
        straight.append((up, send(best_rows.at[up], far_in.at[up, j], far_sent.at[e], far_landed, device(a, b, d, e))))
    with scope("answer"):
        for s in range(PLANES):
            best_rows[s] = best[s]
        for up, copy in straight:
            pl.when(up != 0)(copy.start)
        answers = jnp.zeros((PEERS, SLOTS), jnp.float32)
        for s in range(PLANES):
            line = jnp.broadcast_to(best[s], (PEERS, SLOTS))
            picked = jnp.take_along_axis(line, CAP * peers + (lanes & (CAP - 1)), axis=1)
            answers = jnp.where(lanes // CAP == s, picked, answers)
        best_out[...] = answers.reshape(PEERS, 1, SLOTS)
        for j in FAR_FIRST:
            send(best_out.at[j], best_in.at[j], small_sent, best_landed, within(here, j, -1)).start()
    best_in[0] = best_out[0]
    steps = pl.ds(1, PLANES - 1)
    send(rows_out.at[steps], rows_out.at[steps], rows_sent, rows_landed.at[0], across(here, 1)).wait_send()
    send(dense.at[:, others], dense.at[:, others], dense_sent, dense_landed.at[0], across(here, 1)).wait_send()
    save_flag.wait()
    with scope("best_wait"):
        all_best.wait_recv()
    with scope("back"):
        all_best.wait_send()
        answers = best_in[...].reshape(PEERS, SLOTS)
        backs = []
        for s in (4, 3, 5, 2, 6, 1, 7, 0):
            picked = jnp.take_along_axis(answers, CAP * s + (lanes & (CAP - 1)), axis=1)
            line = jnp.sum(jnp.where(lanes // CAP == peers, picked, 0.0), axis=0, keepdims=True)
            if s == 0:
                back_in[0] = line
                continue
            back_out[s] = line
            back = send(back_out.at[s], back_in.at[s], small_sent, back_landed, across(here, PLANES - s))
            wanted = jnp.logical_not(is_first(lax.rem(z + PLANES - s, PLANES), y, x))
            pl.when(wanted)(back.start)
            backs.append((wanted, back))
    for a in range(PLANES):
        count = len([chip for chip in FIRST if chip[0] != a])

        @pl.when(z == a)
        def _():
            for e in range(2):
                some = best_in.at[pl.ds(0, count)]
                send(some, some, far_sent.at[e], far_landed, across(here, 1)).wait_send()

    sent = sum(wanted.astype(jnp.int32) for wanted, _ in backs)
    for count in range(4, PLANES):

        @pl.when(sent == count)
        def _():
            some = back_out.at[pl.ds(0, count)]
            send(some, some, small_sent, back_landed, across(here, 1)).wait_send()

    first = is_first(z, y, x)

    @pl.when(jnp.logical_not(first))
    def _():
        with scope("back_wait"):
            send(back_in.at[steps], back_in.at[steps], small_sent, back_landed, across(here, 1)).wait_recv()

    @pl.when(first)
    def _():
        with scope("far_wait"):
            send(far_in.at[steps], far_in.at[steps], far_sent.at[0], far_landed, across(here, 1)).wait_recv()
        for s in range(1, PLANES):
            tiles = far_in[s].reshape(PEERS, SLOTS)
            back_in[s] = jnp.sum(jnp.where(lanes // CAP == peers, tiles, 0.0), axis=0, keepdims=True)

    with scope("final"):
        slot = jnp.concatenate(slot_rows * 2, axis=0)
        found = jnp.zeros((2 * BLOCKS, 128), jnp.float32)
        for s in range(PLANES):
            row = jnp.broadcast_to(back_in[s], (2 * BLOCKS, SLOTS))
            picked = jnp.take_along_axis(row, slot & (SLOTS - 1), axis=1)
            found = jnp.where(slot >> 7 == s, picked, found)
        out_ref[...] = found[:BLOCKS]


def exchange(room, number, vmem, embeddings, cluster_ids, ranks):
    dma = pltpu.SemaphoreType.DMA
    return pl.pallas_call(
        functools.partial(kernel, room),
        out_shape=(
            jax.ShapeDtypeStruct((BLOCKS, 128), jnp.float32),
            jax.ShapeDtypeStruct((1,), jnp.int32),
        ),
        in_specs=[
            pl.BlockSpec(memory_space=pltpu.HBM),
            pl.BlockSpec(memory_space=pltpu.HBM),
            pl.BlockSpec(memory_space=pltpu.HBM),
        ],
        out_specs=(pl.BlockSpec(memory_space=pltpu.VMEM), pl.BlockSpec(memory_space=pltpu.HBM)),
        scratch_shapes=[
            pltpu.SMEM((1,), jnp.int32),
            pltpu.VMEM((ROWS_DEV, WIDTH), jnp.bfloat16),
            pltpu.VMEM((BLOCKS, 128), jnp.int32),
            pltpu.VMEM((BLOCKS, 128), jnp.int32),
            pltpu.VMEM((PLANES, 2, SLOTS), jnp.float32),
            pltpu.VMEM((PLANES, 2, SLOTS), jnp.float32),
            pltpu.VMEM((PLANES, room, WIDTH), jnp.bfloat16),
            pltpu.VMEM((PLANES, room, WIDTH), jnp.bfloat16),
            pltpu.VMEM((PLANES, PEERS, CAP, WIDTH), jnp.bfloat16),
            pltpu.VMEM((PLANES, PEERS, CAP, WIDTH), jnp.bfloat16),
            pltpu.VMEM((PLANES * SLOTS, WIDTH), jnp.bfloat16),
            pltpu.VMEM((PLANES, SLOTS), jnp.float32),
            pltpu.VMEM((PEERS, PLANES, SLOTS), jnp.float32),
            pltpu.VMEM((PEERS, 1, SLOTS), jnp.float32),
            pltpu.VMEM((PLANES, 1, SLOTS), jnp.float32),
            pltpu.VMEM((PEERS, 1, SLOTS), jnp.float32),
            pltpu.VMEM((PLANES, PEERS, 1, SLOTS), jnp.float32),
            pltpu.VMEM((PLANES, 1, SLOTS), jnp.float32),
            pltpu.VMEM((PLANES, 1, SLOTS), jnp.float32),
            dma, dma,
            dma((3,)),
            dma, dma((PLANES - 2,)),
            dma, dma((len(TOGETHER),)),
            dma, dma,
            dma((2,)), dma,
            dma, dma,
            pltpu.SemaphoreType.REGULAR((2,)),
            pltpu.SemaphoreType.REGULAR((3,)),
        ],
        compiler_params=pltpu.CompilerParams(
            collective_id=number, has_side_effects=True, vmem_limit_bytes=vmem
        ),
    )(embeddings, cluster_ids, ranks)


def shards(embeddings, cluster_ids, ranks):
    given = embeddings, cluster_ids.reshape(BLOCKS, 128), ranks.reshape(BLOCKS, 128)
    nearest, over = exchange(ROOM, 0, 40 << 20, *given)
    nearest = lax.switch(over[0], (lambda best: best, lambda best: exchange(SLOTS, 1, 67043328, *given)[0]), nearest)
    return nearest.reshape(ROWS_DEV)


def solution(mesh):
    return jax.shard_map(
        shards,
        mesh=mesh,
        in_specs=(
            P(("loader", "split"), None),
            P(("loader", "split"), None),
            P(("loader", "split")),
        ),
        out_specs=P(("loader", "split")),
        check_vma=False,
    )
```

```python
import functools

import jax
import jax.numpy as jnp
from jax import lax
from jax.experimental import pallas as pl
from jax.experimental.pallas import tpu as pltpu
from jax.sharding import PartitionSpec as P

MESH = pl.DeviceIdType.MESH
scope = jax.named_scope
CLUSTERS = 256
CAP = 4
WIDTH = 768
ROWS_DEV = 512
PLANES = 8
PEERS = 32
SLOTS = PEERS * CAP
BLOCKS = ROWS_DEV // 128
ROOM = 80
EMPTY = float(1 << 17)
GROUPS = ((0,), (1, 7), (2, 6), (5, 3), (4,))
ORDER = sum(GROUPS[1:], ())
TOGETHER = (GROUPS[0] + GROUPS[1], GROUPS[2]) + tuple((s,) for s in GROUPS[3] + GROUPS[4])
SHARED = {s: n for n, steps in enumerate(TOGETHER) for s in steps}
epsilon = 1e-06


def place():
    row = lax.axis_index("loader")
    y = lax.axis_index("split")
    return lax.div(row, 8), y, lax.rem(lax.div(row, 2), 4), lax.rem(row, 2)


def device(z, y, x, c):
    return ((z * 4 + x) * 2 + c, y)


def across(here, s):
    z, y, x, c = here
    return device(lax.rem(z + s, PLANES), y, x, c)


def within(here, j, sign):
    z, y, x, c = here
    dy, dx, dc = j % 4, j // 4 % 4, j // 16
    return device(
        z,
        lax.rem(y + (4 + sign * dy) % 4, 4),
        lax.rem(x + (4 + sign * dx) % 4, 4),
        lax.rem(c + dc, 2),
    )


def hops(j):
    return min(j % 4, 4 - j % 4) + min(j // 4 % 4, 4 - j // 4 % 4)


FIRST = [(z, y, x) for z in range(3) for y in range(4) for x in range(4) if z + min(y, 4 - y) + min(x, 4 - x) <= 2]
BESIDE = (1, 3, 4, 12, 16)
CLOSE = (1, 7)
ROUNDS = ((1, 3), (4, 12), (4, 12), (16,))
FAR_FIRST = sorted(range(1, PEERS), key=lambda j: -hops(j))


def is_first(z, y, x):
    return z + jnp.minimum(y, 4 - y) + jnp.minimum(x, 4 - x) <= 2


def send(src, dst, sent, landed, to):
    return pltpu.make_async_remote_copy(
        src_ref=src,
        dst_ref=dst,
        send_sem=sent,
        recv_sem=landed,
        device_id=to,
        device_id_type=MESH,
    )


def product(a, b):
    return lax.dot_general(
        a, b, (((1,), (1,)), ((), ())), preferred_element_type=jnp.float32
    )


def iota(shape, dim):
    return lax.broadcasted_iota(jnp.int32, shape, dim)


def own_lanes(tiles_ref):
    group = iota((PLANES, SLOTS), 1) // CAP
    total = jnp.zeros((PLANES, SLOTS), jnp.float32)
    for j in range(PEERS):
        total = jnp.where(group == j, tiles_ref[j], total)
    return total


def kernel(
    room, emb_hbm, cid_hbm, rank_hbm, out_ref, flag_hbm, flag_ref,
    raw, cid_ref, rank_ref, meta_out, meta_in, rows_out, rows_in, dense, arrived, members,
    ranks_out, ranks_in, best_out, best_rows, best_in, far_in, back_out, back_in,
    raw_sem, cid_sem, meta_landed, rows_sent, rows_landed, dense_sent, dense_landed,
    small_sent, ranks_landed, far_sent, far_landed, best_landed, back_landed, linked, met,
):
    here = place()
    z, y, x, c = here
    load_cid = pltpu.make_async_copy(cid_hbm, cid_ref, cid_sem)
    load_cid.start()
    load = pltpu.make_async_copy(emb_hbm, raw, raw_sem)
    load.start()
    with scope("greet"):
        barrier = pltpu.get_barrier_semaphore()
        for s in CLOSE:
            pl.semaphore_signal(barrier, inc=1, device_id=across(here, s), device_id_type=MESH)
        for j in BESIDE:
            pl.semaphore_signal(barrier, inc=1, device_id=within(here, j, 1), device_id_type=MESH)

    def tell(n):
        for j in ROUNDS[n]:
            pl.semaphore_signal(met.at[(0, 1, 0, 2)[n]], inc=1, device_id=within(here, j, 1), device_id_type=MESH)

    def hear(n):
        with scope(f"hear#n={n}"):
            pl.semaphore_wait(met.at[(0, 1, 0, 2)[n]], len(ROUNDS[n]))

    def tell_across(n):
        for s in (1, PLANES - 1):
            pl.semaphore_signal(linked.at[n % 2], inc=1, device_id=across(here, s), device_id_type=MESH)

    def hear_across(n):
        with scope(f"hear_across#n={n}"):
            pl.semaphore_wait(linked.at[n % 2], 2)

    with scope("count"):
        load_cid.wait()
        cid = cid_ref[...]
        owner = cid & (PEERS - 1)
        step = ((cid >> 5) - z) & (PLANES - 1)
        turned = jnp.concatenate([cid, step], axis=0).T
        before = iota((128, 128), 0) < iota((128, 128), 1)
        pack_rows, over = [], jnp.zeros((1, 128), jnp.float32)
        for b in range(BLOCKS):
            along = jnp.zeros((128, 128), jnp.float32)
            for a in range(b + 1):
                aside = turned[:, BLOCKS + a : BLOCKS + a + 1] == step[b : b + 1]
                along += jnp.where(aside & before if a == b else aside, 1.0, 0.0)
            count = jnp.sum(along, axis=0, keepdims=True).astype(jnp.int32)
            pack_rows.append(jnp.where(count < room, step[b : b + 1] * SLOTS + count, -1))
            over = jnp.maximum(over, jnp.where(count < room, 0.0, 2 * EMPTY))
        pack = jnp.concatenate(pack_rows, axis=1)
    load_rank = pltpu.make_async_copy(rank_hbm, rank_ref, cid_sem)
    load_rank.start()
    with scope("load"):
        load.wait()

    rows = {
        s: send(rows_out.at[s], rows_in.at[s], rows_sent, rows_landed.at[0 if s in GROUPS[1] else ORDER.index(s) - 1], across(here, s))
        for s in range(1, PLANES)
    }
    metas = {
        s: send(meta_out.at[s], meta_in.at[s], small_sent, meta_landed.at[0 if s in GROUPS[1] else 2 if s in GROUPS[4] else 1], across(here, s))
        for s in range(1, PLANES)
    }

    def gather_rows(group):
        chosen = jnp.concatenate(
            [jnp.where(pack == s * SLOTS + iota((room, ROWS_DEV), 0), 1.0, 0.0) for s in group], axis=0
        ).astype(jnp.bfloat16)
        picked = jnp.dot(chosen, raw[...], preferred_element_type=jnp.float32)
        scale = lax.rsqrt(jnp.sum(picked * picked, axis=1, keepdims=True) + epsilon)
        packed = (picked * scale).astype(jnp.bfloat16)
        for n, s in enumerate(group):
            ref = rows_in if s == 0 else rows_out
            ref[s] = packed[n * room : (n + 1) * room]

    with scope("pack"):
        gather_rows(GROUPS[1])
    with scope("barrier_wait"):
        pl.semaphore_wait(barrier, len(CLOSE) + len(BESIDE))
    for s in GROUPS[1]:
        rows[s].start()
    tell_across(0)
    tell(0)

    with scope("slots"):
        peer = (
            (((owner >> 4) - c) & 1) * 16 + (((owner >> 2) - x) & 3) * 4 + ((owner - y) & 3)
        )
        slot_rows = []
        for b in range(BLOCKS):
            same = jnp.zeros((128, 128), jnp.float32)
            for a in range(b + 1):
                alike = turned[:, a : a + 1] == cid[b : b + 1]
                same += jnp.where(alike & before if a == b else alike, 1.0, 0.0)
            position = jnp.sum(same, axis=0, keepdims=True).astype(jnp.int32)
            slot_rows.append(step[b : b + 1] * SLOTS + peer[b : b + 1] * CAP + position)
    over = jnp.max(over, axis=1, keepdims=True)
    slot_turned = jnp.concatenate(slot_rows + pack_rows, axis=0).T
    load_rank.wait()
    rank_turned = (rank_ref[...].astype(jnp.float32) - EMPTY).T
    lane = iota((128, 128), 1)

    def write_names(group):
        with scope("names"):
            for s in group:
                name = jnp.zeros((128, 128), jnp.float32)
                rank = jnp.zeros((128, 128), jnp.float32)
                for b in range(BLOCKS):
                    slots = slot_turned[:, b : b + 1]
                    packs = slot_turned[:, BLOCKS + b : BLOCKS + b + 1]
                    name = jnp.where(packs == s * SLOTS + lane, (slots - (s * SLOTS - 1)).astype(jnp.float32), name)
                    rank = jnp.where(slots == s * SLOTS + lane, rank_turned[:, b : b + 1], rank)
                ref = meta_in if s == 0 else meta_out
                ref[s, 0:1] = jnp.sum(name, axis=0, keepdims=True) - 1.0
                ref[s, 1:2] = jnp.sum(rank, axis=0, keepdims=True) + (EMPTY + over)

    hear_across(0)
    tell_across(1)
    write_names(GROUPS[1])
    for s in GROUPS[1]:
        metas[s].start()
    with scope("pack_rest"):
        gather_rows(GROUPS[2])
    hear_across(1)
    tell_across(2)
    for s in GROUPS[2]:
        rows[s].start()
    hear(0)
    tell(1)
    write_names(GROUPS[2] + GROUPS[3] + GROUPS[4] + GROUPS[0])
    for s in GROUPS[2] + GROUPS[3]:
        metas[s].start()
    hear(1)
    tell(2)
    with scope("pack_rest"):
        gather_rows(GROUPS[3])
    with scope("pack_rest"):
        gather_rows(GROUPS[4] + GROUPS[0])
    hear_across(2)
    for s in GROUPS[4]:
        metas[s].start()
    with scope("rows_wait#s=1"):
        first_two = rows_in.at[pl.ds(0, len(GROUPS[1]))]
        send(first_two, first_two, rows_sent, rows_landed.at[0], across(here, 1)).wait_recv()
    for s in GROUPS[3]:
        rows[s].start()
    hear(2)
    tell(3)
    hear(3)

    others = pl.ds(1, PEERS - 1)

    def spread(s):
        with scope(f"place#s={s}"):
            chosen = jnp.where(
                meta_in[s, 0:1, :room] == iota((SLOTS, room), 0).astype(jnp.float32), 1.0, 0.0
            ).astype(jnp.bfloat16)
            placed = jnp.dot(chosen, rows_in[s], preferred_element_type=jnp.float32).astype(jnp.bfloat16)
            dense[s] = placed.reshape(PEERS, CAP, WIDTH)
            arrived[s, 0] = placed[:CAP]
        with scope(f"deliver#s={s}"):
            for j in FAR_FIRST:
                send(dense.at[s, j], arrived.at[s, j], dense_sent, dense_landed.at[SHARED[s]], within(here, j, 1)).start()

    def all_dense(n):
        some = arrived.at[pl.ds(0, len(TOGETHER[n])), others]
        return send(some, some, dense_sent, dense_landed.at[n], within(here, 1, 1))

    all_ranks = send(ranks_in.at[others], ranks_in.at[others], small_sent, ranks_landed, within(here, 1, 1))
    all_best = send(best_in.at[others], best_in.at[others], small_sent, best_landed, within(here, 1, 1))

    spread(0)
    def metas_in(n, count):
        some = meta_in.at[pl.ds(0, count)]
        return send(some, some, small_sent, meta_landed.at[n], across(here, 1))

    metas_in(0, len(GROUPS[1])).wait_recv()
    for s in GROUPS[1]:
        spread(s)
    with scope("meta_wait"):
        metas_in(1, len(GROUPS[2] + GROUPS[3])).wait_recv()
    for s in GROUPS[4]:
        rows[s].start()
    for s in GROUPS[2]:
        with scope(f"rows_wait#s={s}"):
            rows[s].wait_recv()
        spread(s)
    metas_in(2, len(GROUPS[4])).wait_recv()
    metas_in(0, PLANES - 1).wait_send()
    for s in range(PLANES):
        ranks_out[s : s + 1] = meta_in[s, 1:2]
    ranks_in[0] = ranks_out[...]
    for j in FAR_FIRST:
        send(ranks_out, ranks_in.at[j], small_sent, ranks_landed, within(here, j, 1)).start()

    best = [jnp.full((1, SLOTS), -1.0, jnp.float32)] * PLANES
    seen = []

    def compare(group):
        known = len(seen)
        for s in group:
            if s == TOGETHER[SHARED[s]][0]:
                with scope(f"dense_wait#s={s}"):
                    all_dense(SHARED[s]).wait_recv()
            members[len(seen) * SLOTS : (len(seen) + 1) * SLOTS] = arrived[s].reshape(SLOTS, WIDTH)
            seen.append(s)
        with scope(f"scores#n={len(seen)}"):
            scores = product(members[known * SLOTS : len(seen) * SLOTS], members[: len(seen) * SLOTS])

            def part(n, k):
                return scores[n * SLOTS : (n + 1) * SLOTS, k * SLOTS : (k + 1) * SLOTS]

            over_old = [jnp.full((SLOTS, SLOTS), -1.0, jnp.float32) for _ in group]
            for k, q in enumerate(seen):
                top = jnp.full((SLOTS, SLOTS), -1.0, jnp.float32)
                for n, m in enumerate(group):
                    earlier = rank_col[:, m : m + 1] < rank_row[q : q + 1]
                    top = jnp.maximum(top, jnp.where(earlier, part(n, k), -1.0))
                    if k < known:
                        over_old[n] = jnp.maximum(over_old[n], jnp.where(earlier, -1.0, part(n, k)))
                best[q] = jnp.maximum(best[q], jnp.max(top, axis=0, keepdims=True))
            for n, q in enumerate(group):
                if known:
                    best[q] = jnp.maximum(best[q], jnp.max(over_old[n].T, axis=0, keepdims=True))

    for s in GROUPS[3]:
        with scope(f"rows_wait#s={s}"):
            rows[s].wait_recv()
        spread(s)
    for s in GROUPS[4]:
        with scope(f"rows_wait#s={s}"):
            rows[s].wait_recv()
        spread(s)
    with scope("ranks_wait"):
        all_ranks.wait_recv()
    rank_row = own_lanes(ranks_in)
    rank_col = rank_row.T
    highest = jnp.zeros((PLANES, SLOTS), jnp.float32)
    for j in range(PEERS):
        highest = jnp.maximum(highest, ranks_in[j])
    flag_ref[0] = jnp.max(jnp.where(highest >= 2 * EMPTY, 1, 0))
    save_flag = pltpu.make_async_copy(flag_ref, flag_hbm, cid_sem)
    save_flag.start()

    compare(GROUPS[0])
    compare(GROUPS[1])
    compare(GROUPS[2])
    for s in GROUPS[3] + GROUPS[4]:
        compare((s,))

    all_ranks.wait_send()

    lanes, peers = iota((PEERS, SLOTS), 1), iota((PEERS, SLOTS), 0)
    straight = []
    for a, b, d, e in [(*chip, core) for chip in FIRST for core in (1, 0)]:
        up, j = lax.rem(z - a + PLANES, PLANES), lax.rem(c + e, 2) * 16 + lax.rem(x - d + 4, 4) * 4 + lax.rem(y - b + 4, 4)
        straight.append((up, send(best_rows.at[up], far_in.at[up, j], far_sent.at[e], far_landed, device(a, b, d, e))))
    with scope("answer"):
        for s in range(PLANES):
            best_rows[s] = best[s]
        for up, copy in straight:
            pl.when(up != 0)(copy.start)
        answers = jnp.zeros((PEERS, SLOTS), jnp.float32)
        for s in range(PLANES):
            line = jnp.broadcast_to(best[s], (PEERS, SLOTS))
            picked = jnp.take_along_axis(line, CAP * peers + (lanes & (CAP - 1)), axis=1)
            answers = jnp.where(lanes // CAP == s, picked, answers)
        best_out[...] = answers.reshape(PEERS, 1, SLOTS)
        for j in FAR_FIRST:
            send(best_out.at[j], best_in.at[j], small_sent, best_landed, within(here, j, -1)).start()
    best_in[0] = best_out[0]
    steps = pl.ds(1, PLANES - 1)
    send(rows_out.at[steps], rows_out.at[steps], rows_sent, rows_landed.at[0], across(here, 1)).wait_send()
    send(dense.at[:, others], dense.at[:, others], dense_sent, dense_landed.at[0], across(here, 1)).wait_send()
    save_flag.wait()
    with scope("best_wait"):
        all_best.wait_recv()
    with scope("back"):
        all_best.wait_send()
        answers = best_in[...].reshape(PEERS, SLOTS)
        backs = []
        for s in (4, 3, 5, 2, 6, 1, 7, 0):
            picked = jnp.take_along_axis(answers, CAP * s + (lanes & (CAP - 1)), axis=1)
            line = jnp.sum(jnp.where(lanes // CAP == peers, picked, 0.0), axis=0, keepdims=True)
            if s == 0:
                back_in[0] = line
                continue
            back_out[s] = line
            back = send(back_out.at[s], back_in.at[s], small_sent, back_landed, across(here, PLANES - s))
            wanted = jnp.logical_not(is_first(lax.rem(z + PLANES - s, PLANES), y, x))
            pl.when(wanted)(back.start)
            backs.append((wanted, back))
    for a in range(PLANES):
        count = len([chip for chip in FIRST if chip[0] != a])

        @pl.when(z == a)
        def _():
            for e in range(2):
                some = best_in.at[pl.ds(0, count)]
                send(some, some, far_sent.at[e], far_landed, across(here, 1)).wait_send()

    sent = sum(wanted.astype(jnp.int32) for wanted, _ in backs)
    for count in range(4, PLANES):

        @pl.when(sent == count)
        def _():
            some = back_out.at[pl.ds(0, count)]
            send(some, some, small_sent, back_landed, across(here, 1)).wait_send()

    first = is_first(z, y, x)

    @pl.when(jnp.logical_not(first))
    def _():
        with scope("back_wait"):
            send(back_in.at[steps], back_in.at[steps], small_sent, back_landed, across(here, 1)).wait_recv()

    @pl.when(first)
    def _():
        with scope("far_wait"):
            send(far_in.at[steps], far_in.at[steps], far_sent.at[0], far_landed, across(here, 1)).wait_recv()
        for s in range(1, PLANES):
            tiles = far_in[s].reshape(PEERS, SLOTS)
            back_in[s] = jnp.sum(jnp.where(lanes // CAP == peers, tiles, 0.0), axis=0, keepdims=True)

    with scope("final"):
        slot = jnp.concatenate(slot_rows * 2, axis=0)
        found = jnp.zeros((2 * BLOCKS, 128), jnp.float32)
        for s in range(PLANES):
            row = jnp.broadcast_to(back_in[s], (2 * BLOCKS, SLOTS))
            picked = jnp.take_along_axis(row, slot & (SLOTS - 1), axis=1)
            found = jnp.where(slot >> 7 == s, picked, found)
        out_ref[...] = found[:BLOCKS]


def exchange(room, number, vmem, embeddings, cluster_ids, ranks):
    dma = pltpu.SemaphoreType.DMA
    return pl.pallas_call(
        functools.partial(kernel, room),
        out_shape=(
            jax.ShapeDtypeStruct((BLOCKS, 128), jnp.float32),
            jax.ShapeDtypeStruct((1,), jnp.int32),
        ),
        in_specs=[
            pl.BlockSpec(memory_space=pltpu.HBM),
            pl.BlockSpec(memory_space=pltpu.HBM),
            pl.BlockSpec(memory_space=pltpu.HBM),
        ],
        out_specs=(pl.BlockSpec(memory_space=pltpu.VMEM), pl.BlockSpec(memory_space=pltpu.HBM)),
        scratch_shapes=[
            pltpu.SMEM((1,), jnp.int32),
            pltpu.VMEM((ROWS_DEV, WIDTH), jnp.bfloat16),
            pltpu.VMEM((BLOCKS, 128), jnp.int32),
            pltpu.VMEM((BLOCKS, 128), jnp.int32),
            pltpu.VMEM((PLANES, 2, SLOTS), jnp.float32),
            pltpu.VMEM((PLANES, 2, SLOTS), jnp.float32),
            pltpu.VMEM((PLANES, room, WIDTH), jnp.bfloat16),
            pltpu.VMEM((PLANES, room, WIDTH), jnp.bfloat16),
            pltpu.VMEM((PLANES, PEERS, CAP, WIDTH), jnp.bfloat16),
            pltpu.VMEM((PLANES, PEERS, CAP, WIDTH), jnp.bfloat16),
            pltpu.VMEM((PLANES * SLOTS, WIDTH), jnp.bfloat16),
            pltpu.VMEM((PLANES, SLOTS), jnp.float32),
            pltpu.VMEM((PEERS, PLANES, SLOTS), jnp.float32),
            pltpu.VMEM((PEERS, 1, SLOTS), jnp.float32),
            pltpu.VMEM((PLANES, 1, SLOTS), jnp.float32),
            pltpu.VMEM((PEERS, 1, SLOTS), jnp.float32),
            pltpu.VMEM((PLANES, PEERS, 1, SLOTS), jnp.float32),
            pltpu.VMEM((PLANES, 1, SLOTS), jnp.float32),
            pltpu.VMEM((PLANES, 1, SLOTS), jnp.float32),
            dma, dma,
            dma((3,)),
            dma, dma((PLANES - 2,)),
            dma, dma((len(TOGETHER),)),
            dma, dma,
            dma((2,)), dma,
            dma, dma,
            pltpu.SemaphoreType.REGULAR((2,)),
            pltpu.SemaphoreType.REGULAR((3,)),
        ],
        compiler_params=pltpu.CompilerParams(
            collective_id=number, has_side_effects=True, vmem_limit_bytes=vmem
        ),
    )(embeddings, cluster_ids, ranks)


def shards(embeddings, cluster_ids, ranks):
    given = embeddings, cluster_ids.reshape(BLOCKS, 128), ranks.reshape(BLOCKS, 128)
    nearest, over = exchange(ROOM, 0, 40 << 20, *given)
    nearest = lax.switch(over[0], (lambda best: best, lambda best: exchange(SLOTS, 1, 67043328, *given)[0]), nearest)
    return nearest.reshape(ROWS_DEV)


def solution(mesh):
    return jax.shard_map(
        shards,
        mesh=mesh,
        in_specs=(
            P(("loader", "split"), None),
            P(("loader", "split"), None),
            P(("loader", "split")),
        ),
        out_specs=P(("loader", "split")),
        check_vma=False,
    )
```

```python
import functools

import jax
import jax.numpy as jnp
from jax import lax
from jax.experimental import pallas as pl
from jax.experimental.pallas import tpu as pltpu
from jax.sharding import PartitionSpec as P

MESH = pl.DeviceIdType.MESH
scope = jax.named_scope
CLUSTERS = 256
CAP = 4
WIDTH = 768
ROWS_DEV = 512
PLANES = 8
PEERS = 32
SLOTS = PEERS * CAP
BLOCKS = ROWS_DEV // 128
ROOM = 80
EMPTY = float(1 << 17)
GROUPS = ((0,), (1, 7), (2, 6), (5, 3), (4,))
ORDER = sum(GROUPS[1:], ())
TOGETHER = (GROUPS[0] + GROUPS[1], GROUPS[2]) + tuple((s,) for s in GROUPS[3] + GROUPS[4])
SHARED = {s: n for n, steps in enumerate(TOGETHER) for s in steps}
epsilon = 1e-06


def place():
    row = lax.axis_index("loader")
    y = lax.axis_index("split")
    return lax.div(row, 8), y, lax.rem(lax.div(row, 2), 4), lax.rem(row, 2)


def device(z, y, x, c):
    return ((z * 4 + x) * 2 + c, y)


def across(here, s):
    z, y, x, c = here
    return device(lax.rem(z + s, PLANES), y, x, c)


def within(here, j, sign):
    z, y, x, c = here
    dy, dx, dc = j % 4, j // 4 % 4, j // 16
    return device(
        z,
        lax.rem(y + (4 + sign * dy) % 4, 4),
        lax.rem(x + (4 + sign * dx) % 4, 4),
        lax.rem(c + dc, 2),
    )


def hops(j):
    return min(j % 4, 4 - j % 4) + min(j // 4 % 4, 4 - j // 4 % 4)


FIRST = [
    (z, y, x, c)
    for z in range(4)
    for y in range(4)
    for x in range(4)
    for c in (1, 0)
    if z + min(y, 4 - y) + min(x, 4 - x) + c <= 3
]
BESIDE = (1, 3, 4, 12, 16)
CLOSE = (1, 7)
ROUNDS = ((1, 3), (4, 12), (4, 12), (16,))
FAR_FIRST = sorted(range(1, PEERS), key=lambda j: -hops(j))


def is_first(z, y, x, c):
    return z + jnp.minimum(y, 4 - y) + jnp.minimum(x, 4 - x) + c <= 3


def send(src, dst, sent, landed, to):
    return pltpu.make_async_remote_copy(
        src_ref=src,
        dst_ref=dst,
        send_sem=sent,
        recv_sem=landed,
        device_id=to,
        device_id_type=MESH,
    )


def product(a, b):
    return lax.dot_general(
        a, b, (((1,), (1,)), ((), ())), preferred_element_type=jnp.float32
    )


def iota(shape, dim):
    return lax.broadcasted_iota(jnp.int32, shape, dim)


def own_lanes(tiles_ref):
    group = iota((PLANES, SLOTS), 1) // CAP
    total = jnp.zeros((PLANES, SLOTS), jnp.float32)
    for j in range(PEERS):
        total = jnp.where(group == j, tiles_ref[j], total)
    return total


def kernel(
    room, emb_hbm, cid_hbm, rank_hbm, out_ref, flag_hbm, flag_ref,
    raw, cid_ref, rank_ref, meta_out, meta_in, rows_out, rows_in, dense, arrived, members,
    ranks_out, ranks_in, best_out, best_rows, best_in, far_in, back_out, back_in,
    raw_sem, cid_sem, meta_landed, rows_sent, rows_landed, dense_sent, dense_landed,
    small_sent, ranks_landed, far_sent, far_landed, best_landed, back_landed, linked, met,
):
    here = place()
    z, y, x, c = here
    load_cid = pltpu.make_async_copy(cid_hbm, cid_ref, cid_sem)
    load_cid.start()
    load = pltpu.make_async_copy(emb_hbm, raw, raw_sem)
    load.start()
    with scope("greet"):
        barrier = pltpu.get_barrier_semaphore()
        for s in CLOSE:
            pl.semaphore_signal(barrier, inc=1, device_id=across(here, s), device_id_type=MESH)
        for j in BESIDE:
            pl.semaphore_signal(barrier, inc=1, device_id=within(here, j, 1), device_id_type=MESH)

    def tell(n):
        for j in ROUNDS[n]:
            pl.semaphore_signal(met.at[(0, 1, 0, 2)[n]], inc=1, device_id=within(here, j, 1), device_id_type=MESH)

    def hear(n):
        with scope(f"hear#n={n}"):
            pl.semaphore_wait(met.at[(0, 1, 0, 2)[n]], len(ROUNDS[n]))

    def tell_across(n):
        for s in (1, PLANES - 1):
            pl.semaphore_signal(linked.at[n % 2], inc=1, device_id=across(here, s), device_id_type=MESH)

    def hear_across(n):
        with scope(f"hear_across#n={n}"):
            pl.semaphore_wait(linked.at[n % 2], 2)

    with scope("count"):
        load_cid.wait()
        cid = cid_ref[...]
        owner = cid & (PEERS - 1)
        step = ((cid >> 5) - z) & (PLANES - 1)
        turned = jnp.concatenate([cid, step], axis=0).T
        before = iota((128, 128), 0) < iota((128, 128), 1)
        pack_rows, over = [], jnp.zeros((1, 128), jnp.float32)
        for b in range(BLOCKS):
            along = jnp.zeros((128, 128), jnp.float32)
            for a in range(b + 1):
                aside = turned[:, BLOCKS + a : BLOCKS + a + 1] == step[b : b + 1]
                along += jnp.where(aside & before if a == b else aside, 1.0, 0.0)
            count = jnp.sum(along, axis=0, keepdims=True).astype(jnp.int32)
            pack_rows.append(jnp.where(count < room, step[b : b + 1] * SLOTS + count, -1))
            over = jnp.maximum(over, jnp.where(count < room, 0.0, 2 * EMPTY))
        pack = jnp.concatenate(pack_rows, axis=1)
    load_rank = pltpu.make_async_copy(rank_hbm, rank_ref, cid_sem)
    load_rank.start()
    with scope("load"):
        load.wait()

    rows = {
        s: send(rows_out.at[s], rows_in.at[s], rows_sent, rows_landed.at[0 if s in GROUPS[1] else ORDER.index(s) - 1], across(here, s))
        for s in range(1, PLANES)
    }
    metas = {
        s: send(meta_out.at[s], meta_in.at[s], small_sent, meta_landed.at[0 if s in GROUPS[1] else 2 if s in GROUPS[4] else 1], across(here, s))
        for s in range(1, PLANES)
    }

    def gather_rows(group):
        chosen = jnp.concatenate(
            [jnp.where(pack == s * SLOTS + iota((room, ROWS_DEV), 0), 1.0, 0.0) for s in group], axis=0
        ).astype(jnp.bfloat16)
        picked = jnp.dot(chosen, raw[...], preferred_element_type=jnp.float32)
        scale = lax.rsqrt(jnp.sum(picked * picked, axis=1, keepdims=True) + epsilon)
        packed = (picked * scale).astype(jnp.bfloat16)
        for n, s in enumerate(group):
            ref = rows_in if s == 0 else rows_out
            ref[s] = packed[n * room : (n + 1) * room]

    with scope("pack"):
        gather_rows(GROUPS[1])
    with scope("barrier_wait"):
        pl.semaphore_wait(barrier, len(CLOSE) + len(BESIDE))
    for s in GROUPS[1]:
        rows[s].start()
    tell_across(0)
    tell(0)

    with scope("slots"):
        peer = (
            (((owner >> 4) - c) & 1) * 16 + (((owner >> 2) - x) & 3) * 4 + ((owner - y) & 3)
        )
        slot_rows = []
        for b in range(BLOCKS):
            same = jnp.zeros((128, 128), jnp.float32)
            for a in range(b + 1):
                alike = turned[:, a : a + 1] == cid[b : b + 1]
                same += jnp.where(alike & before if a == b else alike, 1.0, 0.0)
            position = jnp.sum(same, axis=0, keepdims=True).astype(jnp.int32)
            slot_rows.append(step[b : b + 1] * SLOTS + peer[b : b + 1] * CAP + position)
    over = jnp.max(over, axis=1, keepdims=True)
    slot_turned = jnp.concatenate(slot_rows + pack_rows, axis=0).T
    load_rank.wait()
    rank_turned = (rank_ref[...].astype(jnp.float32) - EMPTY).T
    lane = iota((128, 128), 1)

    def write_names(group):
        with scope("names"):
            for s in group:
                name = jnp.zeros((128, 128), jnp.float32)
                rank = jnp.zeros((128, 128), jnp.float32)
                for b in range(BLOCKS):
                    slots = slot_turned[:, b : b + 1]
                    packs = slot_turned[:, BLOCKS + b : BLOCKS + b + 1]
                    name = jnp.where(packs == s * SLOTS + lane, (slots - (s * SLOTS - 1)).astype(jnp.float32), name)
                    rank = jnp.where(slots == s * SLOTS + lane, rank_turned[:, b : b + 1], rank)
                ref = meta_in if s == 0 else meta_out
                ref[s, 0:1] = jnp.sum(name, axis=0, keepdims=True) - 1.0
                ref[s, 1:2] = jnp.sum(rank, axis=0, keepdims=True) + (EMPTY + over)

    hear_across(0)
    tell_across(1)
    write_names(GROUPS[1])
    for s in GROUPS[1]:
        metas[s].start()
    with scope("pack_rest"):
        gather_rows(GROUPS[2])
    hear_across(1)
    tell_across(2)
    for s in GROUPS[2]:
        rows[s].start()
    hear(0)
    tell(1)
    write_names(GROUPS[2] + GROUPS[3] + GROUPS[4] + GROUPS[0])
    for s in GROUPS[2] + GROUPS[3]:
        metas[s].start()
    hear(1)
    tell(2)
    with scope("pack_rest"):
        gather_rows(GROUPS[3])
    with scope("pack_rest"):
        gather_rows(GROUPS[4] + GROUPS[0])
    hear_across(2)
    for s in GROUPS[4]:
        metas[s].start()
    with scope("rows_wait#s=1"):
        first_two = rows_in.at[pl.ds(0, len(GROUPS[1]))]
        send(first_two, first_two, rows_sent, rows_landed.at[0], across(here, 1)).wait_recv()
    for s in GROUPS[3]:
        rows[s].start()
    hear(2)
    tell(3)
    hear(3)

    others = pl.ds(1, PEERS - 1)

    def spread(s):
        with scope(f"place#s={s}"):
            chosen = jnp.where(
                meta_in[s, 0:1, :room] == iota((SLOTS, room), 0).astype(jnp.float32), 1.0, 0.0
            ).astype(jnp.bfloat16)
            placed = jnp.dot(chosen, rows_in[s], preferred_element_type=jnp.float32).astype(jnp.bfloat16)
            dense[s] = placed.reshape(PEERS, CAP, WIDTH)
            arrived[s, 0] = placed[:CAP]
        with scope(f"deliver#s={s}"):
            for j in FAR_FIRST:
                send(dense.at[s, j], arrived.at[s, j], dense_sent, dense_landed.at[SHARED[s]], within(here, j, 1)).start()

    def all_dense(n):
        some = arrived.at[pl.ds(0, len(TOGETHER[n])), others]
        return send(some, some, dense_sent, dense_landed.at[n], within(here, 1, 1))

    all_ranks = send(ranks_in.at[others], ranks_in.at[others], small_sent, ranks_landed, within(here, 1, 1))
    all_best = send(best_in.at[others], best_in.at[others], small_sent, best_landed, within(here, 1, 1))

    spread(0)
    def metas_in(n, count):
        some = meta_in.at[pl.ds(0, count)]
        return send(some, some, small_sent, meta_landed.at[n], across(here, 1))

    metas_in(0, len(GROUPS[1])).wait_recv()
    for s in GROUPS[1]:
        spread(s)
    with scope("meta_wait"):
        metas_in(1, len(GROUPS[2] + GROUPS[3])).wait_recv()
    for s in GROUPS[4]:
        rows[s].start()
    for s in GROUPS[2]:
        with scope(f"rows_wait#s={s}"):
            rows[s].wait_recv()
        spread(s)
    metas_in(2, len(GROUPS[4])).wait_recv()
    metas_in(0, PLANES - 1).wait_send()
    for s in range(PLANES):
        ranks_out[s : s + 1] = meta_in[s, 1:2]
    ranks_in[0] = ranks_out[...]
    for j in FAR_FIRST:
        send(ranks_out, ranks_in.at[j], small_sent, ranks_landed, within(here, j, 1)).start()

    best = [jnp.full((1, SLOTS), -1.0, jnp.float32)] * PLANES
    seen = []

    def compare(group):
        known = len(seen)
        for s in group:
            if s == TOGETHER[SHARED[s]][0]:
                with scope(f"dense_wait#s={s}"):
                    all_dense(SHARED[s]).wait_recv()
            members[len(seen) * SLOTS : (len(seen) + 1) * SLOTS] = arrived[s].reshape(SLOTS, WIDTH)
            seen.append(s)
        with scope(f"scores#n={len(seen)}"):
            scores = product(members[known * SLOTS : len(seen) * SLOTS], members[: len(seen) * SLOTS])

            def part(n, k):
                return scores[n * SLOTS : (n + 1) * SLOTS, k * SLOTS : (k + 1) * SLOTS]

            over_old = [jnp.full((SLOTS, SLOTS), -1.0, jnp.float32) for _ in group]
            for k, q in enumerate(seen):
                top = jnp.full((SLOTS, SLOTS), -1.0, jnp.float32)
                for n, m in enumerate(group):
                    earlier = rank_col[:, m : m + 1] < rank_row[q : q + 1]
                    top = jnp.maximum(top, jnp.where(earlier, part(n, k), -1.0))
                    if k < known:
                        over_old[n] = jnp.maximum(over_old[n], jnp.where(earlier, -1.0, part(n, k)))
                best[q] = jnp.maximum(best[q], jnp.max(top, axis=0, keepdims=True))
            for n, q in enumerate(group):
                if known:
                    best[q] = jnp.maximum(best[q], jnp.max(over_old[n].T, axis=0, keepdims=True))

    for s in GROUPS[3]:
        with scope(f"rows_wait#s={s}"):
            rows[s].wait_recv()
        spread(s)
    for s in GROUPS[4]:
        with scope(f"rows_wait#s={s}"):
            rows[s].wait_recv()
        spread(s)
    with scope("ranks_wait"):
        all_ranks.wait_recv()
    rank_row = own_lanes(ranks_in)
    rank_col = rank_row.T
    highest = jnp.zeros((PLANES, SLOTS), jnp.float32)
    for j in range(PEERS):
        highest = jnp.maximum(highest, ranks_in[j])
    flag_ref[0] = jnp.max(jnp.where(highest >= 2 * EMPTY, 1, 0))
    save_flag = pltpu.make_async_copy(flag_ref, flag_hbm, cid_sem)
    save_flag.start()

    compare(GROUPS[0])
    compare(GROUPS[1])
    compare(GROUPS[2])
    for s in GROUPS[3] + GROUPS[4]:
        compare((s,))

    all_ranks.wait_send()

    lanes, peers = iota((PEERS, SLOTS), 1), iota((PEERS, SLOTS), 0)
    straight = []
    for a, b, d, e in FIRST:
        up, j = lax.rem(z - a + PLANES, PLANES), lax.rem(c + e, 2) * 16 + lax.rem(x - d + 4, 4) * 4 + lax.rem(y - b + 4, 4)
        straight.append((up, send(best_rows.at[up], far_in.at[up, j], far_sent.at[e], far_landed, device(a, b, d, e))))
    with scope("answer"):
        for s in range(PLANES):
            best_rows[s] = best[s]
        for up, copy in straight:
            pl.when(up != 0)(copy.start)
        answers = jnp.zeros((PEERS, SLOTS), jnp.float32)
        for s in range(PLANES):
            line = jnp.broadcast_to(best[s], (PEERS, SLOTS))
            picked = jnp.take_along_axis(line, CAP * peers + (lanes & (CAP - 1)), axis=1)
            answers = jnp.where(lanes // CAP == s, picked, answers)
        best_out[...] = answers.reshape(PEERS, 1, SLOTS)
        for j in FAR_FIRST:
            send(best_out.at[j], best_in.at[j], small_sent, best_landed, within(here, j, -1)).start()
    best_in[0] = best_out[0]
    steps = pl.ds(1, PLANES - 1)
    send(rows_out.at[steps], rows_out.at[steps], rows_sent, rows_landed.at[0], across(here, 1)).wait_send()
    send(dense.at[:, others], dense.at[:, others], dense_sent, dense_landed.at[0], across(here, 1)).wait_send()
    save_flag.wait()
    with scope("best_wait"):
        all_best.wait_recv()
    with scope("back"):
        all_best.wait_send()
        answers = best_in[...].reshape(PEERS, SLOTS)
        backs = []
        for s in (4, 3, 5, 2, 6, 1, 7, 0):
            picked = jnp.take_along_axis(answers, CAP * s + (lanes & (CAP - 1)), axis=1)
            line = jnp.sum(jnp.where(lanes // CAP == peers, picked, 0.0), axis=0, keepdims=True)
            if s == 0:
                back_in[0] = line
                continue
            back_out[s] = line
            back = send(back_out.at[s], back_in.at[s], small_sent, back_landed, across(here, PLANES - s))
            wanted = jnp.logical_not(is_first(lax.rem(z + PLANES - s, PLANES), y, x, c))
            pl.when(wanted)(back.start)
            backs.append((wanted, back))
    for a in range(PLANES):
        counts = [len([to for to in FIRST if to[0] != a and to[3] == e]) for e in range(2)]

        @pl.when(z == a)
        def _():
            for e, count in enumerate(counts):
                some = best_in.at[pl.ds(0, count)]
                send(some, some, far_sent.at[e], far_landed, across(here, 1)).wait_send()

    sent = sum(wanted.astype(jnp.int32) for wanted, _ in backs)
    for count in range(3, PLANES):

        @pl.when(sent == count)
        def _():
            some = back_out.at[pl.ds(0, count)]
            send(some, some, small_sent, back_landed, across(here, 1)).wait_send()

    first = is_first(z, y, x, c)

    @pl.when(jnp.logical_not(first))
    def _():
        with scope("back_wait"):
            send(back_in.at[steps], back_in.at[steps], small_sent, back_landed, across(here, 1)).wait_recv()

    @pl.when(first)
    def _():
        with scope("far_wait"):
            send(far_in.at[steps], far_in.at[steps], far_sent.at[0], far_landed, across(here, 1)).wait_recv()
        for s in range(1, PLANES):
            tiles = far_in[s].reshape(PEERS, SLOTS)
            back_in[s] = jnp.sum(jnp.where(lanes // CAP == peers, tiles, 0.0), axis=0, keepdims=True)

    with scope("final"):
        slot = jnp.concatenate(slot_rows * 2, axis=0)
        found = jnp.zeros((2 * BLOCKS, 128), jnp.float32)
        for s in range(PLANES):
            row = jnp.broadcast_to(back_in[s], (2 * BLOCKS, SLOTS))
            picked = jnp.take_along_axis(row, slot & (SLOTS - 1), axis=1)
            found = jnp.where(slot >> 7 == s, picked, found)
        out_ref[...] = found[:BLOCKS]


def exchange(room, number, vmem, embeddings, cluster_ids, ranks):
    dma = pltpu.SemaphoreType.DMA
    return pl.pallas_call(
        functools.partial(kernel, room),
        out_shape=(
            jax.ShapeDtypeStruct((BLOCKS, 128), jnp.float32),
            jax.ShapeDtypeStruct((1,), jnp.int32),
        ),
        in_specs=[
            pl.BlockSpec(memory_space=pltpu.HBM),
            pl.BlockSpec(memory_space=pltpu.HBM),
            pl.BlockSpec(memory_space=pltpu.HBM),
        ],
        out_specs=(pl.BlockSpec(memory_space=pltpu.VMEM), pl.BlockSpec(memory_space=pltpu.HBM)),
        scratch_shapes=[
            pltpu.SMEM((1,), jnp.int32),
            pltpu.VMEM((ROWS_DEV, WIDTH), jnp.bfloat16),
            pltpu.VMEM((BLOCKS, 128), jnp.int32),
            pltpu.VMEM((BLOCKS, 128), jnp.int32),
            pltpu.VMEM((PLANES, 2, SLOTS), jnp.float32),
            pltpu.VMEM((PLANES, 2, SLOTS), jnp.float32),
            pltpu.VMEM((PLANES, room, WIDTH), jnp.bfloat16),
            pltpu.VMEM((PLANES, room, WIDTH), jnp.bfloat16),
            pltpu.VMEM((PLANES, PEERS, CAP, WIDTH), jnp.bfloat16),
            pltpu.VMEM((PLANES, PEERS, CAP, WIDTH), jnp.bfloat16),
            pltpu.VMEM((PLANES * SLOTS, WIDTH), jnp.bfloat16),
            pltpu.VMEM((PLANES, SLOTS), jnp.float32),
            pltpu.VMEM((PEERS, PLANES, SLOTS), jnp.float32),
            pltpu.VMEM((PEERS, 1, SLOTS), jnp.float32),
            pltpu.VMEM((PLANES, 1, SLOTS), jnp.float32),
            pltpu.VMEM((PEERS, 1, SLOTS), jnp.float32),
            pltpu.VMEM((PLANES, PEERS, 1, SLOTS), jnp.float32),
            pltpu.VMEM((PLANES, 1, SLOTS), jnp.float32),
            pltpu.VMEM((PLANES, 1, SLOTS), jnp.float32),
            dma, dma,
            dma((3,)),
            dma, dma((PLANES - 2,)),
            dma, dma((len(TOGETHER),)),
            dma, dma,
            dma((2,)), dma,
            dma, dma,
            pltpu.SemaphoreType.REGULAR((2,)),
            pltpu.SemaphoreType.REGULAR((3,)),
        ],
        compiler_params=pltpu.CompilerParams(
            collective_id=number, has_side_effects=True, vmem_limit_bytes=vmem
        ),
    )(embeddings, cluster_ids, ranks)


def shards(embeddings, cluster_ids, ranks):
    given = embeddings, cluster_ids.reshape(BLOCKS, 128), ranks.reshape(BLOCKS, 128)
    nearest, over = exchange(ROOM, 0, 40 << 20, *given)
    nearest = lax.switch(over[0], (lambda best: best, lambda best: exchange(SLOTS, 1, 67043328, *given)[0]), nearest)
    return nearest.reshape(ROWS_DEV)


def solution(mesh):
    return jax.shard_map(
        shards,
        mesh=mesh,
        in_specs=(
            P(("loader", "split"), None),
            P(("loader", "split"), None),
            P(("loader", "split")),
        ),
        out_specs=P(("loader", "split")),
        check_vma=False,
    )
```
